512 devices in a mesh: groups: 2 (over y), shell: 128 (over x, z), batch: 2 (over core).
Axes of the slice: x: 4, y: 2, z: 32, core: 2. Of those that a mesh axis runs over, the one named last changes fastest.
The devices are a block of a 4x8x32 slice.
Arguments:
- particles: bfloat16 [320, 16384], P(('groups', 'batch'), 'shell'), parts along dimension 0, may hold values from -5 to 5
- classes: bfloat16 [512, 16384], P('groups', 'shell'), parts along dimension 0, may hold values from -2.5 to 2.5
- ctf: float32 [16, 8192], P('groups', 'shell'), parts along dimension 0, may hold values from 0.1 to 1
- sigma2: float32 [128], P('groups'), parts along dimension 0, may hold values from 0.5 to 8
- shell_of: int32 [8192], P('shell'), may hold values from 0 to 63, as said below
- rot_table: int32 [48, 8192], P(None, 'shell'), may hold values from 0 to 8191, as said below
- ctf_group: int32 [320], P(('groups', 'batch')), parts along dimension 0, may hold values from 0 to 7
Outputs:
- class_sums: float32 [512, 16384], P('groups', 'shell'), parts along dimension 0
- class_weights: float32 [512, 8192], P('groups', 'shell'), parts along dimension 0
- log_evidence: float32 [320], P(('groups', 'batch')), parts along dimension 0
The draws below stay inside these ranges and needn't reach their ends.
There are 2 independent parts, one for each index of `groups`. The reference program is written for one: setup_inputs(seed, part) draws one part's arguments, and reference() takes and returns one part's arrays. A program takes and returns all parts, laid end to end along the dimension named above; an argument that names none is the same for every part. Nothing has to cross between parts.
Inputs may be any that keep to these rules, and one draw needn't show every extreme that they name: shell_of never falls along the coefficients; its first entry is 0 and its last 63. `rot_table`: for each rotation, each aligned block of 64 coefficients is mapped onto itself one to one; rotation 0 maps every coefficient to itself.
All inputs are finite; a program needn't handle non-finite values.
Results may differ from the reference program's by a relative error of at most 0.0041.
Values may be sent and summed in bfloat16 or wider, within the bound.
A program may use at most 64 MiB of HBM per device.

```python
import math
import jax
import jax.numpy as jnp
from jax import lax

K = 256
ROT = 48
CO_DEV = 64
SHELLS = 64
CTFG = 8
COEF = 8192
PARTICLES = 160
N_SHELL = 128


def particle_field(key):
    shape = (PARTICLES, 2 * COEF)
    return jnp.clip(jax.random.normal(jax.random.fold_in(key, 11), shape, jnp.float32), -5.0, 5.0)


def draw_particles(key, part):
    return particle_field(key).astype(jnp.bfloat16)


def draw_classes(key, part):
    noise = jnp.clip(jax.random.normal(jax.random.fold_in(key, 21), (K, 2 * COEF), jnp.float32), -5.0, 5.0) * 0.02
    return noise.astype(jnp.bfloat16)


def draw_shell_of(key, part):
    values = jnp.sort(jax.random.randint(key, (COEF,), 0, SHELLS, dtype=jnp.int32))
    values = values.at[0].set(0).at[COEF - 1].set(SHELLS - 1)
    return values.astype(jnp.int32)


def draw_rot_table(key, part):
    blocks = COEF // CO_DEV
    ranks = jnp.arange(CO_DEV, dtype=jnp.int32)
    keyed = jax.random.randint(key, (ROT, blocks, CO_DEV), 0, 1048576, dtype=jnp.int32) * CO_DEV + ranks
    order = jnp.argsort(keyed, axis=-1, stable=True).astype(jnp.int32)
    identity = jnp.broadcast_to(ranks, (blocks, CO_DEV))
    order = order.at[0].set(identity)
    offsets = (jnp.arange(blocks, dtype=jnp.int32) * CO_DEV)[None, :, None]
    return (order + offsets).reshape(ROT, COEF).astype(jnp.int32)


def touch_ends(values, stream_key, least, high):
    longest = values.shape.index(max(values.shape))
    spots = []
    for shift in (0, 1):
        where = [jax.random.randint(jax.random.fold_in(stream_key, axis), (), 0, length) for axis, length in enumerate(values.shape)]
        where[longest] = (where[longest] + shift) % values.shape[longest]
        spots.append(tuple(where))
    return values.at[spots[0]].set(least).at[spots[1]].set(high)


def levels(own_key, extent, split, low, high):
    factor_of, own = 1.0, jax.random.fold_in(own_key, 6)
    for dim, shards_of in split:
        draws = jnp.exp(jax.random.uniform(jax.random.fold_in(own, dim), (shards_of,), jnp.float32, low / len(split), high / len(split)))
        factor_of = factor_of * jnp.repeat(draws, extent[dim] // shards_of).reshape([-1 if axis == dim else 1 for axis in range(len(extent))])
    return factor_of


def setup_inputs(seed: int = 0, part: int = 0) -> dict:
    seeds = jax.random.split(jax.random.key(seed), 8)
    own_keys = jax.random.split(jax.random.fold_in(seeds[7], part), 8)
    return {
        "particles": draw_particles(jax.random.fold_in(jax.random.fold_in(seeds[7], part), 71), part),
        "classes": draw_classes(jax.random.fold_in(jax.random.fold_in(seeds[7], part), 71), part),
        "ctf": jnp.clip(0.1 + 0.9 * jax.random.uniform(own_keys[2], (CTFG, COEF), jnp.float32) ** levels(own_keys[2], (CTFG, COEF), ((1, 128),), -0.2, 0.2), 0.1, 1.0),
        "sigma2": jnp.clip(jnp.exp(jax.random.uniform(own_keys[3], (SHELLS,), jnp.float32, math.log(0.5), math.log(8.0))), 0.5, 8.0),
        "shell_of": draw_shell_of(jax.random.fold_in(seeds[7], 71), part),
        "rot_table": draw_rot_table(jax.random.fold_in(seeds[7], 71), part),
        "ctf_group": touch_ends(jax.random.randint(own_keys[6], (PARTICLES,), 0, CTFG), jax.random.fold_in(own_keys[6], 1), 0, CTFG - 1).astype(jnp.int32),
    }


def halves(array):
    rows = array.shape[0]
    blocks = array.reshape(rows, N_SHELL, 2, CO_DEV)
    return blocks[:, :, 0, :].reshape(rows, COEF), blocks[:, :, 1, :].reshape(rows, COEF)


def join_parts(real_part, imag_part):
    rows = real_part.shape[0]
    stacked = jnp.stack([real_part.reshape(rows, N_SHELL, CO_DEV), imag_part.reshape(rows, N_SHELL, CO_DEV)], axis=2)
    return stacked.reshape(rows, 2 * COEF)


def reference(particles, classes, ctf, sigma2, shell_of, rot_table, ctf_group):
    highest = lax.Precision.HIGHEST
    weight = 1.0 / sigma2[shell_of]
    real_part, imag_part = halves(particles.astype(jnp.float32))
    class_real, class_imag = halves(classes)
    ctf_part = ctf[ctf_group]
    weighted_ctf = weight[None, :] * ctf_part
    weighted_real = (weighted_ctf * real_part).astype(jnp.bfloat16)
    weighted_imag = (weighted_ctf * imag_part).astype(jnp.bfloat16)
    ctf_power = weight[None, :] * ctf * ctf

    def score_rotation(table_row):
        rot_real = class_real[:, table_row]
        rot_imag = class_imag[:, table_row]
        cross_terms = jnp.dot(weighted_real, rot_real.T, preferred_element_type=jnp.float32)
        cross_terms = cross_terms + jnp.dot(weighted_imag, rot_imag.T, preferred_element_type=jnp.float32)
        class_power = rot_real.astype(jnp.float32) ** 2 + rot_imag.astype(jnp.float32) ** 2
        penalty = jnp.dot(ctf_power, class_power.T, precision=highest, preferred_element_type=jnp.float32)
        return cross_terms - 0.5 * penalty[ctf_group]

    scores = lax.map(score_rotation, rot_table)
    scores = jnp.transpose(scores, (1, 2, 0)).reshape(PARTICLES, K * ROT)
    peak = jnp.max(scores, axis=1)
    log_evidence = peak + jnp.log(jnp.sum(jnp.exp(scores - peak[:, None]), axis=1))
    posterior = jnp.exp(scores - log_evidence[:, None]).astype(jnp.bfloat16).reshape(PARTICLES, K, ROT)
    sources = jnp.concatenate([ctf_part * real_part, ctf_part * imag_part, ctf_part * ctf_part], axis=1).astype(jnp.bfloat16)

    def add_rotation(totals, inputs):
        post_rot, table_row = inputs
        frame = jnp.dot(post_rot.T, sources, preferred_element_type=jnp.float32).reshape(K, 3, COEF)
        return totals.at[:, :, table_row].add(frame), None

    totals, unused = lax.scan(add_rotation, jnp.zeros((K, 3, COEF), jnp.float32), (jnp.transpose(posterior, (2, 0, 1)), rot_table))
    class_sums = join_parts(totals[:, 0], totals[:, 1])
    return class_sums, totals[:, 2], log_evidence
```

```python
import functools

import jax
import jax.numpy as jnp
from jax import lax
from jax.experimental import pallas as pl
from jax.experimental.pallas import tpu as pltpu
from jax.sharding import Mesh
from jax.sharding import PartitionSpec as P

MESH = pl.DeviceIdType.MESH
ROW = 4
SIDE = 4
NP = ROW * SIDE
OWNERS = 4
LANES = 128
F32 = jnp.float32
BF16 = jnp.bfloat16
NT = (((1,), (1,)), ((), ()))
AXES = ("groups", "x", "z", "batch")


def lane(shape):
    return lax.broadcasted_iota(jnp.int32, shape, 1)


def compact(w):
    free = lane((8, LANES)) >= 80
    kept = []
    for r in range(0, w.shape[0], 48):
        a, b = w[r + 32 : r + 40], w[r + 40 : r + 48]
        kept += [
            jnp.where(free, pltpu.roll(a, 80, 1), w[r : r + 8]),
            jnp.where(free, pltpu.roll(a, 32, 1), w[r + 8 : r + 16]),
            jnp.where(free, pltpu.roll(b, 80, 1), w[r + 16 : r + 24]),
            jnp.where(free, pltpu.roll(b, 32, 1), w[r + 24 : r + 32]),
        ]
    return jnp.concatenate(kept, axis=0)


def expand(w):
    first = lane((8, LANES)) < 48
    whole = []
    for r in range(0, w.shape[0], 32):
        part = w[r : r + 32]
        whole += [
            part,
            jnp.where(first, pltpu.roll(part[0:8], 48, 1), pltpu.roll(part[8:16], 96, 1)),
            jnp.where(first, pltpu.roll(part[16:24], 48, 1), pltpu.roll(part[24:32], 96, 1)),
        ]
    return jnp.concatenate(whole, axis=0)


def spread(row):
    free = lane((1, LANES)) >= 80
    return jnp.where(free, pltpu.roll(row, 80, 1), row), jnp.where(free, pltpu.roll(row, 32, 1), row)


def tiles(even, odd, rows):
    e = jnp.broadcast_to(even, (8, LANES))
    o = jnp.broadcast_to(odd, (8, LANES))
    return jnp.concatenate([e, o] * (rows // 16), axis=0)


def over_rows(values, combine, reduce):
    split = [values[r : r + 8] for r in range(0, values.shape[0], 8)]
    even = reduce(functools.reduce(combine, split[0::2]), axis=0, keepdims=True)
    odd = reduce(functools.reduce(combine, split[1::2]), axis=0, keepdims=True)
    first = lane((1, LANES)) < 48
    moved = jnp.where(first, pltpu.roll(even, 48, 1), pltpu.roll(odd, 96, 1))
    return combine(combine(even, odd), moved)


def kernel(
    nz,
    part_hbm,
    cls_hbm,
    ctf_hbm,
    sig_hbm,
    sh_hbm,
    tab_hbm,
    grp_hbm,
    mine_ref,
    other_ref,
    ev_ref,
    cls_ref,
    ctf_ref,
    sig_ref,
    sh_ref,
    tab_ref,
    grp_ref,
    bundle,
    cls_z,
    cls_all,
    place,
    w_all,
    src_all,
    left,
    rot_all,
    score,
    rs_send,
    rs_scale,
    rs_recv,
    rs_rscale,
    ag_send,
    top_send,
    ag_recv,
    top_recv,
    lse_own,
    lse_all,
    post,
    frame,
    out_send,
    sizes,
    in_sem,
    g_ssem,
    z_rsem,
    x_rsem,
    rs_ssem,
    rs_rsem,
    ag_ssem,
    ag_rsem,
    top_rsem,
    lse_ssem,
    lse_rsem,
    o_ssem,
    o_rsem,
    c_ssem,
    c_rsem,
    owner_in,
):
    nb = nz // SIDE
    count, coef = part_hbm.shape[0], ctf_ref.shape[1]
    kb = cls_all.shape[1]
    half = tab_ref.shape[0] // 2
    rows = half * kb // OWNERS
    group = lax.axis_index("groups")
    x = lax.axis_index("x")
    z = lax.axis_index("z")
    core = lax.axis_index("batch")
    zb, zi = z // SIDE, lax.rem(z, SIDE)
    me = zi * ROW + x
    owner = jnp.where(
        jnp.logical_and(zb >= 1, zb < 3), zb - 1, jnp.where(jnp.logical_and(zb >= nb - 3, zb < nb - 1), zb - nb + 5, OWNERS)
    )

    def home(o):
        return jnp.where(o < 2, o + 1, o + nb - 5)

    def turn_in(b):
        return jnp.where(b == 0, nb - 2, jnp.where(b == nb - 1, nb - 1, b - 1))

    my_turn = turn_in(zb)

    def at(x_, z_):
        return (group, x_, z_, core)

    def mate(k):
        i = lax.rem(me + k, NP)
        return i, at(lax.rem(i, ROW), zb * SIDE + i // ROW)

    def far(b):
        return at(x, b * SIDE + zi)

    partner = (group, x, z, 1 - core)

    def remote(src, dst, ssem, rsem, device):
        return pltpu.make_async_remote_copy(
            src_ref=src, dst_ref=dst, send_sem=ssem, recv_sem=rsem, device_id=device, device_id_type=MESH
        )

    def drain(semaphore, size):
        whole = sizes.at[0:size]
        remote(whole, whole, semaphore, semaphore, partner).wait_recv()

    def each(lower, upper, step):
        def turn(k, _):
            step(k)
            return 0

        lax.fori_loop(lower, upper, turn, 0)

    def tell(semaphore, device):
        pl.semaphore_signal(semaphore, inc=1, device_id=device, device_id_type=MESH)

    def rows_of(i, n):
        return pl.ds(pl.multiple_of(i * n, n), n)

    given = (ctf_hbm, sig_hbm, sh_hbm, tab_hbm, part_hbm, cls_hbm.at[rows_of(zi, ROW * kb)], cls_hbm, grp_hbm)
    taken = (ctf_ref, sig_ref, sh_ref, tab_ref, bundle.at[me, 0:count], cls_z.at[zi], cls_ref, grp_ref)
    loads = [pltpu.make_async_copy(a, b, in_sem.at[k]) for k, (a, b) in enumerate(zip(given, taken))]
    for load in loads:
        load.start()

    barrier = pltpu.get_barrier_semaphore()
    each(1, NP, lambda k: tell(barrier, mate(k)[1]))
    tell(barrier, partner)

    def greet_later(b):
        @pl.when(turn_in(b) > my_turn)
        def _():
            tell(barrier, far(b))

    each(0, nb, greet_later)
    for load in loads[:4]:
        load.wait()

    levels = sig_ref.shape[1]
    pick = (lax.broadcasted_iota(jnp.int32, (levels, coef), 0) == sh_ref[...]).astype(F32)
    noise = jnp.dot(
        jnp.broadcast_to(sig_ref[...], (8, levels)), pick, precision=lax.Precision.HIGHEST, preferred_element_type=F32
    )
    ctf = ctf_ref[...]
    par = jnp.concatenate([ctf, (1.0 / noise[0:1]) * ctf], axis=1)
    par_high = par.astype(BF16).astype(F32)
    par_mid = (par - par_high).astype(BF16).astype(F32)
    offset = (x * nz + z) * coef
    table = (tab_ref[...] - offset).astype(F32)
    table = jnp.concatenate([table[:half], table[half:]], axis=1)
    bundle[me, count:] = jnp.concatenate([table, par_high, par_mid, (par - par_high) - par_mid], axis=0).astype(BF16)
    for load in loads[4:]:
        load.wait()
    with jax.named_scope("barrier"):
        pl.semaphore_wait(barrier, NP + my_turn)

    def down(k):
        i = lax.rem(zi + k, SIDE)
        device = at(x, zb * SIDE + i)
        remote(bundle.at[me], bundle.at[me], g_ssem, z_rsem.at[zi], device).start()
        remote(cls_ref.at[rows_of(i, ROW * kb)], cls_z.at[zi], g_ssem, z_rsem.at[zi], device).start()

    def across(i):
        b = i * ROW + x
        for k in range(1, ROW):
            to = lax.rem(x + k, ROW)
            device = at(to, z)
            remote(bundle.at[b], bundle.at[b], g_ssem, x_rsem.at[b], device).start()
            remote(cls_z.at[i, rows_of(to, kb)], cls_all.at[b], g_ssem, x_rsem.at[b], device).start()

    bundle_size = bundle.shape[1] // 2
    each(1, SIDE, down)
    across(zi)

    @pl.when(owner < OWNERS)
    def _():
        def tell_earlier(b):
            @pl.when(turn_in(b) < my_turn)
            def _():
                tell(owner_in.at[owner], far(b))

        each(0, nb, tell_earlier)

    with jax.named_scope("zeros"):
        w_all[...] = jnp.zeros_like(w_all)
        src_all[...] = jnp.zeros_like(src_all)
        left[...] = jnp.zeros_like(left)
    score[...] = jnp.zeros_like(score)
    cls_all[me] = cls_z[zi, rows_of(x, kb), :]
    member = jnp.broadcast_to(grp_ref[...].astype(F32), (LANES, count)).T
    low = lane((count, LANES)) < coef
    low_kb = lane((kb, LANES)) < coef

    def pass_on(i):
        @pl.when(i != zi)
        def _():
            with jax.named_scope("came_down"):
                drain(z_rsem.at[i], bundle_size + ROW * kb // 2)
            across(i)
            cls_all[i * ROW + x] = cls_z[i, rows_of(x, kb), :]

    def amplitudes(tail):
        par = tail[half : half + 8] + tail[half + 8 : half + 16] + tail[half + 16 : half + 24]
        sel = jnp.broadcast_to(par[0:1], (count, LANES))
        for g in range(1, par.shape[0]):
            sel = jnp.where(member == g, par[g : g + 1], sel)
        other = pltpu.roll(sel, coef, 1)
        return jnp.where(low, sel, other), jnp.where(low, other, sel)

    def turned_over(a):
        return jnp.concatenate([a, jnp.zeros((LANES - count, LANES), F32)], axis=0).astype(BF16).T

    def prepare(g, i):
        b = g * 4 + i
        landing = bundle[b, count:].astype(F32)
        amp, wamp = amplitudes(landing)
        weighted = turned_over(wamp * bundle[b, 0:count].astype(F32))
        pen = -0.5 * (wamp * amp)
        pen_hi = pen.astype(BF16).astype(F32)
        pen = turned_over(jnp.where(low, pen_hi, pen - pen_hi))
        for s in range(2):
            lanes = slice(s * LANES, (s + 1) * LANES)
            for k, piece in enumerate((weighted[:coef], weighted[coef:], pen[:coef], pen[:coef], pen[coef:])):
                top = (5 * i + k) * LANES + s * coef
                w_all[g, top : top + coef, lanes] = piece
        index = lax.broadcasted_iota(jnp.int32, (coef, LANES), 0).astype(F32).astype(BF16)
        ones, zeros = jnp.ones((coef, LANES), BF16), jnp.zeros((coef, LANES), BF16)
        for j in range(half):
            row = jnp.broadcast_to(landing[j : j + 1], (16, LANES)).astype(BF16)
            row = jnp.concatenate([row] * (coef // 16), axis=0)
            place[rows_of(b, coef), j * LANES : (j + 1) * LANES] = jnp.where(index == row, ones, zeros)

    def prepare_sources(b):
        amp, _ = amplitudes(bundle[b, count:].astype(F32))
        source = amp * bundle[b, 0:count].astype(F32)
        source_turned = pltpu.roll(source, coef, 1)
        power = amp * amp
        for s in range(2):
            top = s * LANES

            def keep(lower, upper):
                return (jnp.where(low, lower, 0.0) if s == 0 else jnp.where(low, 0.0, upper)).astype(BF16)

            src_all[b, top : top + count, 0:128] = keep(source, source_turned)
            src_all[b, top : top + count, 128:256] = keep(source_turned, source)
            src_all[b, top : top + count, 256:384] = keep(power, power)

    def rotate(g):
        for i in range(4):
            image = cls_all[g * 4 + i].astype(F32)
            turned = pltpu.roll(image, coef, 1)
            if i % 2 == 0:
                re, im = jnp.where(low_kb, image, 0.0), jnp.where(low_kb, turned, 0.0)
            else:
                re, im = jnp.where(low_kb, 0.0, turned), jnp.where(low_kb, 0.0, image)
            top = (i // 2) * LANES
            left[g, 2 * i * kb : (2 * i + 1) * kb, top : top + LANES] = re.astype(BF16)
            left[g, (2 * i + 1) * kb : (2 * i + 2) * kb, top : top + LANES] = im.astype(BF16)
        lhs = left[g]
        for jj in range(half // 2):
            turned = jnp.dot(
                lhs, place[rows_of(g, 4 * coef), jj * 256 : (jj + 1) * 256], preferred_element_type=F32
            )
            for i in range(4):
                for t in range(2):
                    j = jj * 2 + t
                    re = turned[2 * i * kb : (2 * i + 1) * kb, t * LANES : (t + 1) * LANES]
                    im = turned[(2 * i + 1) * kb : (2 * i + 2) * kb, t * LANES : (t + 1) * LANES]
                    power = re * re + im * im
                    power_hi = power.astype(BF16)
                    power_lo = (power - power_hi.astype(F32)).astype(BF16)
                    to = slice(j * kb, (j + 1) * kb)
                    pieces = re.astype(BF16), im.astype(BF16), power_hi, power_lo, power_hi
                    for k, piece in enumerate(pieces):
                        at_lane = (5 * i + k) * LANES
                        rot_all[g, to, at_lane : at_lane + LANES] = piece

    def score_row(g):
        with jax.named_scope("arrive"):
            each(1, ROW, lambda k: drain(x_rsem.at[g * ROW + lax.rem(x + k, ROW)], bundle_size + kb // 2))
        with jax.named_scope("prepare"):
            for i in range(ROW):
                prepare(g, i)
        with jax.named_scope("scores"):
            rotate(g)
            score[...] += jnp.dot(rot_all[g], w_all[g], preferred_element_type=F32)

    each(0, SIDE - 1, pass_on)

    def turn_of(g):
        @pl.when(g == 1)
        def _():
            pass_on(SIDE - 1)

        score_row(g)

    each(0, SIDE, turn_of)

    def share(o):
        return score[rows_of(o, rows), :]

    share_size = rs_send.shape[1] + rs_scale.shape[1]
    for o in (1, 2, 0, 3):

        @pl.when(owner != o)
        def _():
            piece = share(o)
            one, two = piece[:, :LANES], piece[:, LANES:]
            most = jnp.max(jnp.maximum(one, two), axis=0, keepdims=True)
            least = jnp.min(jnp.minimum(one, two), axis=0, keepdims=True)
            middle = 0.5 * (most + least)
            reach = jnp.maximum(0.5 * (most - least), 1e-30)
            fit = 32767.0 / reach
            one = jnp.round((one - middle) * fit).astype(jnp.int32)
            two = jnp.round((two - middle) * fit).astype(jnp.int32)
            rs_send[o] = compact((one & 0xFFFF) | (two << 16))
            rs_scale[o] = jnp.concatenate([*spread(reach * (1.0 / 32767.0)), *spread(middle)], axis=0)

            @pl.when(turn_in(home(o)) > my_turn)
            def _():
                with jax.named_scope("owner_in"):
                    pl.semaphore_wait(owner_in.at[o], 1)

            with jax.named_scope("share_go"):
                remote(rs_send.at[o], rs_recv.at[zb], rs_ssem, rs_rsem.at[zb], far(home(o))).start()
                remote(rs_scale.at[o], rs_rscale.at[zb], rs_ssem, rs_rsem.at[zb], far(home(o))).start()

    with jax.named_scope("sources"):
        each(0, NP, prepare_sources)

    @pl.when(owner < OWNERS)
    def _():
        own = share(owner)
        total = compact(own[:, :LANES]), compact(own[:, LANES:])

        def add_share(k, so_far):
            b = jnp.where(k < zb, k, k + 1)
            with jax.named_scope("share_in"):
                drain(rs_rsem.at[b], share_size)
            word = rs_recv[b]
            step = tiles(rs_rscale[b, 0:1], rs_rscale[b, 1:2], word.shape[0])
            middle = tiles(rs_rscale[b, 2:3], rs_rscale[b, 3:4], word.shape[0])
            return (
                so_far[0] + (((word << 16) >> 16).astype(F32) * step + middle),
                so_far[1] + ((word >> 16).astype(F32) * step + middle),
            )

        total_one, total_two = lax.fori_loop(0, nb - 1, add_share, total)
        peak = over_rows(jnp.maximum(total_one, total_two), jnp.maximum, jnp.max)
        shift = tiles(*spread(peak), total_one.shape[0])
        exp_one, exp_two = jnp.exp(total_one - shift), jnp.exp(total_two - shift)
        evidence = peak + jnp.log(over_rows(exp_one + exp_two, jnp.add, jnp.sum))
        top_send[...] = jnp.concatenate([peak, evidence], axis=0)

        def send_top(b):
            @pl.when(b != zb)
            def _():
                remote(top_send, top_recv.at[owner], ag_ssem, top_rsem.at[owner], far(b)).start()

        each(0, nb, send_top)
        one = (exp_one * 65535.0 + 0.5).astype(jnp.int32)
        two = (exp_two * 65535.0 + 0.5).astype(jnp.int32)
        ag_send[...] = (one & 0xFFFF) | (two << 16)

        def send_post(b):
            @pl.when(b != zb)
            def _():
                remote(ag_send, ag_recv.at[owner], ag_ssem, ag_rsem.at[owner], far(b)).start()

        each(0, nb, send_post)
        ag_recv[owner] = ag_send[...]
        top_recv[owner] = top_send[...]

    def take_top(o):
        @pl.when(o != owner)
        def _():
            with jax.named_scope("top_in"):
                drain(top_rsem.at[o], top_send.shape[0])

    each(0, OWNERS, take_top)

    def merged(parts):
        most = functools.reduce(jnp.maximum, parts)
        return most + jnp.log(functools.reduce(jnp.add, [jnp.exp(e - most) for e in parts]))

    evidence = merged([top_recv[o, 1:2] for o in range(OWNERS)])
    lse_own[...] = evidence
    each(1, NP, lambda k: remote(lse_own, lse_all.at[me], lse_ssem, lse_rsem, mate(k)[1]).start())
    lse_all[me] = evidence
    with jax.named_scope("lse_in"):
        drain(lse_rsem, NP - 1)
    everyone = lse_all[...]
    most = jnp.max(everyone, axis=0)
    evidence = most + jnp.log(jnp.sum(jnp.exp(everyone - most[None]), axis=0))
    ev_ref[...] = evidence
    used = lane((rows, LANES)) < count

    def take_post(o):
        @pl.when(o != owner)
        def _():
            with jax.named_scope("post_in"):
                drain(ag_rsem.at[o], ag_send.shape[0])

        word = expand(ag_recv[o])
        scale = jnp.exp(top_recv[o, 0:1] - evidence) * (1.0 / 65535.0)
        one = jnp.where(used, (word & 0xFFFF).astype(F32) * scale, 0.0)
        two = jnp.where(used, lax.shift_right_logical(word, 16).astype(F32) * scale, 0.0)
        post[rows_of(o, rows), 0:128] = one.astype(BF16)
        post[rows_of(o, rows), 128:256] = two.astype(BF16)

    each(0, OWNERS, take_post)

    def class_row(i):
        for k in range(ROW):
            frames = jnp.dot(post[...], src_all[i * ROW + k], preferred_element_type=F32)
            for j in range(half):
                for t in range(3):
                    frame[k, t * kb : (t + 1) * kb, j * LANES : (j + 1) * LANES] = frames[
                        j * kb : (j + 1) * kb, t * LANES : (t + 1) * LANES
                    ].astype(BF16)
        for k in range(ROW):
            turned = place[rows_of(i * ROW + k, coef), :]
            sums = lax.dot_general(frame[k], turned, NT, preferred_element_type=F32)
            weights = sums[2 * kb : 3 * kb]
            out_send[i * ROW + k] = jnp.concatenate(
                [
                    jnp.concatenate([sums[0:kb], sums[kb : 2 * kb]], axis=1),
                    jnp.concatenate([weights[: kb // 2], weights[kb // 2 :]], axis=1),
                ],
                axis=0,
            )
        for k in range(ROW):
            to = lax.rem(x + k, ROW)
            b = i * ROW + to

            @pl.when(b != me)
            def _():
                remote(out_send.at[b], mine_ref.at[me], o_ssem, o_rsem, at(to, zb * SIDE + i)).start()

    with jax.named_scope("class_rows"):
        each(0, SIDE, class_row)
    mine_ref[me] = out_send[me]
    out_size = (NP - 1) * out_send.shape[1]
    with jax.named_scope("take_out"):
        drain(o_rsem, out_size)
    swap = remote(mine_ref, other_ref, c_ssem, c_rsem, partner)
    swap.start()

    drain(g_ssem, (SIDE - 1) * (bundle_size + ROW * kb // 2) + SIDE * (ROW - 1) * (bundle_size + kb // 2))
    drain(lse_ssem, NP - 1)
    drain(o_ssem, out_size)

    @pl.when(owner < OWNERS)
    def _():
        drain(rs_ssem, (OWNERS - 1) * share_size)
        drain(ag_ssem, (nb - 1) * (ag_send.shape[0] + top_send.shape[0]))

    @pl.when(owner >= OWNERS)
    def _():
        drain(rs_ssem, OWNERS * share_size)

    with jax.named_scope("swap"):
        swap.wait()


def finish(mine_ref, other_ref, ev_ref, cs_ref, cw_ref, out_ref):
    coef, kb = cw_ref.shape[0], cs_ref.shape[0] // NP
    halves = []
    for b in range(NP):
        both = mine_ref[b] + other_ref[b]
        cs_ref[b * kb : (b + 1) * kb, :] = both[:kb]
        halves.append(both[kb:])
    for first in range(0, NP, NP // 2):
        turned = jnp.concatenate(halves[first : first + NP // 2], axis=0).T
        for k in range(NP // 2):
            lanes = slice(k * kb // 2, (k + 1) * kb // 2)
            to = (first + k) * kb
            cw_ref[:, to : to + kb // 2] = turned[:coef, lanes]
            cw_ref[:, to + kb // 2 : to + kb] = turned[coef:, lanes]
    out_ref[...] = ev_ref[:, : out_ref.shape[1]]


def body(nz, particles, classes, ctf, sigma2, shell_of, rot_table, ctf_group):
    count, coef = particles.shape[0], shell_of.shape[0]
    classes_n, rotations = classes.shape[0], rot_table.shape[0]
    nb = nz // SIDE
    kb = classes_n // NP
    half = rotations // 2
    pairs = half * kb
    piece = pairs // OWNERS * 2 // 3
    dma = pltpu.SemaphoreType.DMA
    regular = pltpu.SemaphoreType.REGULAR
    vmem = pltpu.VMEM
    i32 = jnp.int32
    arrays = (
        particles,
        classes,
        ctf,
        sigma2.reshape(1, -1),
        shell_of.reshape(1, -1),
        rot_table,
        ctf_group.reshape(1, -1),
    )
    mine, other, evidence = pl.pallas_call(
        functools.partial(kernel, nz),
        out_shape=[
            jax.ShapeDtypeStruct((NP, 24, LANES), F32),
            jax.ShapeDtypeStruct((NP, 24, LANES), F32),
            jax.ShapeDtypeStruct((1, LANES), F32),
        ],
        in_specs=[pl.BlockSpec(memory_space=pltpu.HBM)] * 7,
        out_specs=[pl.BlockSpec(memory_space=vmem)] * 3,
        scratch_shapes=[
            *[vmem(a.shape, a.dtype) for a in arrays[1:]],
            vmem((NP, count + half + 24, LANES), BF16),
            vmem((SIDE, ROW * kb, LANES), BF16),
            vmem((NP, kb, LANES), BF16),
            vmem((NP * coef, half * LANES), BF16),
            vmem((SIDE, ROW * 5 * LANES, 2 * LANES), BF16),
            vmem((NP, 2 * LANES, 3 * LANES), BF16),
            vmem((NP // 4, 8 * kb, 4 * coef), BF16),
            vmem((SIDE, pairs, ROW * 5 * LANES), BF16),
            vmem((pairs, 2 * LANES), F32),
            vmem((OWNERS, piece, LANES), i32),
            vmem((OWNERS, 4, LANES), F32),
            vmem((nb, piece, LANES), i32),
            vmem((nb, 4, LANES), F32),
            vmem((piece, LANES), i32),
            vmem((2, LANES), F32),
            vmem((OWNERS, piece, LANES), i32),
            vmem((OWNERS, 2, LANES), F32),
            vmem((1, LANES), F32),
            vmem((NP, 1, LANES), F32),
            vmem((pairs, 2 * LANES), BF16),
            vmem((ROW, 3 * kb, half * LANES), BF16),
            vmem((NP, 24, LANES), F32),
            vmem((1152, 1, LANES), F32),
            dma((len(arrays) + 1,)),
            dma,
            dma((SIDE,)),
            dma((NP,)),
            dma,
            dma((nb,)),
            dma,
            dma((OWNERS,)),
            dma((OWNERS,)),
            *[dma] * 6,
            regular((OWNERS,)),
        ],
        compiler_params=pltpu.CompilerParams(
            collective_id=0, has_side_effects=True, vmem_limit_bytes=40 * 1024 * 1024
        ),
        name="averaging",
    )(*[pltpu.with_memory_space_constraint(a, pltpu.HBM) for a in arrays])
    sums, weights, evidence = pl.pallas_call(
        finish,
        out_shape=[
            jax.ShapeDtypeStruct((classes_n, 2 * coef), F32),
            jax.ShapeDtypeStruct((coef, classes_n), F32),
            jax.ShapeDtypeStruct((1, count), F32),
        ],
        in_specs=[pl.BlockSpec(memory_space=vmem)] * 3,
        out_specs=[pl.BlockSpec(memory_space=vmem)] * 3,
        compiler_params=pltpu.CompilerParams(vmem_limit_bytes=4 * 1024 * 1024),
        name="finish",
    )(mine, other, evidence)
    return sums, weights.T, evidence.reshape(-1)


def solution(mesh):
    nz = mesh.shape["shell"] // ROW
    split = Mesh(mesh.devices.reshape(mesh.shape["groups"], ROW, nz, mesh.shape["batch"]), AXES)
    shell = ("x", "z")
    placed = (
        P(("groups", "batch"), shell),
        P("groups", shell),
        P("groups", shell),
        P("groups"),
        P(shell),
        P(None, shell),
        P(("groups", "batch")),
    )
    return jax.shard_map(
        functools.partial(body, nz),
        mesh=split,
        in_specs=placed,
        out_specs=(P("groups", shell), P("groups", shell), P(("groups", "batch"))),
        check_vma=False,
    )
```

```python
import functools

import jax
import jax.numpy as jnp
from jax import lax
from jax.experimental import pallas as pl
from jax.experimental.pallas import tpu as pltpu
from jax.sharding import Mesh
from jax.sharding import PartitionSpec as P

MESH = pl.DeviceIdType.MESH
ROW = 4
SIDE = 4
NP = ROW * SIDE
OWNERS = 4
LANES = 128
F32 = jnp.float32
BF16 = jnp.bfloat16
NT = (((1,), (1,)), ((), ()))
AXES = ("groups", "x", "z", "batch")


def lane(shape):
    return lax.broadcasted_iota(jnp.int32, shape, 1)


def compact(w):
    free = lane((8, LANES)) >= 80
    kept = []
    for r in range(0, w.shape[0], 48):
        a, b = w[r + 32 : r + 40], w[r + 40 : r + 48]
        kept += [
            jnp.where(free, pltpu.roll(a, 80, 1), w[r : r + 8]),
            jnp.where(free, pltpu.roll(a, 32, 1), w[r + 8 : r + 16]),
            jnp.where(free, pltpu.roll(b, 80, 1), w[r + 16 : r + 24]),
            jnp.where(free, pltpu.roll(b, 32, 1), w[r + 24 : r + 32]),
        ]
    return jnp.concatenate(kept, axis=0)


def expand(w):
    first = lane((8, LANES)) < 48
    whole = []
    for r in range(0, w.shape[0], 32):
        part = w[r : r + 32]
        whole += [
            part,
            jnp.where(first, pltpu.roll(part[0:8], 48, 1), pltpu.roll(part[8:16], 96, 1)),
            jnp.where(first, pltpu.roll(part[16:24], 48, 1), pltpu.roll(part[24:32], 96, 1)),
        ]
    return jnp.concatenate(whole, axis=0)


def spread(row):
    free = lane((1, LANES)) >= 80
    return jnp.where(free, pltpu.roll(row, 80, 1), row), jnp.where(free, pltpu.roll(row, 32, 1), row)


def tiles(even, odd, rows):
    e = jnp.broadcast_to(even, (8, LANES))
    o = jnp.broadcast_to(odd, (8, LANES))
    return jnp.concatenate([e, o] * (rows // 16), axis=0)


def over_rows(values, combine, reduce):
    split = [values[r : r + 8] for r in range(0, values.shape[0], 8)]
    even = reduce(functools.reduce(combine, split[0::2]), axis=0, keepdims=True)
    odd = reduce(functools.reduce(combine, split[1::2]), axis=0, keepdims=True)
    first = lane((1, LANES)) < 48
    moved = jnp.where(first, pltpu.roll(even, 48, 1), pltpu.roll(odd, 96, 1))
    return combine(combine(even, odd), moved)


def kernel(
    nz,
    part_hbm,
    cls_hbm,
    ctf_hbm,
    sig_hbm,
    sh_hbm,
    tab_hbm,
    grp_hbm,
    mine_ref,
    other_ref,
    ev_ref,
    cls_ref,
    ctf_ref,
    sig_ref,
    sh_ref,
    tab_ref,
    grp_ref,
    bundle,
    cls_z,
    cls_all,
    place,
    w_all,
    src_all,
    left,
    rot_all,
    score,
    rs_send,
    rs_scale,
    rs_recv,
    rs_rscale,
    ag_send,
    top_send,
    ag_recv,
    top_recv,
    lse_own,
    lse_all,
    post,
    frame,
    out_send,
    sizes,
    in_sem,
    g_ssem,
    z_rsem,
    x_rsem,
    rs_ssem,
    rs_rsem,
    ag_ssem,
    ag_rsem,
    top_rsem,
    lse_ssem,
    lse_rsem,
    o_ssem,
    o_rsem,
    c_ssem,
    c_rsem,
    column_in,
    others_in,
    owner_in,
    first_in,
    partner_in,
):
    nb = nz // SIDE
    count, coef = part_hbm.shape[0], ctf_ref.shape[1]
    kb = cls_all.shape[1]
    half = tab_ref.shape[0] // 2
    rows = half * kb // OWNERS
    group = lax.axis_index("groups")
    x = lax.axis_index("x")
    z = lax.axis_index("z")
    core = lax.axis_index("batch")
    zb, zi = z // SIDE, lax.rem(z, SIDE)
    me = zi * ROW + x
    def owns(b):
        return jnp.logical_or(
            jnp.logical_and(b >= 1, b < 3), jnp.logical_and(b >= nb - 3, b < nb - 1)
        )

    def home(o):
        return jnp.where(o < 2, o + 1, o + nb - 5)

    owner = jnp.where(owns(zb), jnp.where(zb < 3, zb - 1, zb - nb + 5), OWNERS)

    def greets(a, b):
        between = jnp.logical_and(jnp.logical_and(a >= 1, a < b), b < nb - 1)
        return jnp.logical_or(
            jnp.logical_and(between, jnp.logical_or(owns(a), owns(b))),
            jnp.logical_or(
                jnp.logical_and(b == 0, jnp.logical_and(a >= 1, a < 3)), jnp.logical_and(b == nb - 1, owns(a))
            ),
        )

    def at(x_, z_):
        return (group, x_, z_, core)

    def mate(k):
        i = lax.rem(me + k, NP)
        return i, at(lax.rem(i, ROW), zb * SIDE + i // ROW)

    def far(b):
        return at(x, b * SIDE + zi)

    partner = (group, x, z, 1 - core)

    def remote(src, dst, ssem, rsem, device):
        return pltpu.make_async_remote_copy(
            src_ref=src, dst_ref=dst, send_sem=ssem, recv_sem=rsem, device_id=device, device_id_type=MESH
        )

    def drain(semaphore, size):
        whole = sizes.at[0:size]
        remote(whole, whole, semaphore, semaphore, partner).wait_recv()

    def each(lower, upper, step):
        def turn(k, _):
            step(k)
            return 0

        lax.fori_loop(lower, upper, turn, 0)

    def tell(semaphore, device):
        pl.semaphore_signal(semaphore, inc=1, device_id=device, device_id_type=MESH)

    def rows_of(i, n):
        return pl.ds(pl.multiple_of(i * n, n), n)

    given = (ctf_hbm, sig_hbm, sh_hbm, tab_hbm, part_hbm, cls_hbm.at[rows_of(zi, ROW * kb)], cls_hbm, grp_hbm)
    taken = (ctf_ref, sig_ref, sh_ref, tab_ref, bundle.at[me, 0:count], cls_z.at[zi], cls_ref, grp_ref)
    loads = [pltpu.make_async_copy(a, b, in_sem.at[k]) for k, (a, b) in enumerate(zip(given, taken))]
    for load in loads:
        load.start()

    barrier = pltpu.get_barrier_semaphore()
    each(1, ROW, lambda k: tell(barrier, at(lax.rem(x + k, ROW), z)))
    each((zi + 1) * ROW, NP, lambda i: tell(barrier, at(lax.rem(i, ROW), zb * SIDE + i // ROW)))

    @pl.when(core > 0)
    def _():
        tell(barrier, partner)

    def greet(b):
        @pl.when(greets(zb, b))
        def _():
            tell(barrier, far(b))

    each(0, nb, greet)
    for load in loads[:4]:
        load.wait()

    levels = sig_ref.shape[1]
    pick = (lax.broadcasted_iota(jnp.int32, (levels, coef), 0) == sh_ref[...]).astype(F32)
    noise = jnp.dot(
        jnp.broadcast_to(sig_ref[...], (8, levels)), pick, precision=lax.Precision.HIGHEST, preferred_element_type=F32
    )
    ctf = ctf_ref[...]
    par = jnp.concatenate([ctf, (1.0 / noise[0:1]) * ctf], axis=1)
    par_high = par.astype(BF16).astype(F32)
    par_mid = (par - par_high).astype(BF16).astype(F32)
    offset = (x * nz + z) * coef
    table = (tab_ref[...] - offset).astype(F32)
    table = jnp.concatenate([table[:half], table[half:]], axis=1)
    bundle[me, count:] = jnp.concatenate([table, par_high, par_mid, (par - par_high) - par_mid], axis=0).astype(BF16)
    for load in loads[4:]:
        load.wait()
    with jax.named_scope("barrier"):
        greeted = sum(jnp.where(greets(b, zb), 1, 0) for b in range(nb))
        pl.semaphore_wait(barrier, ROW - 1 + zi * ROW + jnp.where(core > 0, 0, 1) + greeted)

    def down(i):
        device = at(x, zb * SIDE + i)
        remote(bundle.at[me], bundle.at[me], g_ssem, z_rsem.at[zi], device).start()
        remote(cls_ref.at[rows_of(i, ROW * kb)], cls_z.at[zi], g_ssem, z_rsem.at[zi], device).start()

    def across(i):
        b = i * ROW + x
        for k in range(1, ROW):
            to = lax.rem(x + k, ROW)
            device = at(to, z)
            remote(bundle.at[b], bundle.at[b], g_ssem, x_rsem.at[b], device).start()
            remote(cls_z.at[i, rows_of(to, kb)], cls_all.at[b], g_ssem, x_rsem.at[b], device).start()

    bundle_size = bundle.shape[1] // 2
    def tell_above(i):
        tell(column_in.at[zi], at(x, zb * SIDE + i))
        each(1, ROW, lambda k: tell(others_in, at(lax.rem(x + k, ROW), zb * SIDE + i)))

    each(0, zi, tell_above)
    each(0, zi, lambda k: down(zi - 1 - k))
    across(zi)

    @pl.when(owner < OWNERS)
    def _():
        def tell_earlier(b):
            @pl.when(greets(b, zb))
            def _():
                tell(owner_in.at[owner], far(b))

        each(0, nb, tell_earlier)

    @pl.when(zb == 0)
    def _():
        tell(first_in, far(1))

    @pl.when(core == 0)
    def _():
        tell(partner_in, partner)

    with jax.named_scope("zeros"):
        w_all[...] = jnp.zeros_like(w_all)
        src_all[...] = jnp.zeros_like(src_all)
        left[...] = jnp.zeros_like(left)
    score[...] = jnp.zeros_like(score)
    cls_all[me] = cls_z[zi, rows_of(x, kb), :]
    member = jnp.broadcast_to(grp_ref[...].astype(F32), (LANES, count)).T
    low = lane((count, LANES)) < coef
    low_kb = lane((kb, LANES)) < coef

    def pass_on(i):
        with jax.named_scope("came_down"):
            drain(z_rsem.at[i], bundle_size + ROW * kb // 2)
        across(i)
        cls_all[i * ROW + x] = cls_z[i, rows_of(x, kb), :]

    def amplitudes(tail):
        par = tail[half : half + 8] + tail[half + 8 : half + 16] + tail[half + 16 : half + 24]
        sel = jnp.broadcast_to(par[0:1], (count, LANES))
        for g in range(1, par.shape[0]):
            sel = jnp.where(member == g, par[g : g + 1], sel)
        other = pltpu.roll(sel, coef, 1)
        return jnp.where(low, sel, other), jnp.where(low, other, sel)

    def turned_over(a):
        return jnp.concatenate([a, jnp.zeros((LANES - count, LANES), F32)], axis=0).astype(BF16).T

    def prepare(g, i):
        b = g * ROW + i
        landing = bundle[b, count:].astype(F32)
        amp, wamp = amplitudes(landing)
        weighted = turned_over(wamp * bundle[b, 0:count].astype(F32))
        pen = -0.5 * (wamp * amp)
        pen_hi = pen.astype(BF16).astype(F32)
        pen = turned_over(jnp.where(low, pen_hi, pen - pen_hi))
        for k, piece in enumerate((weighted[:coef], weighted[coef:], pen[:coef], pen[:coef], pen[coef:])):
            for s in range(2):
                top = pl.multiple_of((5 * b + k) * LANES + s * coef, coef)
                w_all[pl.ds(top, coef), s * LANES : (s + 1) * LANES] = piece
        index = lax.broadcasted_iota(jnp.int32, (coef, LANES), 0).astype(F32).astype(BF16)
        ones, zeros = jnp.ones((coef, LANES), BF16), jnp.zeros((coef, LANES), BF16)
        for j in range(half):
            row = jnp.broadcast_to(landing[j : j + 1], (16, LANES)).astype(BF16)
            row = jnp.concatenate([row] * (coef // 16), axis=0)
            place[rows_of(b, coef), j * LANES : (j + 1) * LANES] = jnp.where(index == row, ones, zeros)

    def prepare_sources(b):
        amp, _ = amplitudes(bundle[b, count:].astype(F32))
        source = amp * bundle[b, 0:count].astype(F32)
        source_turned = pltpu.roll(source, coef, 1)
        power = amp * amp
        for s in range(2):
            top = s * LANES

            def keep(lower, upper):
                return (jnp.where(low, lower, 0.0) if s == 0 else jnp.where(low, 0.0, upper)).astype(BF16)

            src_all[b, top : top + count, 0:128] = keep(source, source_turned)
            src_all[b, top : top + count, 128:256] = keep(source_turned, source)
            src_all[b, top : top + count, 256:384] = keep(power, power)

    def rotate(g):
        for i in range(4):
            image = cls_all[g * 4 + i].astype(F32)
            turned = pltpu.roll(image, coef, 1)
            if i % 2 == 0:
                re, im = jnp.where(low_kb, image, 0.0), jnp.where(low_kb, turned, 0.0)
            else:
                re, im = jnp.where(low_kb, 0.0, turned), jnp.where(low_kb, 0.0, image)
            top = (i // 2) * LANES
            left[g, 2 * i * kb : (2 * i + 1) * kb, top : top + LANES] = re.astype(BF16)
            left[g, (2 * i + 1) * kb : (2 * i + 2) * kb, top : top + LANES] = im.astype(BF16)
        lhs = left[g]
        for jj in range(half // 2):
            turned = jnp.dot(
                lhs, place[g * 4 * coef : (g + 1) * 4 * coef, jj * 256 : (jj + 1) * 256], preferred_element_type=F32
            )
            for i in range(4):
                for t in range(2):
                    j = jj * 2 + t
                    re = turned[2 * i * kb : (2 * i + 1) * kb, t * LANES : (t + 1) * LANES]
                    im = turned[(2 * i + 1) * kb : (2 * i + 2) * kb, t * LANES : (t + 1) * LANES]
                    power = re * re + im * im
                    power_hi = power.astype(BF16)
                    power_lo = (power - power_hi.astype(F32)).astype(BF16)
                    to = slice(j * kb, (j + 1) * kb)
                    pieces = re.astype(BF16), im.astype(BF16), power_hi, power_lo, power_hi
                    for k, piece in enumerate(pieces):
                        at_lane = (5 * (g * ROW + i) + k) * LANES
                        rot_all[to, at_lane : at_lane + LANES] = piece

    def score_rows(rows_in):
        with jax.named_scope("arrive"):
            for g in rows_in:
                each(1, ROW, lambda k: drain(x_rsem.at[g * ROW + lax.rem(x + k, ROW)], bundle_size + kb // 2))
        with jax.named_scope("scores"):
            for g in rows_in:
                for k in range(1, ROW):
                    prepare(g, lax.rem(x + k, ROW))
            for g in rows_in:
                rotate(g)
            depth = slice(rows_in[0] * ROW * 5 * LANES, (rows_in[-1] + 1) * ROW * 5 * LANES)
            score[...] += jnp.dot(rot_all[:, depth], w_all[depth, :], preferred_element_type=F32)

    prepare(zi, x)

    def down_later(i):
        pl.semaphore_wait(column_in.at[i], 1)
        down(i)

    with jax.named_scope("down_later"):
        each(zi + 1, SIDE, down_later)
    nearest = (1, 0, 1, 2), (2, 2, 0, 1), (3, 3, 3, 0)
    for step in nearest:
        i = sum(jnp.where(zi == k, step[k], 0) for k in range(SIDE))
        pass_on(i)
        prepare(i, x)

    def half_of_rows(step):
        first = (zi == SIDE - 1) == (step == 0)

        @pl.when(first)
        def _():
            score_rows([SIDE - 1])

        @pl.when(jnp.logical_not(first))
        def _():
            score_rows(list(range(SIDE - 1)))

    each(0, 2, half_of_rows)

    def share(o):
        return score[rows_of(o, rows), :]

    share_size = rs_send.shape[1] + rs_scale.shape[1]
    for o in (1, 2, 0, 3):

        @pl.when(owner != o)
        def _():
            piece = share(o)
            one, two = piece[:, :LANES], piece[:, LANES:]
            most = jnp.max(jnp.maximum(one, two), axis=0, keepdims=True)
            least = jnp.min(jnp.minimum(one, two), axis=0, keepdims=True)
            middle = 0.5 * (most + least)
            reach = jnp.maximum(0.5 * (most - least), 1e-30)
            fit = 32767.0 / reach
            one = jnp.round((one - middle) * fit).astype(jnp.int32)
            two = jnp.round((two - middle) * fit).astype(jnp.int32)
            rs_send[o] = compact((one & 0xFFFF) | (two << 16))
            rs_scale[o] = jnp.concatenate([*spread(reach * (1.0 / 32767.0)), *spread(middle)], axis=0)

            @pl.when(jnp.logical_not(greets(home(o), zb)))
            def _():
                with jax.named_scope("owner_in"):
                    pl.semaphore_wait(owner_in.at[o], 1)

            with jax.named_scope("share_go"):
                remote(rs_send.at[o], rs_recv.at[zb], rs_ssem, rs_rsem.at[zb], far(home(o))).start()
                remote(rs_scale.at[o], rs_rscale.at[zb], rs_ssem, rs_rsem.at[zb], far(home(o))).start()

    @pl.when(zb == 1)
    def _():
        pl.semaphore_wait(first_in, 1)
        tell(owner_in.at[2], far(0))
        tell(owner_in.at[3], far(0))

    with jax.named_scope("sources"):
        each(0, NP, prepare_sources)

    urgent = jnp.where(zb < nb // 2, nb, nb - 2)

    def send_post(b):
        @pl.when(b != zb)
        def _():
            remote(ag_send, ag_recv.at[owner], ag_ssem, ag_rsem.at[owner], far(b)).start()

    @pl.when(owner < OWNERS)
    def _():
        own = share(owner)
        total = compact(own[:, :LANES]), compact(own[:, LANES:])

        def add_share(k, so_far):
            b = jnp.where(k < zb, k, k + 1)
            with jax.named_scope("share_in"):
                drain(rs_rsem.at[b], share_size)
            word = rs_recv[b]
            step = tiles(rs_rscale[b, 0:1], rs_rscale[b, 1:2], word.shape[0])
            middle = tiles(rs_rscale[b, 2:3], rs_rscale[b, 3:4], word.shape[0])
            return (
                so_far[0] + (((word << 16) >> 16).astype(F32) * step + middle),
                so_far[1] + ((word >> 16).astype(F32) * step + middle),
            )

        total_one, total_two = lax.fori_loop(0, nb - 1, add_share, total)
        peak = over_rows(jnp.maximum(total_one, total_two), jnp.maximum, jnp.max)
        shift = tiles(*spread(peak), total_one.shape[0])
        exp_one, exp_two = jnp.exp(total_one - shift), jnp.exp(total_two - shift)
        evidence = peak + jnp.log(over_rows(exp_one + exp_two, jnp.add, jnp.sum))
        top_send[...] = jnp.concatenate([peak, evidence], axis=0)

        def send_top(b):
            @pl.when(b != zb)
            def _():
                remote(top_send, top_recv.at[owner], ag_ssem, top_rsem.at[owner], far(b)).start()

        each(0, nb, send_top)
        one = (exp_one * 65535.0 + 0.5).astype(jnp.int32)
        two = (exp_two * 65535.0 + 0.5).astype(jnp.int32)
        ag_send[...] = (one & 0xFFFF) | (two << 16)

        each(0, urgent, send_post)
        ag_recv[owner] = ag_send[...]
        top_recv[owner] = top_send[...]

    def take_top(o):
        @pl.when(o != owner)
        def _():
            with jax.named_scope("top_in"):
                drain(top_rsem.at[o], top_send.shape[0])

    each(0, OWNERS, take_top)

    def merged(parts):
        most = functools.reduce(jnp.maximum, parts)
        return most + jnp.log(functools.reduce(jnp.add, [jnp.exp(e - most) for e in parts]))

    evidence = merged([top_recv[o, 1:2] for o in range(OWNERS)])
    lse_own[...] = evidence

    @pl.when(zi < SIDE - 1)
    def _():
        pl.semaphore_wait(others_in, (SIDE - 1 - zi) * (ROW - 1))

    each(1, NP, lambda k: remote(lse_own, lse_all.at[me], lse_ssem, lse_rsem, mate(k)[1]).start())
    lse_all[me] = evidence

    @pl.when(owner < OWNERS)
    def _():
        each(urgent, nb, send_post)

    with jax.named_scope("lse_in"):
        drain(lse_rsem, NP - 1)
    everyone = lse_all[...]
    most = jnp.max(everyone, axis=0)
    evidence = most + jnp.log(jnp.sum(jnp.exp(everyone - most[None]), axis=0))
    ev_ref[...] = evidence
    used = lane((rows, LANES)) < count

    def take_post(o):
        @pl.when(o != owner)
        def _():
            with jax.named_scope("post_in"):
                drain(ag_rsem.at[o], ag_send.shape[0])

        word = expand(ag_recv[o])
        scale = jnp.exp(top_recv[o, 0:1] - evidence) * (1.0 / 65535.0)
        one = jnp.where(used, (word & 0xFFFF).astype(F32) * scale, 0.0)
        two = jnp.where(used, lax.shift_right_logical(word, 16).astype(F32) * scale, 0.0)
        post[rows_of(o, rows), 0:128] = one.astype(BF16)
        post[rows_of(o, rows), 128:256] = two.astype(BF16)

    each(0, OWNERS, take_post)

    def class_row(i):
        for k in range(ROW):
            frames = jnp.dot(post[...], src_all[i * ROW + k], preferred_element_type=F32)
            for j in range(half):
                for t in range(3):
                    frame[k, t * kb : (t + 1) * kb, j * LANES : (j + 1) * LANES] = frames[
                        j * kb : (j + 1) * kb, t * LANES : (t + 1) * LANES
                    ].astype(BF16)
        for k in range(ROW):
            turned = place[rows_of(i * ROW + k, coef), :]
            sums = lax.dot_general(frame[k], turned, NT, preferred_element_type=F32)
            weights = sums[2 * kb : 3 * kb]
            out_send[i * ROW + k] = jnp.concatenate(
                [
                    jnp.concatenate([sums[0:kb], sums[kb : 2 * kb]], axis=1),
                    jnp.concatenate([weights[: kb // 2], weights[kb // 2 :]], axis=1),
                ],
                axis=0,
            )
        for k in range(ROW):
            to = lax.rem(x + k, ROW)
            b = i * ROW + to

            @pl.when(b != me)
            def _():
                remote(out_send.at[b], mine_ref.at[me], o_ssem, o_rsem, at(to, zb * SIDE + i)).start()

    with jax.named_scope("class_rows"):
        each(0, SIDE, class_row)
    mine_ref[me] = out_send[me]
    out_size = (NP - 1) * out_send.shape[1]
    with jax.named_scope("take_out"):
        drain(o_rsem, out_size)

    @pl.when(core > 0)
    def _():
        pl.semaphore_wait(partner_in, 1)

    swap = remote(mine_ref, other_ref, c_ssem, c_rsem, partner)
    swap.start()

    drain(g_ssem, (SIDE - 1) * (bundle_size + ROW * kb // 2) + SIDE * (ROW - 1) * (bundle_size + kb // 2))
    drain(lse_ssem, NP - 1)
    drain(o_ssem, out_size)

    @pl.when(owner < OWNERS)
    def _():
        drain(rs_ssem, (OWNERS - 1) * share_size)
        drain(ag_ssem, (nb - 1) * (ag_send.shape[0] + top_send.shape[0]))

    @pl.when(owner >= OWNERS)
    def _():
        drain(rs_ssem, OWNERS * share_size)

    with jax.named_scope("swap"):
        swap.wait()


def finish(mine_ref, other_ref, ev_ref, cs_ref, cw_ref, out_ref):
    coef, kb = cw_ref.shape[0], cs_ref.shape[0] // NP
    halves = []
    for b in range(NP):
        both = mine_ref[b] + other_ref[b]
        cs_ref[b * kb : (b + 1) * kb, :] = both[:kb]
        halves.append(both[kb:])
    for first in range(0, NP, NP // 2):
        turned = jnp.concatenate(halves[first : first + NP // 2], axis=0).T
        for k in range(NP // 2):
            lanes = slice(k * kb // 2, (k + 1) * kb // 2)
            to = (first + k) * kb
            cw_ref[:, to : to + kb // 2] = turned[:coef, lanes]
            cw_ref[:, to + kb // 2 : to + kb] = turned[coef:, lanes]
    out_ref[...] = ev_ref[:, : out_ref.shape[1]]


def body(nz, particles, classes, ctf, sigma2, shell_of, rot_table, ctf_group):
    count, coef = particles.shape[0], shell_of.shape[0]
    classes_n, rotations = classes.shape[0], rot_table.shape[0]
    nb = nz // SIDE
    kb = classes_n // NP
    half = rotations // 2
    pairs = half * kb
    piece = pairs // OWNERS * 2 // 3
    dma = pltpu.SemaphoreType.DMA
    regular = pltpu.SemaphoreType.REGULAR
    vmem = pltpu.VMEM
    i32 = jnp.int32
    arrays = (
        particles,
        classes,
        ctf,
        sigma2.reshape(1, -1),
        shell_of.reshape(1, -1),
        rot_table,
        ctf_group.reshape(1, -1),
    )
    mine, other, evidence = pl.pallas_call(
        functools.partial(kernel, nz),
        out_shape=[
            jax.ShapeDtypeStruct((NP, 24, LANES), F32),
            jax.ShapeDtypeStruct((NP, 24, LANES), F32),
            jax.ShapeDtypeStruct((1, LANES), F32),
        ],
        in_specs=[pl.BlockSpec(memory_space=pltpu.HBM)] * 7,
        out_specs=[pl.BlockSpec(memory_space=vmem)] * 3,
        scratch_shapes=[
            *[vmem(a.shape, a.dtype) for a in arrays[1:]],
            vmem((NP, count + half + 24, LANES), BF16),
            vmem((SIDE, ROW * kb, LANES), BF16),
            vmem((NP, kb, LANES), BF16),
            vmem((NP * coef, half * LANES), BF16),
            vmem((NP * 5 * LANES, 2 * LANES), BF16),
            vmem((NP, 2 * LANES, 3 * LANES), BF16),
            vmem((NP // 4, 8 * kb, 4 * coef), BF16),
            vmem((pairs, NP * 5 * LANES), BF16),
            vmem((pairs, 2 * LANES), F32),
            vmem((OWNERS, piece, LANES), i32),
            vmem((OWNERS, 4, LANES), F32),
            vmem((nb, piece, LANES), i32),
            vmem((nb, 4, LANES), F32),
            vmem((piece, LANES), i32),
            vmem((2, LANES), F32),
            vmem((OWNERS, piece, LANES), i32),
            vmem((OWNERS, 2, LANES), F32),
            vmem((1, LANES), F32),
            vmem((NP, 1, LANES), F32),
            vmem((pairs, 2 * LANES), BF16),
            vmem((ROW, 3 * kb, half * LANES), BF16),
            vmem((NP, 24, LANES), F32),
            vmem((1152, 1, LANES), F32),
            dma((len(arrays) + 1,)),
            dma,
            dma((SIDE,)),
            dma((NP,)),
            dma,
            dma((nb,)),
            dma,
            dma((OWNERS,)),
            dma((OWNERS,)),
            *[dma] * 6,
            regular((SIDE,)),
            regular,
            regular((OWNERS,)),
            regular,
            regular,
        ],
        compiler_params=pltpu.CompilerParams(
            collective_id=0, has_side_effects=True, vmem_limit_bytes=40 * 1024 * 1024
        ),
        name="averaging",
    )(*[pltpu.with_memory_space_constraint(a, pltpu.HBM) for a in arrays])
    sums, weights, evidence = pl.pallas_call(
        finish,
        out_shape=[
            jax.ShapeDtypeStruct((classes_n, 2 * coef), F32),
            jax.ShapeDtypeStruct((coef, classes_n), F32),
            jax.ShapeDtypeStruct((1, count), F32),
        ],
        in_specs=[pl.BlockSpec(memory_space=vmem)] * 3,
        out_specs=[pl.BlockSpec(memory_space=vmem)] * 3,
        compiler_params=pltpu.CompilerParams(vmem_limit_bytes=4 * 1024 * 1024),
        name="finish",
    )(mine, other, evidence)
    return sums, weights.T, evidence.reshape(-1)


def solution(mesh):
    nz = mesh.shape["shell"] // ROW
    split = Mesh(mesh.devices.reshape(mesh.shape["groups"], ROW, nz, mesh.shape["batch"]), AXES)
    shell = ("x", "z")
    placed = (
        P(("groups", "batch"), shell),
        P("groups", shell),
        P("groups", shell),
        P("groups"),
        P(shell),
        P(None, shell),
        P(("groups", "batch")),
    )
    return jax.shard_map(
        functools.partial(body, nz),
        mesh=split,
        in_specs=placed,
        out_specs=(P("groups", shell), P("groups", shell), P(("groups", "batch"))),
        check_vma=False,
    )
```

```python
import functools

import jax
import jax.numpy as jnp
from jax import lax
from jax.experimental import pallas as pl
from jax.experimental.pallas import tpu as pltpu
from jax.sharding import Mesh
from jax.sharding import PartitionSpec as P

MESH = pl.DeviceIdType.MESH
ROW = 4
SIDE = 4
NP = ROW * SIDE
OWNERS = 4
LANES = 128
F32 = jnp.float32
BF16 = jnp.bfloat16
NT = (((1,), (1,)), ((), ()))
AXES = ("groups", "x", "z", "batch")


def lane(shape):
    return lax.broadcasted_iota(jnp.int32, shape, 1)


def compact(w):
    free = lane((8, LANES)) >= 80
    kept = []
    for r in range(0, w.shape[0], 48):
        a, b = w[r + 32 : r + 40], w[r + 40 : r + 48]
        kept += [
            jnp.where(free, pltpu.roll(a, 80, 1), w[r : r + 8]),
            jnp.where(free, pltpu.roll(a, 32, 1), w[r + 8 : r + 16]),
            jnp.where(free, pltpu.roll(b, 80, 1), w[r + 16 : r + 24]),
            jnp.where(free, pltpu.roll(b, 32, 1), w[r + 24 : r + 32]),
        ]
    return jnp.concatenate(kept, axis=0)


def expand(w):
    first = lane((8, LANES)) < 48
    whole = []
    for r in range(0, w.shape[0], 32):
        part = w[r : r + 32]
        whole += [
            part,
            jnp.where(first, pltpu.roll(part[0:8], 48, 1), pltpu.roll(part[8:16], 96, 1)),
            jnp.where(first, pltpu.roll(part[16:24], 48, 1), pltpu.roll(part[24:32], 96, 1)),
        ]
    return jnp.concatenate(whole, axis=0)


def spread(row):
    free = lane((1, LANES)) >= 80
    return jnp.where(free, pltpu.roll(row, 80, 1), row), jnp.where(free, pltpu.roll(row, 32, 1), row)


def tiles(even, odd, rows):
    e = jnp.broadcast_to(even, (8, LANES))
    o = jnp.broadcast_to(odd, (8, LANES))
    return jnp.concatenate([e, o] * (rows // 16), axis=0)


def over_rows(values, combine, reduce):
    split = [values[r : r + 8] for r in range(0, values.shape[0], 8)]
    even = reduce(functools.reduce(combine, split[0::2]), axis=0, keepdims=True)
    odd = reduce(functools.reduce(combine, split[1::2]), axis=0, keepdims=True)
    first = lane((1, LANES)) < 48
    moved = jnp.where(first, pltpu.roll(even, 48, 1), pltpu.roll(odd, 96, 1))
    return combine(combine(even, odd), moved)


def kernel(
    nz,
    part_hbm,
    cls_hbm,
    ctf_hbm,
    sig_hbm,
    sh_hbm,
    tab_hbm,
    grp_hbm,
    mine_ref,
    other_ref,
    ev_ref,
    cls_ref,
    ctf_ref,
    sig_ref,
    sh_ref,
    tab_ref,
    grp_ref,
    bundle,
    cls_z,
    cls_all,
    place,
    place_turned,
    w_all,
    src_all,
    left,
    rot_all,
    score,
    rs_send,
    rs_scale,
    rs_recv,
    rs_rscale,
    ag_send,
    top_send,
    ag_recv,
    top_recv,
    lse_send,
    lse_first,
    lse_own,
    lse_all,
    post,
    frame,
    out_send,
    sizes,
    in_sem,
    g_ssem,
    z_rsem,
    x_rsem,
    rs_ssem,
    rs_rsem,
    ag_ssem,
    pass_ssem,
    ag_rsem,
    top_rsem,
    first_rsem,
    lse_ssem,
    lse_rsem,
    o_ssem,
    o_rsem,
    c_ssem,
    c_rsem,
    column_in,
    others_in,
    owner_in,
    first_in,
    partner_in,
):
    nb = nz // SIDE
    count, coef = part_hbm.shape[0], ctf_ref.shape[1]
    kb = cls_all.shape[1]
    half = tab_ref.shape[0] // 2
    rows = half * kb // OWNERS
    group = lax.axis_index("groups")
    x = lax.axis_index("x")
    z = lax.axis_index("z")
    core = lax.axis_index("batch")
    zb, zi = z // SIDE, lax.rem(z, SIDE)
    me = zi * ROW + x
    def owns(b):
        return jnp.logical_or(
            jnp.logical_and(b >= 1, b < 3), jnp.logical_and(b >= nb - 3, b < nb - 1)
        )

    def home(o):
        return jnp.where(o < 2, o + 1, o + nb - 5)

    owner = jnp.where(owns(zb), jnp.where(zb < 3, zb - 1, zb - nb + 5), OWNERS)

    def greets(a, b):
        between = jnp.logical_and(jnp.logical_and(a >= 1, a < b), b < nb - 1)
        return jnp.logical_or(
            jnp.logical_and(between, jnp.logical_or(owns(a), owns(b))),
            jnp.logical_or(
                jnp.logical_and(b == 0, jnp.logical_and(a >= 1, a < 3)), jnp.logical_and(b == nb - 1, owns(a))
            ),
        )

    def at(x_, z_):
        return (group, x_, z_, core)

    def mate(k):
        i = lax.rem(me + k, NP)
        return i, at(lax.rem(i, ROW), zb * SIDE + i // ROW)

    def far(b):
        return at(x, b * SIDE + zi)

    partner = (group, x, z, 1 - core)

    def remote(src, dst, ssem, rsem, device):
        return pltpu.make_async_remote_copy(
            src_ref=src, dst_ref=dst, send_sem=ssem, recv_sem=rsem, device_id=device, device_id_type=MESH
        )

    def drain(semaphore, size):
        whole = sizes.at[0:size]
        remote(whole, whole, semaphore, semaphore, partner).wait_recv()

    def each(lower, upper, step):
        def turn(k, _):
            step(k)
            return 0

        lax.fori_loop(lower, upper, turn, 0)

    def tell(semaphore, device):
        pl.semaphore_signal(semaphore, inc=1, device_id=device, device_id_type=MESH)

    def rows_of(i, n):
        return pl.ds(pl.multiple_of(i * n, n), n)

    given = (ctf_hbm, sig_hbm, sh_hbm, tab_hbm, part_hbm, cls_hbm.at[rows_of(zi, ROW * kb)], cls_hbm, grp_hbm)
    taken = (ctf_ref, sig_ref, sh_ref, tab_ref, bundle.at[me, 0:count], cls_z.at[zi], cls_ref, grp_ref)
    loads = [pltpu.make_async_copy(a, b, in_sem.at[k]) for k, (a, b) in enumerate(zip(given, taken))]
    for load in loads:
        load.start()

    barrier = pltpu.get_barrier_semaphore()
    each(1, ROW, lambda k: tell(barrier, at(lax.rem(x + k, ROW), z)))
    each((zi + 1) * ROW, NP, lambda i: tell(barrier, at(lax.rem(i, ROW), zb * SIDE + i // ROW)))

    @pl.when(core > 0)
    def _():
        tell(barrier, partner)

    def greet(b):
        @pl.when(greets(zb, b))
        def _():
            tell(barrier, far(b))

    each(0, nb, greet)
    for load in loads[:4]:
        load.wait()

    levels = sig_ref.shape[1]
    pick = lax.broadcasted_iota(jnp.int32, (levels, coef), 0) == sh_ref[...]
    noise_of = jnp.broadcast_to(sig_ref[...], (coef, levels)).T
    noise = jnp.sum(jnp.where(pick, noise_of, 0.0), axis=0, keepdims=True)
    ctf = ctf_ref[...]
    par = jnp.concatenate([ctf, (1.0 / noise) * ctf], axis=1)
    par_high = par.astype(BF16).astype(F32)
    par_mid = (par - par_high).astype(BF16).astype(F32)
    offset = (x * nz + z) * coef
    table = (tab_ref[...] - offset).astype(F32)
    table = jnp.concatenate([table[:half], table[half:]], axis=1)
    bundle[me, count:] = jnp.concatenate([table, par_high, par_mid, (par - par_high) - par_mid], axis=0).astype(BF16)
    for load in loads[4:]:
        load.wait()
    with jax.named_scope("barrier"):
        greeted = sum(jnp.where(greets(b, zb), 1, 0) for b in range(nb))
        pl.semaphore_wait(barrier, ROW - 1 + zi * ROW + jnp.where(core > 0, 0, 1) + greeted)

    def down(i):
        device = at(x, zb * SIDE + i)
        remote(bundle.at[me], bundle.at[me], g_ssem, z_rsem.at[zi], device).start()
        remote(cls_ref.at[rows_of(i, ROW * kb)], cls_z.at[zi], g_ssem, z_rsem.at[zi], device).start()

    def across(i):
        b = i * ROW + x
        for k in range(1, ROW):
            to = lax.rem(x + k, ROW)
            device = at(to, z)
            remote(bundle.at[b], bundle.at[b], g_ssem, x_rsem.at[i], device).start()
            remote(cls_z.at[i, rows_of(to, kb)], cls_all.at[b], g_ssem, x_rsem.at[i], device).start()

    bundle_size = bundle.shape[1] // 2
    def tell_above(i):
        tell(column_in.at[zi], at(x, zb * SIDE + i))
        each(1, ROW, lambda k: tell(others_in, at(lax.rem(x + k, ROW), zb * SIDE + i)))

    each(0, zi, tell_above)
    each(0, zi, lambda k: down(zi - 1 - k))
    across(zi)

    @pl.when(owner < OWNERS)
    def _():
        def tell_earlier(b):
            @pl.when(greets(b, zb))
            def _():
                tell(owner_in.at[owner], far(b))

        each(0, nb, tell_earlier)

    @pl.when(zb == 0)
    def _():
        tell(first_in, far(1))

    @pl.when(core == 0)
    def _():
        tell(partner_in, partner)

    with jax.named_scope("zeros"):
        w_all[...] = jnp.zeros_like(w_all)
        src_all[...] = jnp.zeros_like(src_all)
        left[...] = jnp.zeros_like(left)
    score[...] = jnp.zeros_like(score)
    cls_all[me] = cls_z[zi, rows_of(x, kb), :]
    member = jnp.broadcast_to(grp_ref[...].astype(F32), (LANES, count)).T
    low = lane((count, LANES)) < coef
    low_kb = lane((kb, LANES)) < coef

    def pass_on(i):
        with jax.named_scope("came_down"):
            drain(z_rsem.at[i], bundle_size + ROW * kb // 2)
        across(i)
        cls_all[i * ROW + x] = cls_z[i, rows_of(x, kb), :]

    def amplitudes(tail):
        par = tail[half : half + 8] + tail[half + 8 : half + 16] + tail[half + 16 : half + 24]
        sel = jnp.broadcast_to(par[0:1], (count, LANES))
        for g in range(1, par.shape[0]):
            sel = jnp.where(member == g, par[g : g + 1], sel)
        other = pltpu.roll(sel, coef, 1)
        return jnp.where(low, sel, other), jnp.where(low, other, sel)

    def turned_over(a):
        return jnp.concatenate([a, jnp.zeros((LANES - count, LANES), F32)], axis=0).astype(BF16).T

    def prepare(g, i):
        b = g * ROW + i
        landing = bundle[b, count:].astype(F32)
        amp, wamp = amplitudes(landing)
        weighted = turned_over(wamp * bundle[b, 0:count].astype(F32))
        pen = -0.5 * (wamp * amp)
        pen_hi = pen.astype(BF16).astype(F32)
        pen = turned_over(jnp.where(low, pen_hi, pen - pen_hi))
        for k, piece in enumerate((weighted[:coef], weighted[coef:], pen[:coef], pen[:coef], pen[coef:])):
            for s in range(2):
                top = pl.multiple_of((5 * i + k) * LANES + s * coef, coef)
                w_all[g, pl.ds(top, coef), s * LANES : (s + 1) * LANES] = piece
        index = lax.broadcasted_iota(jnp.int32, (coef, LANES), 0).astype(F32).astype(BF16)
        ones, zeros = jnp.ones((coef, LANES), BF16), jnp.zeros((coef, LANES), BF16)
        for j in range(half):
            row = jnp.broadcast_to(landing[j : j + 1], (16, LANES)).astype(BF16)
            row = jnp.concatenate([row] * (coef // 16), axis=0)
            place[rows_of(b, coef), j * LANES : (j + 1) * LANES] = jnp.where(index == row, ones, zeros)

    def prepare_sources(pair):
        for i in range(2):
            b = pair * 2 + i
            amp, _ = amplitudes(bundle[b, count:].astype(F32))
            source = amp * bundle[b, 0:count].astype(F32)
            source_turned = pltpu.roll(source, coef, 1)
            power = amp * amp
            for s in range(2):
                top = s * LANES

                def keep(lower, upper):
                    return (jnp.where(low, lower, 0.0) if s == 0 else jnp.where(low, 0.0, upper)).astype(BF16)

                for t, kept in (
                    (2 * i, keep(source, source_turned)),
                    (2 * i + 1, keep(source_turned, source)),
                    (4 + i, keep(power, power)),
                ):
                    src_all[pair, top : top + count, t * LANES : (t + 1) * LANES] = kept
        for j in range(half):
            lanes = slice(j * LANES, (j + 1) * LANES)
            place_turned[pair, lanes, :] = place[rows_of(pair, 2 * coef), lanes].T

    def rotate(g):
        for i in range(4):
            image = cls_all[g * 4 + i].astype(F32)
            turned = pltpu.roll(image, coef, 1)
            if i % 2 == 0:
                re, im = jnp.where(low_kb, image, 0.0), jnp.where(low_kb, turned, 0.0)
            else:
                re, im = jnp.where(low_kb, 0.0, turned), jnp.where(low_kb, 0.0, image)
            top = (i // 2) * LANES
            left[g, 2 * i * kb : (2 * i + 1) * kb, top : top + LANES] = re.astype(BF16)
            left[g, (2 * i + 1) * kb : (2 * i + 2) * kb, top : top + LANES] = im.astype(BF16)
        lhs = left[g]
        for jj in range(half // 2):
            turned = jnp.dot(
                lhs, place[rows_of(g, 4 * coef), jj * 256 : (jj + 1) * 256], preferred_element_type=F32
            )
            for i in range(4):
                for t in range(2):
                    j = jj * 2 + t
                    re = turned[2 * i * kb : (2 * i + 1) * kb, t * LANES : (t + 1) * LANES]
                    im = turned[(2 * i + 1) * kb : (2 * i + 2) * kb, t * LANES : (t + 1) * LANES]
                    power = re * re + im * im
                    power_hi = power.astype(BF16)
                    power_lo = (power - power_hi.astype(F32)).astype(BF16)
                    to = slice(j * kb, (j + 1) * kb)
                    pieces = re.astype(BF16), im.astype(BF16), power_hi, power_lo, power_hi
                    for k, piece in enumerate(pieces):
                        at_lane = (5 * i + k) * LANES
                        rot_all[g, to, at_lane : at_lane + LANES] = piece

    def score_row(g):
        with jax.named_scope("arrive"):
            drain(x_rsem.at[g], (ROW - 1) * (bundle_size + kb // 2))
        with jax.named_scope("scores"):
            for k in range(1, ROW):
                prepare(g, lax.rem(x + k, ROW))
            rotate(g)
            score[...] += jnp.dot(rot_all[g], w_all[g], preferred_element_type=F32)

    prepare(zi, x)

    def down_later(i):
        pl.semaphore_wait(column_in.at[i], 1)
        down(i)

    with jax.named_scope("down_later"):
        each(zi + 1, SIDE, down_later)

    nearest = (0, 1, 2, 3), (1, 0, 1, 2), (2, 2, 0, 1), (3, 3, 3, 0)

    def place_of(step):
        return sum(
            jnp.where(jnp.logical_and(step == t, zi == k), nearest[t][k], 0) for t in range(SIDE) for k in range(SIDE)
        )

    def turn_of(step):
        @pl.when(step == 1)
        def _():
            for t in range(1, SIDE):
                pass_on(place_of(t))
                prepare(place_of(t), x)

        score_row(place_of(step))

    each(0, SIDE, turn_of)

    @pl.when(zi < SIDE - 1)
    def _():
        pl.semaphore_wait(others_in, (SIDE - 1 - zi) * (ROW - 1))

    def share(o):
        return score[rows_of(o, rows), :]

    share_size = rs_send.shape[1] + rs_scale.shape[1]
    for o in (1, 2, 0, 3):

        @pl.when(owner != o)
        def _():
            piece = share(o)
            one, two = piece[:, :LANES], piece[:, LANES:]
            most = jnp.max(jnp.maximum(one, two), axis=0, keepdims=True)
            least = jnp.min(jnp.minimum(one, two), axis=0, keepdims=True)
            middle = 0.5 * (most + least)
            reach = jnp.maximum(0.5 * (most - least), 1e-30)
            fit = 32767.0 / reach
            one = jnp.round((one - middle) * fit).astype(jnp.int32)
            two = jnp.round((two - middle) * fit).astype(jnp.int32)
            rs_send[o] = compact((one & 0xFFFF) | (two << 16))
            rs_scale[o] = jnp.concatenate([*spread(reach * (1.0 / 32767.0)), *spread(middle)], axis=0)

            @pl.when(jnp.logical_not(greets(home(o), zb)))
            def _():
                with jax.named_scope("owner_in"):
                    pl.semaphore_wait(owner_in.at[o], 1)

            with jax.named_scope("share_go"):
                remote(rs_send.at[o], rs_recv.at[zb], rs_ssem, rs_rsem.at[zb], far(home(o))).start()
                remote(rs_scale.at[o], rs_rscale.at[zb], rs_ssem, rs_rsem.at[zb], far(home(o))).start()

    @pl.when(zb == 1)
    def _():
        pl.semaphore_wait(first_in, 1)
        tell(owner_in.at[2], far(0))
        tell(owner_in.at[3], far(0))

    with jax.named_scope("sources"):
        each(0, NP // 2, prepare_sources)

    later = zb >= nb // 2

    def send_post(b):
        @pl.when(b != zb)
        def _():
            remote(ag_send, ag_recv.at[owner], ag_ssem, ag_rsem.at[owner], far(b)).start()

    @pl.when(owner < OWNERS)
    def _():
        own = share(owner)
        total = compact(own[:, :LANES]), compact(own[:, LANES:])

        def add_share(k, so_far):
            b = jnp.where(k < zb, k, k + 1)
            with jax.named_scope("share_in"):
                drain(rs_rsem.at[b], share_size)
            word = rs_recv[b]
            step = tiles(rs_rscale[b, 0:1], rs_rscale[b, 1:2], word.shape[0])
            middle = tiles(rs_rscale[b, 2:3], rs_rscale[b, 3:4], word.shape[0])
            return (
                so_far[0] + (((word << 16) >> 16).astype(F32) * step + middle),
                so_far[1] + ((word >> 16).astype(F32) * step + middle),
            )

        total_one, total_two = lax.fori_loop(0, nb - 1, add_share, total)
        peak = over_rows(jnp.maximum(total_one, total_two), jnp.maximum, jnp.max)
        shift = tiles(*spread(peak), total_one.shape[0])
        exp_one, exp_two = jnp.exp(total_one - shift), jnp.exp(total_two - shift)
        evidence = peak + jnp.log(over_rows(exp_one + exp_two, jnp.add, jnp.sum))
        top_send[...] = jnp.concatenate([peak, evidence], axis=0)
        lse_send[...] = evidence

        each(
            0,
            NP,
            lambda k: remote(
                lse_send, lse_first.at[owner * NP + me], ag_ssem, first_rsem, at(lax.rem(k, ROW), k // ROW)
            ).start(),
        )

        def send_top(b):
            @pl.when(b != zb)
            def _():
                remote(top_send, top_recv.at[owner], ag_ssem, top_rsem, far(b)).start()

        each(0, nb, send_top)
        one = (exp_one * 65535.0 + 0.5).astype(jnp.int32)
        two = (exp_two * 65535.0 + 0.5).astype(jnp.int32)
        ag_send[...] = (one & 0xFFFF) | (two << 16)


        def send_early(b):
            @pl.when(jnp.logical_not(jnp.logical_and(later, b == 1)))
            def _():
                send_post(b)

        each(0, nb - 2, send_early)
        ag_recv[owner] = ag_send[...]
        top_recv[owner] = top_send[...]

    with jax.named_scope("top_in"):

        @pl.when(owner < OWNERS)
        def _():
            drain(top_rsem, (OWNERS - 1) * top_send.shape[0])

        @pl.when(owner >= OWNERS)
        def _():
            drain(top_rsem, OWNERS * top_send.shape[0])

    def merged(parts, axis):
        most = jnp.max(parts, axis=axis, keepdims=True)
        return most + jnp.log(jnp.sum(jnp.exp(parts - most), axis=axis, keepdims=True))

    @pl.when(jnp.logical_and(owner < OWNERS, later))
    def _():
        each(nb - 2, nb, send_post)

    def pass_post(o, b):
        with jax.named_scope("post_in"):
            drain(ag_rsem.at[o], ag_send.shape[0])
        remote(ag_recv.at[o], ag_recv.at[o], pass_ssem, ag_rsem.at[o], far(b)).start()

    @pl.when(zb == 0)
    def _():
        for o in range(OWNERS):
            pass_post(o, nb - 1 if o < OWNERS // 2 else 1)

    @pl.when(zb == 0)
    def _():
        with jax.named_scope("first_in"):
            drain(first_rsem, OWNERS * NP)
        ev_ref[...] = merged(lse_first[...], 0)[0]

    @pl.when(zb > 0)
    def _():
        lse_own[...] = merged(jnp.concatenate([top_recv[o, 1:2] for o in range(OWNERS)], axis=0), 0)
        each(1, NP, lambda k: remote(lse_own, lse_all.at[me], lse_ssem, lse_rsem, mate(k)[1]).start())
        lse_all[me] = lse_own[...]
        with jax.named_scope("lse_in"):
            drain(lse_rsem, NP - 1)
        drain(lse_ssem, NP - 1)
        ev_ref[...] = merged(lse_all[...], 0)[0]

    evidence = ev_ref[...]
    used = lane((rows, LANES)) < count

    def take_post(o):
        passes = jnp.logical_and(zb == nb - 1, o < OWNERS // 2)

        @pl.when(passes)
        def _():
            pass_post(o, nb - 2)

        @pl.when(jnp.logical_not(jnp.logical_or(passes, jnp.logical_or(o == owner, zb == 0))))
        def _():
            with jax.named_scope("post_in"):
                drain(ag_rsem.at[o], ag_send.shape[0])

        word = expand(ag_recv[o])
        scale = jnp.exp(top_recv[o, 0:1] - evidence) * (1.0 / 65535.0)
        one = jnp.where(used, (word & 0xFFFF).astype(F32) * scale, 0.0)
        two = jnp.where(used, lax.shift_right_logical(word, 16).astype(F32) * scale, 0.0)
        post[rows_of(o, rows), 0:128] = one.astype(BF16)
        post[rows_of(o, rows), 128:256] = two.astype(BF16)

    each(0, OWNERS, take_post)

    def class_row(i):
        pairs_in = [i * (ROW // 2) + k for k in range(ROW // 2)]
        for k, pair in enumerate(pairs_in):
            frames = jnp.dot(post[...], src_all[pair], preferred_element_type=F32)
            for j in range(half):
                for t in range(6):
                    to = ((t // 2) * 3 + t % 2 if t < 4 else (t - 4) * 3 + 2) * kb
                    frame[k, to : to + kb, j * LANES : (j + 1) * LANES] = frames[
                        j * kb : (j + 1) * kb, t * LANES : (t + 1) * LANES
                    ].astype(BF16)
        low_out = lane((kb, LANES)) < coef
        for k, pair in enumerate(pairs_in):
            sums = jnp.zeros((6 * kb, LANES), F32)
            for at_depth in range(0, half * LANES, 2 * LANES):
                depth = slice(at_depth, at_depth + 2 * LANES)
                sums += jnp.dot(frame[k, :, depth], place_turned[pair, depth, :], preferred_element_type=F32)
            for t in range(2):
                mine = sums[3 * t * kb : 3 * (t + 1) * kb]
                other = pltpu.roll(mine, coef, 1)
                lower, upper = (mine, other) if t == 0 else (other, mine)
                out_send[i * ROW + 2 * k + t] = jnp.concatenate(
                    [
                        jnp.where(low_out, lower[:kb], upper[kb : 2 * kb]),
                        jnp.where(
                            low_out[: kb // 2], lower[2 * kb : 2 * kb + kb // 2], upper[2 * kb + kb // 2 : 3 * kb]
                        ),
                    ],
                    axis=0,
                )
        for k in range(ROW):
            to = lax.rem(x + k, ROW)
            b = i * ROW + to

            @pl.when(b != me)
            def _():
                remote(out_send.at[b], mine_ref.at[me], o_ssem, o_rsem, at(to, zb * SIDE + i)).start()

    with jax.named_scope("class_rows"):
        each(0, SIDE, class_row)
    mine_ref[me] = out_send[me]
    out_size = (NP - 1) * out_send.shape[1]
    with jax.named_scope("take_out"):
        drain(o_rsem, out_size)

    @pl.when(core > 0)
    def _():
        pl.semaphore_wait(partner_in, 1)

    swap = remote(mine_ref, other_ref, c_ssem, c_rsem, partner)
    swap.start()

    drain(g_ssem, (SIDE - 1) * (bundle_size + ROW * kb // 2) + SIDE * (ROW - 1) * (bundle_size + kb // 2))
    drain(o_ssem, out_size)

    @pl.when(owner < OWNERS)
    def _():
        drain(rs_ssem, (OWNERS - 1) * share_size)
        drain(ag_ssem, (nb - 3) * ag_send.shape[0] + (nb - 1) * top_send.shape[0] + NP)

        @pl.when(later)
        def _():
            drain(ag_ssem, ag_send.shape[0])

    @pl.when(zb == 0)
    def _():
        drain(pass_ssem, OWNERS * ag_send.shape[0])

    @pl.when(zb == nb - 1)
    def _():
        drain(pass_ssem, OWNERS // 2 * ag_send.shape[0])

    @pl.when(owner >= OWNERS)
    def _():
        drain(rs_ssem, OWNERS * share_size)

    with jax.named_scope("swap"):
        swap.wait()


def finish(mine_ref, other_ref, ev_ref, cs_ref, cw_ref, out_ref):
    coef, kb = cw_ref.shape[0], cs_ref.shape[0] // NP
    halves = []
    for b in range(NP):
        both = mine_ref[b] + other_ref[b]
        cs_ref[b * kb : (b + 1) * kb, :] = both[:kb]
        halves.append(both[kb:])
    for first in range(0, NP, NP // 2):
        turned = jnp.concatenate(halves[first : first + NP // 2], axis=0).T
        for k in range(NP // 2):
            lanes = slice(k * kb // 2, (k + 1) * kb // 2)
            to = (first + k) * kb
            cw_ref[:, to : to + kb // 2] = turned[:coef, lanes]
            cw_ref[:, to + kb // 2 : to + kb] = turned[coef:, lanes]
    out_ref[...] = ev_ref[:, : out_ref.shape[1]]


def body(nz, particles, classes, ctf, sigma2, shell_of, rot_table, ctf_group):
    count, coef = particles.shape[0], shell_of.shape[0]
    classes_n, rotations = classes.shape[0], rot_table.shape[0]
    nb = nz // SIDE
    kb = classes_n // NP
    half = rotations // 2
    pairs = half * kb
    piece = pairs // OWNERS * 2 // 3
    dma = pltpu.SemaphoreType.DMA
    regular = pltpu.SemaphoreType.REGULAR
    vmem = pltpu.VMEM
    i32 = jnp.int32
    arrays = (
        particles,
        classes,
        ctf,
        sigma2.reshape(1, -1),
        shell_of.reshape(1, -1),
        rot_table,
        ctf_group.reshape(1, -1),
    )
    mine, other, evidence = pl.pallas_call(
        functools.partial(kernel, nz),
        out_shape=[
            jax.ShapeDtypeStruct((NP, 24, LANES), F32),
            jax.ShapeDtypeStruct((NP, 24, LANES), F32),
            jax.ShapeDtypeStruct((1, LANES), F32),
        ],
        in_specs=[pl.BlockSpec(memory_space=pltpu.HBM)] * 7,
        out_specs=[pl.BlockSpec(memory_space=vmem)] * 3,
        scratch_shapes=[
            *[vmem(a.shape, a.dtype) for a in arrays[1:]],
            vmem((NP, count + half + 24, LANES), BF16),
            vmem((SIDE, ROW * kb, LANES), BF16),
            vmem((NP, kb, LANES), BF16),
            vmem((NP * coef, half * LANES), BF16),
            vmem((NP // 2, half * LANES, 2 * coef), BF16),
            vmem((SIDE, ROW * 5 * LANES, 2 * LANES), BF16),
            vmem((NP // 2, 2 * LANES, 6 * LANES), BF16),
            vmem((NP // 4, 8 * kb, 4 * coef), BF16),
            vmem((SIDE, pairs, ROW * 5 * LANES), BF16),
            vmem((pairs, 2 * LANES), F32),
            vmem((OWNERS, piece, LANES), i32),
            vmem((OWNERS, 4, LANES), F32),
            vmem((nb, piece, LANES), i32),
            vmem((nb, 4, LANES), F32),
            vmem((piece, LANES), i32),
            vmem((2, LANES), F32),
            vmem((OWNERS, piece, LANES), i32),
            vmem((OWNERS, 2, LANES), F32),
            vmem((1, LANES), F32),
            vmem((OWNERS * NP, 1, LANES), F32),
            vmem((1, LANES), F32),
            vmem((NP, 1, LANES), F32),
            vmem((pairs, 2 * LANES), BF16),
            vmem((ROW // 2, 6 * kb, half * LANES), BF16),
            vmem((NP, 24, LANES), F32),
            vmem((1152, 1, LANES), F32),
            dma((len(arrays) + 1,)),
            dma,
            dma((SIDE,)),
            dma((SIDE,)),
            dma,
            dma((nb,)),
            dma,
            dma,
            dma((OWNERS,)),
            *[dma] * 8,
            regular((SIDE,)),
            regular,
            regular((OWNERS,)),
            regular,
            regular,
        ],
        compiler_params=pltpu.CompilerParams(
            collective_id=0, has_side_effects=True, vmem_limit_bytes=40 * 1024 * 1024
        ),
        name="averaging",
    )(*[pltpu.with_memory_space_constraint(a, pltpu.HBM) for a in arrays])
    sums, weights, evidence = pl.pallas_call(
        finish,
        out_shape=[
            jax.ShapeDtypeStruct((classes_n, 2 * coef), F32),
            jax.ShapeDtypeStruct((coef, classes_n), F32),
            jax.ShapeDtypeStruct((1, count), F32),
        ],
        in_specs=[pl.BlockSpec(memory_space=vmem)] * 3,
        out_specs=[pl.BlockSpec(memory_space=vmem)] * 3,
        compiler_params=pltpu.CompilerParams(vmem_limit_bytes=4 * 1024 * 1024),
        name="finish",
    )(mine, other, evidence)
    return sums, weights.T, evidence.reshape(-1)


def solution(mesh):
    nz = mesh.shape["shell"] // ROW
    split = Mesh(mesh.devices.reshape(mesh.shape["groups"], ROW, nz, mesh.shape["batch"]), AXES)
    shell = ("x", "z")
    placed = (
        P(("groups", "batch"), shell),
        P("groups", shell),
        P("groups", shell),
        P("groups"),
        P(shell),
        P(None, shell),
        P(("groups", "batch")),
    )
    return jax.shard_map(
        functools.partial(body, nz),
        mesh=split,
        in_specs=placed,
        out_specs=(P("groups", shell), P("groups", shell), P(("groups", "batch"))),
        check_vma=False,
    )
```

```python
import functools

import jax
import jax.numpy as jnp
from jax import lax
from jax.experimental import pallas as pl
from jax.experimental.pallas import tpu as pltpu
from jax.sharding import Mesh
from jax.sharding import PartitionSpec as P

MESH = pl.DeviceIdType.MESH
ROW = 4
SIDE = 4
NP = ROW * SIDE
OWNERS = 4
KEPT = 3
LANES = 128
F32 = jnp.float32
BF16 = jnp.bfloat16
NT = (((1,), (1,)), ((), ()))
AXES = ("groups", "x", "z", "batch")


def lane(shape):
    return lax.broadcasted_iota(jnp.int32, shape, 1)


def compact(w):
    free = lane((8, LANES)) >= 80
    kept = []
    for r in range(0, w.shape[0], 48):
        a, b = w[r + 32 : r + 40], w[r + 40 : r + 48]
        kept += [
            jnp.where(free, pltpu.roll(a, 80, 1), w[r : r + 8]),
            jnp.where(free, pltpu.roll(a, 32, 1), w[r + 8 : r + 16]),
            jnp.where(free, pltpu.roll(b, 80, 1), w[r + 16 : r + 24]),
            jnp.where(free, pltpu.roll(b, 32, 1), w[r + 24 : r + 32]),
        ]
    return jnp.concatenate(kept, axis=0)


def expand(w):
    first = lane((8, LANES)) < 48
    whole = []
    for r in range(0, w.shape[0], 32):
        part = w[r : r + 32]
        whole += [
            part,
            jnp.where(first, pltpu.roll(part[0:8], 48, 1), pltpu.roll(part[8:16], 96, 1)),
            jnp.where(first, pltpu.roll(part[16:24], 48, 1), pltpu.roll(part[24:32], 96, 1)),
        ]
    return jnp.concatenate(whole, axis=0)


def spread(row):
    free = lane((1, LANES)) >= 80
    return jnp.where(free, pltpu.roll(row, 80, 1), row), jnp.where(free, pltpu.roll(row, 32, 1), row)


def tiles(even, odd, rows):
    e = jnp.broadcast_to(even, (8, LANES))
    o = jnp.broadcast_to(odd, (8, LANES))
    return jnp.concatenate([e, o] * (rows // 16), axis=0)


def over_rows(values, combine, reduce):
    split = [values[r : r + 8] for r in range(0, values.shape[0], 8)]
    even = reduce(functools.reduce(combine, split[0::2]), axis=0, keepdims=True)
    odd = reduce(functools.reduce(combine, split[1::2]), axis=0, keepdims=True)
    first = lane((1, LANES)) < 48
    moved = jnp.where(first, pltpu.roll(even, 48, 1), pltpu.roll(odd, 96, 1))
    return combine(combine(even, odd), moved)


def kernel(
    nz,
    part_hbm,
    cls_hbm,
    ctf_hbm,
    sig_hbm,
    sh_hbm,
    tab_hbm,
    grp_hbm,
    mine_ref,
    other_ref,
    ev_ref,
    cls_ref,
    ctf_ref,
    sig_ref,
    sh_ref,
    tab_ref,
    grp_ref,
    bundle,
    cls_z,
    cls_all,
    place,
    place_turned,
    w_all,
    src_all,
    left,
    rot_all,
    score,
    rs_send,
    rs_scale,
    rs_recv,
    rs_rscale,
    ag_send,
    top_send,
    ag_recv,
    top_recv,
    lse_send,
    lse_first,
    lse_own,
    lse_all,
    raw,
    post,
    frame,
    out_send,
    sizes,
    in_sem,
    g_ssem,
    z_rsem,
    x_rsem,
    rs_ssem,
    rs_rsem,
    ag_ssem,
    pass_ssem,
    ag_rsem,
    top_rsem,
    first_rsem,
    lse_ssem,
    lse_rsem,
    o_ssem,
    o_rsem,
    c_ssem,
    c_rsem,
    column_in,
    others_in,
    owner_in,
    first_in,
    partner_in,
):
    nb = nz // SIDE
    count, coef = part_hbm.shape[0], ctf_ref.shape[1]
    kb = cls_all.shape[1]
    half = tab_ref.shape[0] // 2
    rows = half * kb // OWNERS
    group = lax.axis_index("groups")
    x = lax.axis_index("x")
    z = lax.axis_index("z")
    core = lax.axis_index("batch")
    zb, zi = z // SIDE, lax.rem(z, SIDE)
    me = zi * ROW + x
    def owns(b):
        return jnp.logical_or(
            jnp.logical_and(b >= 1, b < 3), jnp.logical_and(b >= nb - 3, b < nb - 1)
        )

    def home(o):
        return jnp.where(o < 2, o + 1, o + nb - 5)

    owner = jnp.where(owns(zb), jnp.where(zb < 3, zb - 1, zb - nb + 5), OWNERS)

    def greets(a, b):
        between = jnp.logical_and(jnp.logical_and(a >= 1, a < b), b < nb - 1)
        return jnp.logical_or(
            jnp.logical_and(between, jnp.logical_or(owns(a), owns(b))),
            jnp.logical_or(
                jnp.logical_and(b == 0, jnp.logical_and(a >= 1, a < 3)), jnp.logical_and(b == nb - 1, owns(a))
            ),
        )

    def at(x_, z_):
        return (group, x_, z_, core)

    def mate(k):
        i = lax.rem(me + k, NP)
        return i, at(lax.rem(i, ROW), zb * SIDE + i // ROW)

    def far(b):
        return at(x, b * SIDE + zi)

    partner = (group, x, z, 1 - core)

    def remote(src, dst, ssem, rsem, device):
        return pltpu.make_async_remote_copy(
            src_ref=src, dst_ref=dst, send_sem=ssem, recv_sem=rsem, device_id=device, device_id_type=MESH
        )

    def drain(semaphore, size):
        whole = sizes.at[0:size]
        remote(whole, whole, semaphore, semaphore, partner).wait_recv()

    def each(lower, upper, step):
        def turn(k, _):
            step(k)
            return 0

        lax.fori_loop(lower, upper, turn, 0)

    def tell(semaphore, device):
        pl.semaphore_signal(semaphore, inc=1, device_id=device, device_id_type=MESH)

    def rows_of(i, n):
        return pl.ds(pl.multiple_of(i * n, n), n)

    given = (ctf_hbm, sig_hbm, sh_hbm, tab_hbm, part_hbm, cls_hbm.at[rows_of(zi, ROW * kb)], cls_hbm, grp_hbm)
    taken = (ctf_ref, sig_ref, sh_ref, tab_ref, bundle.at[me, 0:count], cls_z.at[zi], cls_ref, grp_ref)
    loads = [pltpu.make_async_copy(a, b, in_sem.at[k]) for k, (a, b) in enumerate(zip(given, taken))]
    for load in loads:
        load.start()

    barrier = pltpu.get_barrier_semaphore()
    each(1, ROW, lambda k: tell(barrier, at(lax.rem(x + k, ROW), z)))
    each((zi + 1) * ROW, NP, lambda i: tell(barrier, at(lax.rem(i, ROW), zb * SIDE + i // ROW)))

    @pl.when(core > 0)
    def _():
        tell(barrier, partner)

    def greet(b):
        @pl.when(greets(zb, b))
        def _():
            tell(barrier, far(b))

    each(0, nb, greet)
    for load in loads[:4]:
        load.wait()

    levels = sig_ref.shape[1]
    pick = lax.broadcasted_iota(jnp.int32, (levels, coef), 0) == sh_ref[...]
    noise_of = jnp.broadcast_to(sig_ref[...], (coef, levels)).T
    noise = jnp.sum(jnp.where(pick, noise_of, 0.0), axis=0, keepdims=True)
    ctf = ctf_ref[...]
    par = jnp.concatenate([ctf, (1.0 / noise) * ctf], axis=1)
    par_high = par.astype(BF16).astype(F32)
    par_mid = (par - par_high).astype(BF16).astype(F32)
    offset = (x * nz + z) * coef
    table = (tab_ref[...] - offset).astype(F32)
    table = jnp.concatenate([table[:half], table[half:]], axis=1)
    bundle[me, count:] = jnp.concatenate([table, par_high, par_mid, (par - par_high) - par_mid], axis=0).astype(BF16)
    for load in loads[4:]:
        load.wait()
    with jax.named_scope("barrier"):
        greeted = sum(jnp.where(greets(b, zb), 1, 0) for b in range(nb))
        pl.semaphore_wait(barrier, ROW - 1 + zi * ROW + jnp.where(core > 0, 0, 1) + greeted)

    def down(i):
        device = at(x, zb * SIDE + i)
        remote(bundle.at[me], bundle.at[me], g_ssem, z_rsem.at[zi], device).start()
        remote(cls_ref.at[rows_of(i, ROW * kb)], cls_z.at[zi], g_ssem, z_rsem.at[zi], device).start()

    def across(i):
        b = i * ROW + x
        for k in range(1, ROW):
            to = lax.rem(x + k, ROW)
            device = at(to, z)
            remote(bundle.at[b], bundle.at[b], g_ssem, x_rsem.at[i], device).start()
            remote(cls_z.at[i, rows_of(to, kb)], cls_all.at[b], g_ssem, x_rsem.at[i], device).start()

    bundle_size = bundle.shape[1] // 2
    def tell_above(i):
        tell(column_in.at[zi], at(x, zb * SIDE + i))
        each(1, ROW, lambda k: tell(others_in, at(lax.rem(x + k, ROW), zb * SIDE + i)))

    each(0, zi, tell_above)
    each(0, zi, lambda k: down(zi - 1 - k))
    across(zi)

    @pl.when(owner < OWNERS)
    def _():
        def tell_earlier(b):
            @pl.when(greets(b, zb))
            def _():
                tell(owner_in.at[owner], far(b))

        each(0, nb, tell_earlier)

    @pl.when(zb == 0)
    def _():
        tell(first_in, far(1))

    @pl.when(core == 0)
    def _():
        tell(partner_in, partner)

    with jax.named_scope("zeros"):
        w_all[...] = jnp.zeros_like(w_all)
        src_all[...] = jnp.zeros_like(src_all)
        left[...] = jnp.zeros_like(left)
    score[...] = jnp.zeros_like(score)
    cls_all[me] = cls_z[zi, rows_of(x, kb), :]
    member = jnp.broadcast_to(grp_ref[...].astype(F32), (LANES, count)).T
    low = lane((count, LANES)) < coef
    low_kb = lane((kb, LANES)) < coef

    def pass_on(i):
        with jax.named_scope("came_down"):
            drain(z_rsem.at[i], bundle_size + ROW * kb // 2)
        across(i)
        cls_all[i * ROW + x] = cls_z[i, rows_of(x, kb), :]

    def amplitudes(tail):
        par = tail[half : half + 8] + tail[half + 8 : half + 16] + tail[half + 16 : half + 24]
        sel = jnp.broadcast_to(par[0:1], (count, LANES))
        for g in range(1, par.shape[0]):
            sel = jnp.where(member == g, par[g : g + 1], sel)
        other = pltpu.roll(sel, coef, 1)
        return jnp.where(low, sel, other), jnp.where(low, other, sel)

    def turned_over(a):
        return jnp.concatenate([a, jnp.zeros((LANES - count, LANES), F32)], axis=0).astype(BF16).T

    def prepare(g, i):
        b = g * ROW + i
        landing = bundle[b, count:].astype(F32)
        amp, wamp = amplitudes(landing)
        weighted = turned_over(wamp * bundle[b, 0:count].astype(F32))
        pen = -0.5 * (wamp * amp)
        pen_hi = pen.astype(BF16).astype(F32)
        pen = turned_over(jnp.where(low, pen_hi, pen - pen_hi))
        for k, piece in enumerate((weighted[:coef], weighted[coef:], pen[:coef], pen[:coef], pen[coef:])):
            for s in range(2):
                top = pl.multiple_of((5 * i + k) * LANES + s * coef, coef)
                w_all[g, pl.ds(top, coef), s * LANES : (s + 1) * LANES] = piece
        index = lax.broadcasted_iota(jnp.int32, (coef, LANES), 0).astype(F32).astype(BF16)
        ones, zeros = jnp.ones((coef, LANES), BF16), jnp.zeros((coef, LANES), BF16)
        for j in range(half):
            row = jnp.broadcast_to(landing[j : j + 1], (16, LANES)).astype(BF16)
            row = jnp.concatenate([row] * (coef // 16), axis=0)
            place[rows_of(b, coef), j * LANES : (j + 1) * LANES] = jnp.where(index == row, ones, zeros)

    def prepare_sources(pair):
        for i in range(2):
            b = pair * 2 + i
            amp, _ = amplitudes(bundle[b, count:].astype(F32))
            source = amp * bundle[b, 0:count].astype(F32)
            source_turned = pltpu.roll(source, coef, 1)
            power = amp * amp
            for s in range(2):
                top = s * LANES

                def keep(lower, upper):
                    return (jnp.where(low, lower, 0.0) if s == 0 else jnp.where(low, 0.0, upper)).astype(BF16)

                for t, kept in (
                    (2 * i, keep(source, source_turned)),
                    (2 * i + 1, keep(source_turned, source)),
                    (4 + i, keep(power, power)),
                ):
                    src_all[pair, top : top + count, t * LANES : (t + 1) * LANES] = kept
        for j in range(half):
            lanes = slice(j * LANES, (j + 1) * LANES)
            place_turned[pair, lanes, :] = place[rows_of(pair, 2 * coef), lanes].T

    def rotate(g):
        for i in range(4):
            image = cls_all[g * 4 + i].astype(F32)
            turned = pltpu.roll(image, coef, 1)
            if i % 2 == 0:
                re, im = jnp.where(low_kb, image, 0.0), jnp.where(low_kb, turned, 0.0)
            else:
                re, im = jnp.where(low_kb, 0.0, turned), jnp.where(low_kb, 0.0, image)
            top = (i // 2) * LANES
            left[g, 2 * i * kb : (2 * i + 1) * kb, top : top + LANES] = re.astype(BF16)
            left[g, (2 * i + 1) * kb : (2 * i + 2) * kb, top : top + LANES] = im.astype(BF16)
        lhs = left[g]
        for jj in range(half // 2):
            turned = jnp.dot(
                lhs, place[rows_of(g, 4 * coef), jj * 256 : (jj + 1) * 256], preferred_element_type=F32
            )
            for i in range(4):
                for t in range(2):
                    j = jj * 2 + t
                    re = turned[2 * i * kb : (2 * i + 1) * kb, t * LANES : (t + 1) * LANES]
                    im = turned[(2 * i + 1) * kb : (2 * i + 2) * kb, t * LANES : (t + 1) * LANES]
                    power = re * re + im * im
                    power_hi = power.astype(BF16)
                    power_lo = (power - power_hi.astype(F32)).astype(BF16)
                    to = slice(j * kb, (j + 1) * kb)
                    pieces = re.astype(BF16), im.astype(BF16), power_hi, power_lo, power_hi
                    for k, piece in enumerate(pieces):
                        at_lane = (5 * i + k) * LANES
                        rot_all[g, to, at_lane : at_lane + LANES] = piece

    def score_row(g):
        with jax.named_scope("arrive"):
            drain(x_rsem.at[g], (ROW - 1) * (bundle_size + kb // 2))
        with jax.named_scope("scores"):
            for k in range(1, ROW):
                prepare(g, lax.rem(x + k, ROW))
            rotate(g)
            score[...] += jnp.dot(rot_all[g], w_all[g], preferred_element_type=F32)

    prepare(zi, x)

    def down_later(i):
        pl.semaphore_wait(column_in.at[i], 1)
        down(i)

    with jax.named_scope("down_later"):
        each(zi + 1, SIDE, down_later)

    nearest = (0, 1, 2, 3), (1, 0, 1, 2), (2, 2, 0, 1), (3, 3, 3, 0)

    def place_of(step):
        return sum(
            jnp.where(jnp.logical_and(step == t, zi == k), nearest[t][k], 0) for t in range(SIDE) for k in range(SIDE)
        )

    def turn_of(step):
        @pl.when(step == 1)
        def _():
            for t in range(1, SIDE):
                pass_on(place_of(t))
                prepare(place_of(t), x)

        score_row(place_of(step))

    each(0, SIDE, turn_of)

    @pl.when(zi < SIDE - 1)
    def _():
        pl.semaphore_wait(others_in, (SIDE - 1 - zi) * (ROW - 1))

    def share(o):
        return score[rows_of(o, rows), :]

    share_size = rs_send.shape[1] + rs_scale.shape[1]
    for o in (1, 2, 0, 3):

        @pl.when(owner != o)
        def _():
            piece = share(o)
            one, two = piece[:, :LANES], piece[:, LANES:]
            most = jnp.max(jnp.maximum(one, two), axis=0, keepdims=True)
            least = jnp.min(jnp.minimum(one, two), axis=0, keepdims=True)
            middle = 0.5 * (most + least)
            reach = jnp.maximum(0.5 * (most - least), 1e-30)
            fit = 32767.0 / reach
            one = jnp.round((one - middle) * fit).astype(jnp.int32)
            two = jnp.round((two - middle) * fit).astype(jnp.int32)
            rs_send[o] = compact((one & 0xFFFF) | (two << 16))
            rs_scale[o] = jnp.concatenate([*spread(reach * (1.0 / 32767.0)), *spread(middle)], axis=0)

            @pl.when(jnp.logical_not(greets(home(o), zb)))
            def _():
                with jax.named_scope("owner_in"):
                    pl.semaphore_wait(owner_in.at[o], 1)

            with jax.named_scope("share_go"):
                remote(rs_send.at[o], rs_recv.at[zb], rs_ssem, rs_rsem.at[zb], far(home(o))).start()
                remote(rs_scale.at[o], rs_rscale.at[zb], rs_ssem, rs_rsem.at[zb], far(home(o))).start()

    @pl.when(zb == 1)
    def _():
        pl.semaphore_wait(first_in, 1)
        tell(owner_in.at[2], far(0))
        tell(owner_in.at[3], far(0))

    kept_back = jnp.where(owner < OWNERS, KEPT, 0)
    with jax.named_scope("sources"):
        each(kept_back, NP // 2, prepare_sources)

    later = zb >= nb // 2

    def send_post(b):
        @pl.when(b != zb)
        def _():
            remote(ag_send, ag_recv.at[owner], ag_ssem, ag_rsem.at[owner], far(b)).start()

    @pl.when(owner < OWNERS)
    def _():
        own = share(owner)
        total = compact(own[:, :LANES]), compact(own[:, LANES:])

        def add_share(k, so_far):
            b = jnp.where(k < zb, k, k + 1)
            with jax.named_scope("share_in"):
                drain(rs_rsem.at[b], share_size)
            word = rs_recv[b]
            step = tiles(rs_rscale[b, 0:1], rs_rscale[b, 1:2], word.shape[0])
            middle = tiles(rs_rscale[b, 2:3], rs_rscale[b, 3:4], word.shape[0])
            return (
                so_far[0] + (((word << 16) >> 16).astype(F32) * step + middle),
                so_far[1] + ((word >> 16).astype(F32) * step + middle),
            )

        total_one, total_two = lax.fori_loop(0, nb - 1, add_share, total)
        peak = over_rows(jnp.maximum(total_one, total_two), jnp.maximum, jnp.max)
        shift = tiles(*spread(peak), total_one.shape[0])
        exp_one, exp_two = jnp.exp(total_one - shift), jnp.exp(total_two - shift)
        evidence = peak + jnp.log(over_rows(exp_one + exp_two, jnp.add, jnp.sum))
        top_send[...] = jnp.concatenate([peak, evidence], axis=0)
        lse_send[...] = evidence

        for k in range(NP):
            remote(
                lse_send, lse_first.at[owner * NP + me], ag_ssem, first_rsem, at(k % ROW, k // ROW)
            ).start()
        for b in range(nb):

            @pl.when(b != zb)
            def _():
                remote(top_send, top_recv.at[owner], ag_ssem, top_rsem, far(b)).start()

        one = (exp_one * 65535.0 + 0.5).astype(jnp.int32)
        two = (exp_two * 65535.0 + 0.5).astype(jnp.int32)
        ag_send[...] = (one & 0xFFFF) | (two << 16)
        with jax.named_scope("kept_back"):
            each(0, KEPT, prepare_sources)

        def send_early(b):
            @pl.when(jnp.logical_not(jnp.logical_and(later, b == 1)))
            def _():
                send_post(b)

        each(0, nb - 2, send_early)
        ag_recv[owner] = ag_send[...]
        top_recv[owner] = top_send[...]

    with jax.named_scope("top_in"):

        @pl.when(owner < OWNERS)
        def _():
            drain(top_rsem, (OWNERS - 1) * top_send.shape[0])

        @pl.when(owner >= OWNERS)
        def _():
            drain(top_rsem, OWNERS * top_send.shape[0])

    def merged(parts, axis):
        most = jnp.max(parts, axis=axis, keepdims=True)
        return most + jnp.log(jnp.sum(jnp.exp(parts - most), axis=axis, keepdims=True))

    @pl.when(jnp.logical_and(owner < OWNERS, later))
    def _():
        each(nb - 2, nb, send_post)

    def pass_post(o, b):
        with jax.named_scope("post_in"):
            drain(ag_rsem.at[o], ag_send.shape[0])
        remote(ag_recv.at[o], ag_recv.at[o], pass_ssem, ag_rsem.at[o], far(b)).start()

    used = lane((rows, LANES)) < count

    def unpack(o):
        word = expand(ag_recv[o])
        raw[rows_of(o, rows), 0:128] = jnp.where(used, (word & 0xFFFF).astype(F32), 0.0)
        raw[rows_of(o, rows), 128:256] = jnp.where(used, lax.shift_right_logical(word, 16).astype(F32), 0.0)

    @pl.when(zb == 0)
    def _():
        for o in range(OWNERS):
            pass_post(o, nb - 1 if o < OWNERS // 2 else 1)
        each(0, OWNERS, unpack)
        with jax.named_scope("first_in"):
            drain(first_rsem, OWNERS * NP)
        ev_ref[...] = merged(lse_first[...], 0)[0]

    @pl.when(zb > 0)
    def _():
        lse_own[...] = merged(jnp.concatenate([top_recv[o, 1:2] for o in range(OWNERS)], axis=0), 0)
        each(1, NP, lambda k: remote(lse_own, lse_all.at[me], lse_ssem, lse_rsem, mate(k)[1]).start())
        lse_all[me] = lse_own[...]
        with jax.named_scope("lse_in"):
            drain(lse_rsem, NP - 1)
        drain(lse_ssem, NP - 1)
        ev_ref[...] = merged(lse_all[...], 0)[0]

    evidence = ev_ref[...]
    def take_post(o):
        passes = jnp.logical_and(zb == nb - 1, o < OWNERS // 2)

        @pl.when(passes)
        def _():
            pass_post(o, nb - 2)

        @pl.when(jnp.logical_not(jnp.logical_or(passes, jnp.logical_or(o == owner, zb == 0))))
        def _():
            with jax.named_scope("post_in"):
                drain(ag_rsem.at[o], ag_send.shape[0])

        @pl.when(zb > 0)
        def _():
            unpack(o)

        scale = jnp.exp(top_recv[o, 0:1] - evidence) * (1.0 / 65535.0)
        scale = jnp.where(lane((1, LANES)) < count, scale, 0.0)
        post[rows_of(o, rows), 0:128] = (raw[rows_of(o, rows), 0:128] * scale).astype(BF16)
        post[rows_of(o, rows), 128:256] = (raw[rows_of(o, rows), 128:256] * scale).astype(BF16)

    each(0, OWNERS, take_post)

    def class_row(i):
        pairs_in = [i * (ROW // 2) + k for k in range(ROW // 2)]
        for k, pair in enumerate(pairs_in):
            frames = jnp.dot(post[...], src_all[pair], preferred_element_type=F32)
            for j in range(half):
                for t in range(6):
                    to = ((t // 2) * 3 + t % 2 if t < 4 else (t - 4) * 3 + 2) * kb
                    frame[k, to : to + kb, j * LANES : (j + 1) * LANES] = frames[
                        j * kb : (j + 1) * kb, t * LANES : (t + 1) * LANES
                    ].astype(BF16)
        low_out = lane((kb, LANES)) < coef
        for k, pair in enumerate(pairs_in):
            sums = jnp.zeros((6 * kb, LANES), F32)
            for at_depth in range(0, half * LANES, 2 * LANES):
                depth = slice(at_depth, at_depth + 2 * LANES)
                sums += jnp.dot(frame[k, :, depth], place_turned[pair, depth, :], preferred_element_type=F32)
            for t in range(2):
                mine = sums[3 * t * kb : 3 * (t + 1) * kb]
                other = pltpu.roll(mine, coef, 1)
                lower, upper = (mine, other) if t == 0 else (other, mine)
                out_send[i * ROW + 2 * k + t] = jnp.concatenate(
                    [
                        jnp.where(low_out, lower[:kb], upper[kb : 2 * kb]),
                        jnp.where(
                            low_out[: kb // 2], lower[2 * kb : 2 * kb + kb // 2], upper[2 * kb + kb // 2 : 3 * kb]
                        ),
                    ],
                    axis=0,
                )
        for k in range(ROW):
            to = lax.rem(x + k, ROW)
            b = i * ROW + to

            @pl.when(b != me)
            def _():
                remote(out_send.at[b], mine_ref.at[me], o_ssem, o_rsem, at(to, zb * SIDE + i)).start()

    with jax.named_scope("class_rows"):
        each(0, SIDE, class_row)
    mine_ref[me] = out_send[me]
    out_size = (NP - 1) * out_send.shape[1]
    with jax.named_scope("take_out"):
        drain(o_rsem, out_size)

    @pl.when(core > 0)
    def _():
        pl.semaphore_wait(partner_in, 1)

    swap = remote(mine_ref, other_ref, c_ssem, c_rsem, partner)
    swap.start()

    drain(g_ssem, (SIDE - 1) * (bundle_size + ROW * kb // 2) + SIDE * (ROW - 1) * (bundle_size + kb // 2))
    drain(o_ssem, out_size)

    @pl.when(owner < OWNERS)
    def _():
        drain(rs_ssem, (OWNERS - 1) * share_size)
        drain(ag_ssem, (nb - 3) * ag_send.shape[0] + (nb - 1) * top_send.shape[0] + NP)

        @pl.when(later)
        def _():
            drain(ag_ssem, ag_send.shape[0])

    @pl.when(zb == 0)
    def _():
        drain(pass_ssem, OWNERS * ag_send.shape[0])

    @pl.when(zb == nb - 1)
    def _():
        drain(pass_ssem, OWNERS // 2 * ag_send.shape[0])

    @pl.when(owner >= OWNERS)
    def _():
        drain(rs_ssem, OWNERS * share_size)

    with jax.named_scope("swap"):
        swap.wait()


def finish(mine_ref, other_ref, ev_ref, cs_ref, cw_ref, out_ref):
    coef, kb = cw_ref.shape[0], cs_ref.shape[0] // NP
    halves = []
    for b in range(NP):
        both = mine_ref[b] + other_ref[b]
        cs_ref[b * kb : (b + 1) * kb, :] = both[:kb]
        halves.append(both[kb:])
    for first in range(0, NP, NP // 2):
        turned = jnp.concatenate(halves[first : first + NP // 2], axis=0).T
        for k in range(NP // 2):
            lanes = slice(k * kb // 2, (k + 1) * kb // 2)
            to = (first + k) * kb
            cw_ref[:, to : to + kb // 2] = turned[:coef, lanes]
            cw_ref[:, to + kb // 2 : to + kb] = turned[coef:, lanes]
    out_ref[...] = ev_ref[:, : out_ref.shape[1]]


def body(nz, particles, classes, ctf, sigma2, shell_of, rot_table, ctf_group):
    count, coef = particles.shape[0], shell_of.shape[0]
    classes_n, rotations = classes.shape[0], rot_table.shape[0]
    nb = nz // SIDE
    kb = classes_n // NP
    half = rotations // 2
    pairs = half * kb
    piece = pairs // OWNERS * 2 // 3
    dma = pltpu.SemaphoreType.DMA
    regular = pltpu.SemaphoreType.REGULAR
    vmem = pltpu.VMEM
    i32 = jnp.int32
    arrays = (
        particles,
        classes,
        ctf,
        sigma2.reshape(1, -1),
        shell_of.reshape(1, -1),
        rot_table,
        ctf_group.reshape(1, -1),
    )
    mine, other, evidence = pl.pallas_call(
        functools.partial(kernel, nz),
        out_shape=[
            jax.ShapeDtypeStruct((NP, 24, LANES), F32),
            jax.ShapeDtypeStruct((NP, 24, LANES), F32),
            jax.ShapeDtypeStruct((1, LANES), F32),
        ],
        in_specs=[pl.BlockSpec(memory_space=pltpu.HBM)] * 7,
        out_specs=[pl.BlockSpec(memory_space=vmem)] * 3,
        scratch_shapes=[
            *[vmem(a.shape, a.dtype) for a in arrays[1:]],
            vmem((NP, count + half + 24, LANES), BF16),
            vmem((SIDE, ROW * kb, LANES), BF16),
            vmem((NP, kb, LANES), BF16),
            vmem((NP * coef, half * LANES), BF16),
            vmem((NP // 2, half * LANES, 2 * coef), BF16),
            vmem((SIDE, ROW * 5 * LANES, 2 * LANES), BF16),
            vmem((NP // 2, 2 * LANES, 6 * LANES), BF16),
            vmem((NP // 4, 8 * kb, 4 * coef), BF16),
            vmem((SIDE, pairs, ROW * 5 * LANES), BF16),
            vmem((pairs, 2 * LANES), F32),
            vmem((OWNERS, piece, LANES), i32),
            vmem((OWNERS, 4, LANES), F32),
            vmem((nb, piece, LANES), i32),
            vmem((nb, 4, LANES), F32),
            vmem((piece, LANES), i32),
            vmem((2, LANES), F32),
            vmem((OWNERS, piece, LANES), i32),
            vmem((OWNERS, 2, LANES), F32),
            vmem((1, LANES), F32),
            vmem((OWNERS * NP, 1, LANES), F32),
            vmem((1, LANES), F32),
            vmem((NP, 1, LANES), F32),
            vmem((pairs, 2 * LANES), F32),
            vmem((pairs, 2 * LANES), BF16),
            vmem((ROW // 2, 6 * kb, half * LANES), BF16),
            vmem((NP, 24, LANES), F32),
            vmem((1152, 1, LANES), F32),
            dma((len(arrays) + 1,)),
            dma,
            dma((SIDE,)),
            dma((SIDE,)),
            dma,
            dma((nb,)),
            dma,
            dma,
            dma((OWNERS,)),
            *[dma] * 8,
            regular((SIDE,)),
            regular,
            regular((OWNERS,)),
            regular,
            regular,
        ],
        compiler_params=pltpu.CompilerParams(
            collective_id=0, has_side_effects=True, vmem_limit_bytes=40 * 1024 * 1024
        ),
        name="averaging",
    )(*[pltpu.with_memory_space_constraint(a, pltpu.HBM) for a in arrays])
    sums, weights, evidence = pl.pallas_call(
        finish,
        out_shape=[
            jax.ShapeDtypeStruct((classes_n, 2 * coef), F32),
            jax.ShapeDtypeStruct((coef, classes_n), F32),
            jax.ShapeDtypeStruct((1, count), F32),
        ],
        in_specs=[pl.BlockSpec(memory_space=vmem)] * 3,
        out_specs=[pl.BlockSpec(memory_space=vmem)] * 3,
        compiler_params=pltpu.CompilerParams(vmem_limit_bytes=4 * 1024 * 1024),
        name="finish",
    )(mine, other, evidence)
    return sums, weights.T, evidence.reshape(-1)


def solution(mesh):
    nz = mesh.shape["shell"] // ROW
    split = Mesh(mesh.devices.reshape(mesh.shape["groups"], ROW, nz, mesh.shape["batch"]), AXES)
    shell = ("x", "z")
    placed = (
        P(("groups", "batch"), shell),
        P("groups", shell),
        P("groups", shell),
        P("groups"),
        P(shell),
        P(None, shell),
        P(("groups", "batch")),
    )
    return jax.shard_map(
        functools.partial(body, nz),
        mesh=split,
        in_specs=placed,
        out_specs=(P("groups", shell), P("groups", shell), P(("groups", "batch"))),
        check_vma=False,
    )
```

```python
import functools

import jax
import jax.numpy as jnp
from jax import lax
from jax.experimental import pallas as pl
from jax.experimental.pallas import tpu as pltpu
from jax.sharding import Mesh
from jax.sharding import PartitionSpec as P

MESH = pl.DeviceIdType.MESH
ROW = 4
SIDE = 4
NP = ROW * SIDE
OWNERS = 4
LANES = 128
F32 = jnp.float32
BF16 = jnp.bfloat16
NT = (((1,), (1,)), ((), ()))
AXES = ("groups", "x", "z", "batch")


def lane(shape):
    return lax.broadcasted_iota(jnp.int32, shape, 1)


def compact(w):
    free = lane((8, LANES)) >= 80
    kept = []
    for r in range(0, w.shape[0], 48):
        a, b = w[r + 32 : r + 40], w[r + 40 : r + 48]
        kept += [
            jnp.where(free, pltpu.roll(a, 80, 1), w[r : r + 8]),
            jnp.where(free, pltpu.roll(a, 32, 1), w[r + 8 : r + 16]),
            jnp.where(free, pltpu.roll(b, 80, 1), w[r + 16 : r + 24]),
            jnp.where(free, pltpu.roll(b, 32, 1), w[r + 24 : r + 32]),
        ]
    return jnp.concatenate(kept, axis=0)


def expand(w):
    first = lane((8, LANES)) < 48
    whole = []
    for r in range(0, w.shape[0], 32):
        part = w[r : r + 32]
        whole += [
            part,
            jnp.where(first, pltpu.roll(part[0:8], 48, 1), pltpu.roll(part[8:16], 96, 1)),
            jnp.where(first, pltpu.roll(part[16:24], 48, 1), pltpu.roll(part[24:32], 96, 1)),
        ]
    return jnp.concatenate(whole, axis=0)


def spread(row):
    free = lane((1, LANES)) >= 80
    return jnp.where(free, pltpu.roll(row, 80, 1), row), jnp.where(free, pltpu.roll(row, 32, 1), row)


def tiles(even, odd, rows):
    e = jnp.broadcast_to(even, (8, LANES))
    o = jnp.broadcast_to(odd, (8, LANES))
    return jnp.concatenate([e, o] * (rows // 16), axis=0)


def over_rows(values, combine, reduce):
    split = [values[r : r + 8] for r in range(0, values.shape[0], 8)]
    even = reduce(functools.reduce(combine, split[0::2]), axis=0, keepdims=True)
    odd = reduce(functools.reduce(combine, split[1::2]), axis=0, keepdims=True)
    first = lane((1, LANES)) < 48
    moved = jnp.where(first, pltpu.roll(even, 48, 1), pltpu.roll(odd, 96, 1))
    return combine(combine(even, odd), moved)


def kernel(
    nz,
    part_hbm,
    cls_hbm,
    ctf_hbm,
    sig_hbm,
    sh_hbm,
    tab_hbm,
    grp_hbm,
    mine_ref,
    other_ref,
    ev_ref,
    cls_ref,
    ctf_ref,
    sig_ref,
    sh_ref,
    tab_ref,
    grp_ref,
    bundle,
    cls_z,
    cls_all,
    place,
    place_turned,
    w_all,
    src_all,
    left,
    rot_all,
    score,
    rs_send,
    rs_scale,
    rs_recv,
    rs_rscale,
    ag_send,
    top_send,
    ag_recv,
    top_recv,
    lse_send,
    lse_first,
    lse_own,
    lse_all,
    post,
    frame,
    out_send,
    sizes,
    in_sem,
    g_ssem,
    z_rsem,
    x_rsem,
    rs_ssem,
    rs_rsem,
    ag_ssem,
    pass_ssem,
    ag_rsem,
    top_rsem,
    first_rsem,
    lse_ssem,
    lse_rsem,
    o_ssem,
    o_rsem,
    c_ssem,
    c_rsem,
    column_in,
    others_in,
    owner_in,
    first_in,
    partner_in,
):
    nb = nz // SIDE
    count, coef = part_hbm.shape[0], ctf_ref.shape[1]
    kb = cls_all.shape[1]
    half = tab_ref.shape[0] // 2
    rows = half * kb // OWNERS
    group = lax.axis_index("groups")
    x = lax.axis_index("x")
    z = lax.axis_index("z")
    core = lax.axis_index("batch")
    zb, zi = z // SIDE, lax.rem(z, SIDE)
    me = zi * ROW + x
    def owns(b):
        return jnp.logical_or(
            jnp.logical_and(b >= 1, b < 3), jnp.logical_and(b >= nb - 3, b < nb - 1)
        )

    def home(o):
        return jnp.where(o < 2, o + 1, o + nb - 5)

    owner = jnp.where(owns(zb), jnp.where(zb < 3, zb - 1, zb - nb + 5), OWNERS)

    def greets(a, b):
        between = jnp.logical_and(jnp.logical_and(a >= 1, a < b), b < nb - 1)
        return jnp.logical_or(
            jnp.logical_and(between, jnp.logical_or(owns(a), owns(b))),
            jnp.logical_or(
                jnp.logical_and(b == 0, jnp.logical_and(a >= 1, a < 3)), jnp.logical_and(b == nb - 1, owns(a))
            ),
        )

    def at(x_, z_):
        return (group, x_, z_, core)

    def mate(k):
        i = lax.rem(me + k, NP)
        return i, at(lax.rem(i, ROW), zb * SIDE + i // ROW)

    def far(b):
        return at(x, b * SIDE + zi)

    partner = (group, x, z, 1 - core)

    def remote(src, dst, ssem, rsem, device):
        return pltpu.make_async_remote_copy(
            src_ref=src, dst_ref=dst, send_sem=ssem, recv_sem=rsem, device_id=device, device_id_type=MESH
        )

    def drain(semaphore, size):
        whole = sizes.at[0:size]
        remote(whole, whole, semaphore, semaphore, partner).wait_recv()

    def each(lower, upper, step):
        def turn(k, _):
            step(k)
            return 0

        lax.fori_loop(lower, upper, turn, 0)

    def tell(semaphore, device):
        pl.semaphore_signal(semaphore, inc=1, device_id=device, device_id_type=MESH)

    def rows_of(i, n):
        return pl.ds(pl.multiple_of(i * n, n), n)

    given = (ctf_hbm, sig_hbm, sh_hbm, tab_hbm, part_hbm, cls_hbm.at[rows_of(zi, ROW * kb)], cls_hbm, grp_hbm)
    taken = (ctf_ref, sig_ref, sh_ref, tab_ref, bundle.at[me, 0:count], cls_z.at[zi], cls_ref, grp_ref)
    loads = [pltpu.make_async_copy(a, b, in_sem.at[k]) for k, (a, b) in enumerate(zip(given, taken))]
    for load in loads:
        load.start()

    barrier = pltpu.get_barrier_semaphore()
    each(1, ROW, lambda k: tell(barrier, at(lax.rem(x + k, ROW), z)))
    each((zi + 1) * ROW, NP, lambda i: tell(barrier, at(lax.rem(i, ROW), zb * SIDE + i // ROW)))

    @pl.when(core > 0)
    def _():
        tell(barrier, partner)

    def greet(b):
        @pl.when(greets(zb, b))
        def _():
            tell(barrier, far(b))

    each(0, nb, greet)
    for load in loads[:4]:
        load.wait()

    levels = sig_ref.shape[1]
    pick = lax.broadcasted_iota(jnp.int32, (levels, coef), 0) == sh_ref[...]
    noise_of = jnp.broadcast_to(sig_ref[...], (coef, levels)).T
    noise = jnp.sum(jnp.where(pick, noise_of, 0.0), axis=0, keepdims=True)
    ctf = ctf_ref[...]
    par = jnp.concatenate([ctf, (1.0 / noise) * ctf], axis=1)
    par_high = par.astype(BF16).astype(F32)
    par_mid = (par - par_high).astype(BF16).astype(F32)
    offset = (x * nz + z) * coef
    table = (tab_ref[...] - offset).astype(F32)
    table = jnp.concatenate([table[:half], table[half:]], axis=1)
    bundle[me, count:] = jnp.concatenate([table, par_high, par_mid, (par - par_high) - par_mid], axis=0).astype(BF16)
    for load in loads[4:]:
        load.wait()
    with jax.named_scope("barrier"):
        greeted = sum(jnp.where(greets(b, zb), 1, 0) for b in range(nb))
        pl.semaphore_wait(barrier, ROW - 1 + zi * ROW + jnp.where(core > 0, 0, 1) + greeted)

    def down(i):
        device = at(x, zb * SIDE + i)
        remote(bundle.at[me], bundle.at[me], g_ssem, z_rsem.at[zi], device).start()
        remote(cls_ref.at[rows_of(i, ROW * kb)], cls_z.at[zi], g_ssem, z_rsem.at[zi], device).start()

    def across(i):
        b = i * ROW + x
        for k in range(1, ROW):
            to = lax.rem(x + k, ROW)
            device = at(to, z)
            remote(bundle.at[b], bundle.at[b], g_ssem, x_rsem.at[i], device).start()
            remote(cls_z.at[i, rows_of(to, kb)], cls_all.at[b], g_ssem, x_rsem.at[i], device).start()

    bundle_size = bundle.shape[1] // 2
    def tell_above(i):
        tell(column_in.at[zi], at(x, zb * SIDE + i))
        each(1, ROW, lambda k: tell(others_in, at(lax.rem(x + k, ROW), zb * SIDE + i)))

    each(0, zi, tell_above)
    each(0, zi, lambda k: down(zi - 1 - k))
    across(zi)

    @pl.when(owner < OWNERS)
    def _():
        def tell_earlier(b):
            @pl.when(greets(b, zb))
            def _():
                tell(owner_in.at[owner], far(b))

        each(0, nb, tell_earlier)

    @pl.when(zb == 0)
    def _():
        tell(first_in, far(1))

    @pl.when(core == 0)
    def _():
        tell(partner_in, partner)

    with jax.named_scope("zeros"):
        w_all[...] = jnp.zeros_like(w_all)
        src_all[...] = jnp.zeros_like(src_all)
        left[...] = jnp.zeros_like(left)
    score[...] = jnp.zeros_like(score)
    cls_all[me] = cls_z[zi, rows_of(x, kb), :]
    member = jnp.broadcast_to(grp_ref[...].astype(F32), (LANES, count)).T
    low = lane((count, LANES)) < coef
    low_kb = lane((kb, LANES)) < coef

    def pass_on(i):
        with jax.named_scope("came_down"):
            drain(z_rsem.at[i], bundle_size + ROW * kb // 2)
        across(i)
        cls_all[i * ROW + x] = cls_z[i, rows_of(x, kb), :]

    def amplitudes(tail):
        par = tail[half : half + 8] + tail[half + 8 : half + 16] + tail[half + 16 : half + 24]
        sel = jnp.broadcast_to(par[0:1], (count, LANES))
        for g in range(1, par.shape[0]):
            sel = jnp.where(member == g, par[g : g + 1], sel)
        other = pltpu.roll(sel, coef, 1)
        return jnp.where(low, sel, other), jnp.where(low, other, sel)

    def turned_over(a):
        return jnp.concatenate([a, jnp.zeros((LANES - count, LANES), F32)], axis=0).astype(BF16).T

    def prepare(g, i):
        b = g * ROW + i
        landing = bundle[b, count:].astype(F32)
        amp, wamp = amplitudes(landing)
        weighted = turned_over(wamp * bundle[b, 0:count].astype(F32))
        pen = -0.5 * (wamp * amp)
        pen_hi = pen.astype(BF16).astype(F32)
        pen = turned_over(jnp.where(low, pen_hi, pen - pen_hi))
        for k, piece in enumerate((weighted[:coef], weighted[coef:], pen[:coef], pen[:coef], pen[coef:])):
            for s in range(2):
                top = pl.multiple_of((5 * i + k) * LANES + s * coef, coef)
                w_all[g, pl.ds(top, coef), s * LANES : (s + 1) * LANES] = piece
        index = lax.broadcasted_iota(jnp.int32, (coef, LANES), 0).astype(F32).astype(BF16)
        ones, zeros = jnp.ones((coef, LANES), BF16), jnp.zeros((coef, LANES), BF16)
        for j in range(half):
            row = jnp.broadcast_to(landing[j : j + 1], (16, LANES)).astype(BF16)
            row = jnp.concatenate([row] * (coef // 16), axis=0)
            place[rows_of(b, coef), j * LANES : (j + 1) * LANES] = jnp.where(index == row, ones, zeros)

    def prepare_sources(pair):
        for i in range(2):
            b = pair * 2 + i
            amp, _ = amplitudes(bundle[b, count:].astype(F32))
            source = amp * bundle[b, 0:count].astype(F32)
            source_turned = pltpu.roll(source, coef, 1)
            power = amp * amp
            for s in range(2):
                top = s * LANES

                def keep(lower, upper):
                    return (jnp.where(low, lower, 0.0) if s == 0 else jnp.where(low, 0.0, upper)).astype(BF16)

                for t, kept in (
                    (2 * i, keep(source, source_turned)),
                    (2 * i + 1, keep(source_turned, source)),
                    (4 + i, keep(power, power)),
                ):
                    src_all[pair, top : top + count, t * LANES : (t + 1) * LANES] = kept
        for j in range(half):
            lanes = slice(j * LANES, (j + 1) * LANES)
            place_turned[pair, lanes, :] = place[rows_of(pair, 2 * coef), lanes].T

    def rotate(g):
        for i in range(4):
            image = cls_all[g * 4 + i].astype(F32)
            turned = pltpu.roll(image, coef, 1)
            if i % 2 == 0:
                re, im = jnp.where(low_kb, image, 0.0), jnp.where(low_kb, turned, 0.0)
            else:
                re, im = jnp.where(low_kb, 0.0, turned), jnp.where(low_kb, 0.0, image)
            top = (i // 2) * LANES
            left[g, 2 * i * kb : (2 * i + 1) * kb, top : top + LANES] = re.astype(BF16)
            left[g, (2 * i + 1) * kb : (2 * i + 2) * kb, top : top + LANES] = im.astype(BF16)
        lhs = left[g]
        for jj in range(half // 2):
            turned = jnp.dot(
                lhs, place[rows_of(g, 4 * coef), jj * 256 : (jj + 1) * 256], preferred_element_type=F32
            )
            for i in range(4):
                for t in range(2):
                    j = jj * 2 + t
                    re = turned[2 * i * kb : (2 * i + 1) * kb, t * LANES : (t + 1) * LANES]
                    im = turned[(2 * i + 1) * kb : (2 * i + 2) * kb, t * LANES : (t + 1) * LANES]
                    power = re * re + im * im
                    power_hi = power.astype(BF16)
                    power_lo = (power - power_hi.astype(F32)).astype(BF16)
                    to = slice(j * kb, (j + 1) * kb)
                    pieces = re.astype(BF16), im.astype(BF16), power_hi, power_lo, power_hi
                    for k, piece in enumerate(pieces):
                        at_lane = (5 * i + k) * LANES
                        rot_all[g, to, at_lane : at_lane + LANES] = piece

    def score_row(g):
        with jax.named_scope("arrive"):
            drain(x_rsem.at[g], (ROW - 1) * (bundle_size + kb // 2))
        with jax.named_scope("scores"):
            for k in range(1, ROW):
                prepare(g, lax.rem(x + k, ROW))
            rotate(g)
            score[...] += jnp.dot(rot_all[g], w_all[g], preferred_element_type=F32)

    prepare(zi, x)

    def down_later(i):
        pl.semaphore_wait(column_in.at[i], 1)
        down(i)

    with jax.named_scope("down_later"):
        each(zi + 1, SIDE, down_later)

    nearest = (0, 1, 2, 3), (1, 0, 1, 2), (2, 2, 0, 1), (3, 3, 3, 0)

    def place_of(step):
        return sum(
            jnp.where(jnp.logical_and(step == t, zi == k), nearest[t][k], 0) for t in range(SIDE) for k in range(SIDE)
        )

    def turn_of(step):
        @pl.when(step == 1)
        def _():
            for t in range(1, SIDE):
                pass_on(place_of(t))
                prepare(place_of(t), x)

        score_row(place_of(step))

    each(0, SIDE, turn_of)

    @pl.when(zi < SIDE - 1)
    def _():
        pl.semaphore_wait(others_in, (SIDE - 1 - zi) * (ROW - 1))

    def share(o):
        return score[rows_of(o, rows), :]

    share_size = rs_send.shape[1] + rs_scale.shape[1]
    for o in (1, 2, 0, 3):

        @pl.when(owner != o)
        def _():
            piece = share(o)
            one, two = piece[:, :LANES], piece[:, LANES:]
            most = jnp.max(jnp.maximum(one, two), axis=0, keepdims=True)
            least = jnp.min(jnp.minimum(one, two), axis=0, keepdims=True)
            middle = 0.5 * (most + least)
            reach = jnp.maximum(0.5 * (most - least), 1e-30)
            fit = 32767.0 / reach
            one = jnp.round((one - middle) * fit).astype(jnp.int32)
            two = jnp.round((two - middle) * fit).astype(jnp.int32)
            rs_send[o] = compact((one & 0xFFFF) | (two << 16))
            rs_scale[o] = jnp.concatenate([*spread(reach * (1.0 / 32767.0)), *spread(middle)], axis=0)

            @pl.when(jnp.logical_not(greets(home(o), zb)))
            def _():
                with jax.named_scope("owner_in"):
                    pl.semaphore_wait(owner_in.at[o], 1)

            with jax.named_scope("share_go"):
                remote(rs_send.at[o], rs_recv.at[zb], rs_ssem, rs_rsem.at[zb], far(home(o))).start()
                remote(rs_scale.at[o], rs_rscale.at[zb], rs_ssem, rs_rsem.at[zb], far(home(o))).start()

    @pl.when(zb == 1)
    def _():
        pl.semaphore_wait(first_in, 1)
        tell(owner_in.at[2], far(0))
        tell(owner_in.at[3], far(0))

    with jax.named_scope("sources"):
        each(0, NP // 2, prepare_sources)

    later = zb >= nb // 2

    def send_post(b):
        @pl.when(b != zb)
        def _():
            remote(ag_send, ag_recv.at[owner], ag_ssem, ag_rsem.at[owner], far(b)).start()

    @pl.when(owner < OWNERS)
    def _():
        own = share(owner)
        total = compact(own[:, :LANES]), compact(own[:, LANES:])

        def add_share(k, so_far):
            b = jnp.where(k < zb, k, k + 1)
            with jax.named_scope("share_in"):
                drain(rs_rsem.at[b], share_size)
            word = rs_recv[b]
            step = tiles(rs_rscale[b, 0:1], rs_rscale[b, 1:2], word.shape[0])
            middle = tiles(rs_rscale[b, 2:3], rs_rscale[b, 3:4], word.shape[0])
            return (
                so_far[0] + (((word << 16) >> 16).astype(F32) * step + middle),
                so_far[1] + ((word >> 16).astype(F32) * step + middle),
            )

        total_one, total_two = lax.fori_loop(0, nb - 1, add_share, total)
        peak = over_rows(jnp.maximum(total_one, total_two), jnp.maximum, jnp.max)
        shift = tiles(*spread(peak), total_one.shape[0])
        exp_one, exp_two = jnp.exp(total_one - shift), jnp.exp(total_two - shift)
        evidence = peak + jnp.log(over_rows(exp_one + exp_two, jnp.add, jnp.sum))
        top_send[...] = jnp.concatenate([peak, evidence], axis=0)
        lse_send[...] = evidence

        each(
            0,
            NP,
            lambda k: remote(
                lse_send, lse_first.at[owner * NP + me], ag_ssem, first_rsem, at(lax.rem(k, ROW), k // ROW)
            ).start(),
        )

        def send_top(b):
            @pl.when(b != zb)
            def _():
                remote(top_send, top_recv.at[owner], ag_ssem, top_rsem, far(b)).start()

        each(0, nb, send_top)
        one = (exp_one * 65535.0 + 0.5).astype(jnp.int32)
        two = (exp_two * 65535.0 + 0.5).astype(jnp.int32)
        ag_send[...] = (one & 0xFFFF) | (two << 16)


        def send_early(b):
            @pl.when(jnp.logical_not(jnp.logical_and(later, b == 1)))
            def _():
                send_post(b)

        each(0, nb - 2, send_early)
        ag_recv[owner] = ag_send[...]
        top_recv[owner] = top_send[...]

    with jax.named_scope("top_in"):

        @pl.when(owner < OWNERS)
        def _():
            drain(top_rsem, (OWNERS - 1) * top_send.shape[0])

        @pl.when(owner >= OWNERS)
        def _():
            drain(top_rsem, OWNERS * top_send.shape[0])

    def merged(parts, axis):
        most = jnp.max(parts, axis=axis, keepdims=True)
        return most + jnp.log(jnp.sum(jnp.exp(parts - most), axis=axis, keepdims=True))

    @pl.when(jnp.logical_and(owner < OWNERS, later))
    def _():
        each(nb - 2, nb, send_post)

    def pass_post(o, b):
        with jax.named_scope("post_in"):
            drain(ag_rsem.at[o], ag_send.shape[0])
        remote(ag_recv.at[o], ag_recv.at[o], pass_ssem, ag_rsem.at[o], far(b)).start()

    @pl.when(zb == 0)
    def _():
        for o in range(OWNERS):
            pass_post(o, nb - 1 if o < OWNERS // 2 else 1)

    @pl.when(zb == 0)
    def _():
        with jax.named_scope("first_in"):
            drain(first_rsem, OWNERS * NP)
        ev_ref[...] = merged(lse_first[...], 0)[0]

    @pl.when(zb > 0)
    def _():
        lse_own[...] = merged(jnp.concatenate([top_recv[o, 1:2] for o in range(OWNERS)], axis=0), 0)
        each(1, NP, lambda k: remote(lse_own, lse_all.at[me], lse_ssem, lse_rsem, mate(k)[1]).start())
        lse_all[me] = lse_own[...]
        with jax.named_scope("lse_in"):
            drain(lse_rsem, NP - 1)
        drain(lse_ssem, NP - 1)
        ev_ref[...] = merged(lse_all[...], 0)[0]

    evidence = ev_ref[...]
    used = lane((rows, LANES)) < count

    def take_post(o):
        passes = jnp.logical_and(zb == nb - 1, o < OWNERS // 2)

        @pl.when(passes)
        def _():
            pass_post(o, nb - 2)

        @pl.when(jnp.logical_not(jnp.logical_or(passes, jnp.logical_or(o == owner, zb == 0))))
        def _():
            with jax.named_scope("post_in"):
                drain(ag_rsem.at[o], ag_send.shape[0])

        word = expand(ag_recv[o])
        scale = jnp.exp(top_recv[o, 0:1] - evidence) * (1.0 / 65535.0)
        one = jnp.where(used, (word & 0xFFFF).astype(F32) * scale, 0.0)
        two = jnp.where(used, lax.shift_right_logical(word, 16).astype(F32) * scale, 0.0)
        post[rows_of(o, rows), 0:128] = one.astype(BF16)
        post[rows_of(o, rows), 128:256] = two.astype(BF16)

    each(0, OWNERS, take_post)

    def class_row(i):
        pairs_in = [i * (ROW // 2) + k for k in range(ROW // 2)]
        for k, pair in enumerate(pairs_in):
            frames = jnp.dot(post[...], src_all[pair], preferred_element_type=F32)
            for j in range(half):
                for t in range(6):
                    to = ((t // 2) * 3 + t % 2 if t < 4 else (t - 4) * 3 + 2) * kb
                    frame[k, to : to + kb, j * LANES : (j + 1) * LANES] = frames[
                        j * kb : (j + 1) * kb, t * LANES : (t + 1) * LANES
                    ].astype(BF16)
        low_out = lane((kb, LANES)) < coef
        for k, pair in enumerate(pairs_in):
            sums = jnp.zeros((6 * kb, LANES), F32)
            for at_depth in range(0, half * LANES, 2 * LANES):
                depth = slice(at_depth, at_depth + 2 * LANES)
                sums += jnp.dot(frame[k, :, depth], place_turned[pair, depth, :], preferred_element_type=F32)
            for t in range(2):
                mine = sums[3 * t * kb : 3 * (t + 1) * kb]
                other = pltpu.roll(mine, coef, 1)
                lower, upper = (mine, other) if t == 0 else (other, mine)
                out_send[i * ROW + 2 * k + t] = jnp.concatenate(
                    [
                        jnp.where(low_out, lower[:kb], upper[kb : 2 * kb]),
                        jnp.where(
                            low_out[: kb // 2], lower[2 * kb : 2 * kb + kb // 2], upper[2 * kb + kb // 2 : 3 * kb]
                        ),
                    ],
                    axis=0,
                ).astype(BF16)
        for k in range(ROW):
            to = lax.rem(x + k, ROW)
            b = i * ROW + to

            @pl.when(b != me)
            def _():
                remote(out_send.at[b], mine_ref.at[me], o_ssem, o_rsem, at(to, zb * SIDE + i)).start()

    with jax.named_scope("class_rows"):
        each(0, SIDE, class_row)
    mine_ref[me] = out_send[me]
    out_size = (NP - 1) * out_send.shape[1] // 2
    with jax.named_scope("take_out"):
        drain(o_rsem, out_size)

    @pl.when(core > 0)
    def _():
        pl.semaphore_wait(partner_in, 1)

    swap = remote(mine_ref, other_ref, c_ssem, c_rsem, partner)
    swap.start()

    drain(g_ssem, (SIDE - 1) * (bundle_size + ROW * kb // 2) + SIDE * (ROW - 1) * (bundle_size + kb // 2))
    drain(o_ssem, out_size)

    @pl.when(owner < OWNERS)
    def _():
        drain(rs_ssem, (OWNERS - 1) * share_size)
        drain(ag_ssem, (nb - 3) * ag_send.shape[0] + (nb - 1) * top_send.shape[0] + NP)

        @pl.when(later)
        def _():
            drain(ag_ssem, ag_send.shape[0])

    @pl.when(zb == 0)
    def _():
        drain(pass_ssem, OWNERS * ag_send.shape[0])

    @pl.when(zb == nb - 1)
    def _():
        drain(pass_ssem, OWNERS // 2 * ag_send.shape[0])

    @pl.when(owner >= OWNERS)
    def _():
        drain(rs_ssem, OWNERS * share_size)

    with jax.named_scope("swap"):
        swap.wait()


def finish(mine_ref, other_ref, ev_ref, cs_ref, cw_ref, out_ref):
    coef, kb = cw_ref.shape[0], cs_ref.shape[0] // NP
    halves = []
    for b in range(NP):
        both = mine_ref[b].astype(F32) + other_ref[b].astype(F32)
        cs_ref[b * kb : (b + 1) * kb, :] = both[:kb]
        halves.append(both[kb:])
    for first in range(0, NP, NP // 2):
        turned = jnp.concatenate(halves[first : first + NP // 2], axis=0).T
        for k in range(NP // 2):
            lanes = slice(k * kb // 2, (k + 1) * kb // 2)
            to = (first + k) * kb
            cw_ref[:, to : to + kb // 2] = turned[:coef, lanes]
            cw_ref[:, to + kb // 2 : to + kb] = turned[coef:, lanes]
    out_ref[...] = ev_ref[:, : out_ref.shape[1]]


def body(nz, particles, classes, ctf, sigma2, shell_of, rot_table, ctf_group):
    count, coef = particles.shape[0], shell_of.shape[0]
    classes_n, rotations = classes.shape[0], rot_table.shape[0]
    nb = nz // SIDE
    kb = classes_n // NP
    half = rotations // 2
    pairs = half * kb
    piece = pairs // OWNERS * 2 // 3
    dma = pltpu.SemaphoreType.DMA
    regular = pltpu.SemaphoreType.REGULAR
    vmem = pltpu.VMEM
    i32 = jnp.int32
    arrays = (
        particles,
        classes,
        ctf,
        sigma2.reshape(1, -1),
        shell_of.reshape(1, -1),
        rot_table,
        ctf_group.reshape(1, -1),
    )
    mine, other, evidence = pl.pallas_call(
        functools.partial(kernel, nz),
        out_shape=[
            jax.ShapeDtypeStruct((NP, 24, LANES), BF16),
            jax.ShapeDtypeStruct((NP, 24, LANES), BF16),
            jax.ShapeDtypeStruct((1, LANES), F32),
        ],
        in_specs=[pl.BlockSpec(memory_space=pltpu.HBM)] * 7,
        out_specs=[pl.BlockSpec(memory_space=vmem)] * 3,
        scratch_shapes=[
            *[vmem(a.shape, a.dtype) for a in arrays[1:]],
            vmem((NP, count + half + 24, LANES), BF16),
            vmem((SIDE, ROW * kb, LANES), BF16),
            vmem((NP, kb, LANES), BF16),
            vmem((NP * coef, half * LANES), BF16),
            vmem((NP // 2, half * LANES, 2 * coef), BF16),
            vmem((SIDE, ROW * 5 * LANES, 2 * LANES), BF16),
            vmem((NP // 2, 2 * LANES, 6 * LANES), BF16),
            vmem((NP // 4, 8 * kb, 4 * coef), BF16),
            vmem((SIDE, pairs, ROW * 5 * LANES), BF16),
            vmem((pairs, 2 * LANES), F32),
            vmem((OWNERS, piece, LANES), i32),
            vmem((OWNERS, 4, LANES), F32),
            vmem((nb, piece, LANES), i32),
            vmem((nb, 4, LANES), F32),
            vmem((piece, LANES), i32),
            vmem((2, LANES), F32),
            vmem((OWNERS, piece, LANES), i32),
            vmem((OWNERS, 2, LANES), F32),
            vmem((1, LANES), F32),
            vmem((OWNERS * NP, 1, LANES), F32),
            vmem((1, LANES), F32),
            vmem((NP, 1, LANES), F32),
            vmem((pairs, 2 * LANES), BF16),
            vmem((ROW // 2, 6 * kb, half * LANES), BF16),
            vmem((NP, 24, LANES), BF16),
            vmem((1152, 1, LANES), F32),
            dma((len(arrays) + 1,)),
            dma,
            dma((SIDE,)),
            dma((SIDE,)),
            dma,
            dma((nb,)),
            dma,
            dma,
            dma((OWNERS,)),
            *[dma] * 8,
            regular((SIDE,)),
            regular,
            regular((OWNERS,)),
            regular,
            regular,
        ],
        compiler_params=pltpu.CompilerParams(
            collective_id=0, has_side_effects=True, vmem_limit_bytes=40 * 1024 * 1024
        ),
        name="averaging",
    )(*[pltpu.with_memory_space_constraint(a, pltpu.HBM) for a in arrays])
    sums, weights, evidence = pl.pallas_call(
        finish,
        out_shape=[
            jax.ShapeDtypeStruct((classes_n, 2 * coef), F32),
            jax.ShapeDtypeStruct((coef, classes_n), F32),
            jax.ShapeDtypeStruct((1, count), F32),
        ],
        in_specs=[pl.BlockSpec(memory_space=vmem)] * 3,
        out_specs=[pl.BlockSpec(memory_space=vmem)] * 3,
        compiler_params=pltpu.CompilerParams(vmem_limit_bytes=4 * 1024 * 1024),
        name="finish",
    )(mine, other, evidence)
    return sums, weights.T, evidence.reshape(-1)


def solution(mesh):
    nz = mesh.shape["shell"] // ROW
    split = Mesh(mesh.devices.reshape(mesh.shape["groups"], ROW, nz, mesh.shape["batch"]), AXES)
    shell = ("x", "z")
    placed = (
        P(("groups", "batch"), shell),
        P("groups", shell),
        P("groups", shell),
        P("groups"),
        P(shell),
        P(None, shell),
        P(("groups", "batch")),
    )
    return jax.shard_map(
        functools.partial(body, nz),
        mesh=split,
        in_specs=placed,
        out_specs=(P("groups", shell), P("groups", shell), P(("groups", "batch"))),
        check_vma=False,
    )
```

```python
import functools

import jax
import jax.numpy as jnp
from jax import lax
from jax.experimental import pallas as pl
from jax.experimental.pallas import tpu as pltpu
from jax.sharding import Mesh
from jax.sharding import PartitionSpec as P

MESH = pl.DeviceIdType.MESH
ROW = 4
SIDE = 4
NP = ROW * SIDE
OUTWARD = 2, 1, 3
OWNERS = 4
LANES = 128
F32 = jnp.float32
BF16 = jnp.bfloat16
NT = (((1,), (1,)), ((), ()))
AXES = ("groups", "x", "z", "batch")


def lane(shape):
    return lax.broadcasted_iota(jnp.int32, shape, 1)


def compact(w):
    free = lane((8, LANES)) >= 80
    kept = []
    for r in range(0, w.shape[0], 48):
        a, b = w[r + 32 : r + 40], w[r + 40 : r + 48]
        kept += [
            jnp.where(free, pltpu.roll(a, 80, 1), w[r : r + 8]),
            jnp.where(free, pltpu.roll(a, 32, 1), w[r + 8 : r + 16]),
            jnp.where(free, pltpu.roll(b, 80, 1), w[r + 16 : r + 24]),
            jnp.where(free, pltpu.roll(b, 32, 1), w[r + 24 : r + 32]),
        ]
    return jnp.concatenate(kept, axis=0)


def expand(w):
    first = lane((8, LANES)) < 48
    whole = []
    for r in range(0, w.shape[0], 32):
        part = w[r : r + 32]
        whole += [
            part,
            jnp.where(first, pltpu.roll(part[0:8], 48, 1), pltpu.roll(part[8:16], 96, 1)),
            jnp.where(first, pltpu.roll(part[16:24], 48, 1), pltpu.roll(part[24:32], 96, 1)),
        ]
    return jnp.concatenate(whole, axis=0)


def spread(row):
    free = lane((1, LANES)) >= 80
    return jnp.where(free, pltpu.roll(row, 80, 1), row), jnp.where(free, pltpu.roll(row, 32, 1), row)


def tiles(even, odd, rows):
    e = jnp.broadcast_to(even, (8, LANES))
    o = jnp.broadcast_to(odd, (8, LANES))
    return jnp.concatenate([e, o] * (rows // 16), axis=0)


def over_rows(values, combine, reduce):
    split = [values[r : r + 8] for r in range(0, values.shape[0], 8)]
    even = reduce(functools.reduce(combine, split[0::2]), axis=0, keepdims=True)
    odd = reduce(functools.reduce(combine, split[1::2]), axis=0, keepdims=True)
    first = lane((1, LANES)) < 48
    moved = jnp.where(first, pltpu.roll(even, 48, 1), pltpu.roll(odd, 96, 1))
    return combine(combine(even, odd), moved)


def kernel(
    nz,
    part_hbm,
    cls_hbm,
    ctf_hbm,
    sig_hbm,
    sh_hbm,
    tab_hbm,
    grp_hbm,
    mine_ref,
    other_ref,
    ev_ref,
    cls_ref,
    ctf_ref,
    sig_ref,
    sh_ref,
    tab_ref,
    grp_ref,
    bundle,
    cls_z,
    cls_all,
    place,
    place_turned,
    w_all,
    src_all,
    left,
    rot_all,
    score,
    rs_send,
    rs_scale,
    rs_recv,
    rs_rscale,
    ag_send,
    top_send,
    ag_recv,
    top_recv,
    lse_send,
    lse_first,
    lse_own,
    lse_all,
    post,
    frame,
    out_send,
    sizes,
    in_sem,
    g_ssem,
    z_rsem,
    x_rsem,
    rs_ssem,
    rs_rsem,
    ag_ssem,
    pass_ssem,
    ag_rsem,
    top_rsem,
    first_rsem,
    lse_ssem,
    lse_rsem,
    o_ssem,
    o_rsem,
    c_ssem,
    c_rsem,
    column_in,
    others_in,
    owner_in,
    first_in,
    partner_in,
):
    nb = nz // SIDE
    count, coef = part_hbm.shape[0], ctf_ref.shape[1]
    kb = cls_all.shape[1]
    half = tab_ref.shape[0] // 2
    rows = half * kb // OWNERS
    group = lax.axis_index("groups")
    x = lax.axis_index("x")
    z = lax.axis_index("z")
    core = lax.axis_index("batch")
    zb, zi = z // SIDE, lax.rem(z, SIDE)
    me = zi * ROW + x
    def owns(b):
        return jnp.logical_or(
            jnp.logical_and(b >= 1, b < 3), jnp.logical_and(b >= nb - 3, b < nb - 1)
        )

    def home(o):
        return jnp.where(o < 2, o + 1, o + nb - 5)

    owner = jnp.where(owns(zb), jnp.where(zb < 3, zb - 1, zb - nb + 5), OWNERS)

    def greets(a, b):
        between = jnp.logical_and(jnp.logical_and(a >= 1, a < b), b < nb - 1)
        return jnp.logical_or(
            jnp.logical_and(between, jnp.logical_or(owns(a), owns(b))),
            jnp.logical_or(
                jnp.logical_and(b == 0, jnp.logical_and(a >= 1, a < 3)), jnp.logical_and(b == nb - 1, owns(a))
            ),
        )

    def at(x_, z_):
        return (group, x_, z_, core)

    def mate(k):
        i = lax.rem(me + k, NP)
        return i, at(lax.rem(i, ROW), zb * SIDE + i // ROW)

    def far(b):
        return at(x, b * SIDE + zi)

    partner = (group, x, z, 1 - core)

    def remote(src, dst, ssem, rsem, device):
        return pltpu.make_async_remote_copy(
            src_ref=src, dst_ref=dst, send_sem=ssem, recv_sem=rsem, device_id=device, device_id_type=MESH
        )

    def drain(semaphore, size):
        whole = sizes.at[0:size]
        remote(whole, whole, semaphore, semaphore, partner).wait_recv()

    def each(lower, upper, step):
        def turn(k, _):
            step(k)
            return 0

        lax.fori_loop(lower, upper, turn, 0)

    def tell(semaphore, device):
        pl.semaphore_signal(semaphore, inc=1, device_id=device, device_id_type=MESH)

    def rows_of(i, n):
        return pl.ds(pl.multiple_of(i * n, n), n)

    given = (ctf_hbm, sig_hbm, sh_hbm, tab_hbm, part_hbm, cls_hbm.at[rows_of(zi, ROW * kb)], cls_hbm, grp_hbm)
    taken = (ctf_ref, sig_ref, sh_ref, tab_ref, bundle.at[me, 0:count], cls_z.at[zi], cls_ref, grp_ref)
    loads = [pltpu.make_async_copy(a, b, in_sem.at[k]) for k, (a, b) in enumerate(zip(given, taken))]
    for load in loads:
        load.start()

    barrier = pltpu.get_barrier_semaphore()
    each(1, ROW, lambda k: tell(barrier, at(lax.rem(x + k, ROW), z)))
    each((zi + 1) * ROW, NP, lambda i: tell(barrier, at(lax.rem(i, ROW), zb * SIDE + i // ROW)))

    @pl.when(core > 0)
    def _():
        tell(barrier, partner)

    def greet(b):
        @pl.when(greets(zb, b))
        def _():
            tell(barrier, far(b))

    each(0, nb, greet)
    for load in loads[:4]:
        load.wait()

    levels = sig_ref.shape[1]
    pick = lax.broadcasted_iota(jnp.int32, (levels, coef), 0) == sh_ref[...]
    noise_of = jnp.broadcast_to(sig_ref[...], (coef, levels)).T
    noise = jnp.sum(jnp.where(pick, noise_of, 0.0), axis=0, keepdims=True)
    ctf = ctf_ref[...]
    par = jnp.concatenate([ctf, (1.0 / noise) * ctf], axis=1)
    par_high = par.astype(BF16).astype(F32)
    par_mid = (par - par_high).astype(BF16).astype(F32)
    offset = (x * nz + z) * coef
    table = (tab_ref[...] - offset).astype(F32)
    table = jnp.concatenate([table[:half], table[half:]], axis=1)
    bundle[me, count:] = jnp.concatenate([table, par_high, par_mid, (par - par_high) - par_mid], axis=0).astype(BF16)
    for load in loads[4:]:
        load.wait()
    with jax.named_scope("barrier"):
        greeted = sum(jnp.where(greets(b, zb), 1, 0) for b in range(nb))
        pl.semaphore_wait(barrier, ROW - 1 + zi * ROW + jnp.where(core > 0, 0, 1) + greeted)

    def down(i):
        device = at(x, zb * SIDE + i)
        remote(bundle.at[me], bundle.at[me], g_ssem, z_rsem.at[zi], device).start()
        remote(cls_ref.at[rows_of(i, ROW * kb)], cls_z.at[zi], g_ssem, z_rsem.at[zi], device).start()

    def across(i):
        b = i * ROW + x
        for k in OUTWARD:
            to = lax.rem(x + k, ROW)
            device = at(to, z)
            remote(bundle.at[b], bundle.at[b], g_ssem, x_rsem.at[i], device).start()
            remote(cls_z.at[i, rows_of(to, kb)], cls_all.at[b], g_ssem, x_rsem.at[i], device).start()

    bundle_size = bundle.shape[1] // 2
    def tell_above(i):
        tell(column_in.at[zi], at(x, zb * SIDE + i))
        each(1, ROW, lambda k: tell(others_in, at(lax.rem(x + k, ROW), zb * SIDE + i)))

    each(0, zi, tell_above)
    each(0, zi, lambda k: down(zi - 1 - k))
    across(zi)

    @pl.when(owner < OWNERS)
    def _():
        def tell_earlier(b):
            @pl.when(greets(b, zb))
            def _():
                tell(owner_in.at[owner], far(b))

        each(0, nb, tell_earlier)

    @pl.when(zb == 0)
    def _():
        tell(first_in, far(1))

    @pl.when(core == 0)
    def _():
        tell(partner_in, partner)

    with jax.named_scope("zeros"):
        w_all[...] = jnp.zeros_like(w_all)
        src_all[...] = jnp.zeros_like(src_all)
        left[...] = jnp.zeros_like(left)
    score[...] = jnp.zeros_like(score)
    cls_all[me] = cls_z[zi, rows_of(x, kb), :]
    member = jnp.broadcast_to(grp_ref[...].astype(F32), (LANES, count)).T
    low = lane((count, LANES)) < coef
    low_kb = lane((kb, LANES)) < coef

    def pass_on(i):
        with jax.named_scope("came_down"):
            drain(z_rsem.at[i], bundle_size + ROW * kb // 2)
        across(i)
        cls_all[i * ROW + x] = cls_z[i, rows_of(x, kb), :]

    def amplitudes(tail):
        par = tail[half : half + 8] + tail[half + 8 : half + 16] + tail[half + 16 : half + 24]
        sel = jnp.broadcast_to(par[0:1], (count, LANES))
        for g in range(1, par.shape[0]):
            sel = jnp.where(member == g, par[g : g + 1], sel)
        other = pltpu.roll(sel, coef, 1)
        return jnp.where(low, sel, other), jnp.where(low, other, sel)

    def turned_over(a):
        return jnp.concatenate([a, jnp.zeros((LANES - count, LANES), F32)], axis=0).astype(BF16).T

    def prepare(g, i):
        b = g * ROW + i
        landing = bundle[b, count:].astype(F32)
        amp, wamp = amplitudes(landing)
        weighted = turned_over(wamp * bundle[b, 0:count].astype(F32))
        pen = -0.5 * (wamp * amp)
        pen_hi = pen.astype(BF16).astype(F32)
        pen = turned_over(jnp.where(low, pen_hi, pen - pen_hi))
        for k, piece in enumerate((weighted[:coef], weighted[coef:], pen[:coef], pen[:coef], pen[coef:])):
            for s in range(2):
                top = pl.multiple_of((5 * i + k) * LANES + s * coef, coef)
                w_all[g, pl.ds(top, coef), s * LANES : (s + 1) * LANES] = piece
        index = lax.broadcasted_iota(jnp.int32, (coef, LANES), 0).astype(F32).astype(BF16)
        ones, zeros = jnp.ones((coef, LANES), BF16), jnp.zeros((coef, LANES), BF16)
        for j in range(half):
            row = jnp.broadcast_to(landing[j : j + 1], (16, LANES)).astype(BF16)
            row = jnp.concatenate([row] * (coef // 16), axis=0)
            place[rows_of(b, coef), j * LANES : (j + 1) * LANES] = jnp.where(index == row, ones, zeros)

    def prepare_sources(pair):
        for i in range(2):
            b = pair * 2 + i
            amp, _ = amplitudes(bundle[b, count:].astype(F32))
            source = amp * bundle[b, 0:count].astype(F32)
            source_turned = pltpu.roll(source, coef, 1)
            power = amp * amp
            for s in range(2):
                top = s * LANES

                def keep(lower, upper):
                    return (jnp.where(low, lower, 0.0) if s == 0 else jnp.where(low, 0.0, upper)).astype(BF16)

                for t, kept in (
                    (2 * i, keep(source, source_turned)),
                    (2 * i + 1, keep(source_turned, source)),
                    (4 + i, keep(power, power)),
                ):
                    src_all[pair, top : top + count, t * LANES : (t + 1) * LANES] = kept
        for j in range(half):
            lanes = slice(j * LANES, (j + 1) * LANES)
            place_turned[pair, lanes, :] = place[rows_of(pair, 2 * coef), lanes].T

    def rotate(g):
        for i in range(4):
            image = cls_all[g * 4 + i].astype(F32)
            turned = pltpu.roll(image, coef, 1)
            if i % 2 == 0:
                re, im = jnp.where(low_kb, image, 0.0), jnp.where(low_kb, turned, 0.0)
            else:
                re, im = jnp.where(low_kb, 0.0, turned), jnp.where(low_kb, 0.0, image)
            top = (i // 2) * LANES
            left[g, 2 * i * kb : (2 * i + 1) * kb, top : top + LANES] = re.astype(BF16)
            left[g, (2 * i + 1) * kb : (2 * i + 2) * kb, top : top + LANES] = im.astype(BF16)
        lhs = left[g]
        for jj in range(half // 2):
            turned = jnp.dot(
                lhs, place[rows_of(g, 4 * coef), jj * 256 : (jj + 1) * 256], preferred_element_type=F32
            )
            for i in range(4):
                for t in range(2):
                    j = jj * 2 + t
                    re = turned[2 * i * kb : (2 * i + 1) * kb, t * LANES : (t + 1) * LANES]
                    im = turned[(2 * i + 1) * kb : (2 * i + 2) * kb, t * LANES : (t + 1) * LANES]
                    power = re * re + im * im
                    power_hi = power.astype(BF16)
                    power_lo = (power - power_hi.astype(F32)).astype(BF16)
                    to = slice(j * kb, (j + 1) * kb)
                    pieces = re.astype(BF16), im.astype(BF16), power_hi, power_lo, power_hi
                    for k, piece in enumerate(pieces):
                        at_lane = (5 * i + k) * LANES
                        rot_all[g, to, at_lane : at_lane + LANES] = piece

    def score_row(g):
        with jax.named_scope("arrive"):
            drain(x_rsem.at[g], (ROW - 1) * (bundle_size + kb // 2))
        with jax.named_scope("scores"):
            for k in range(1, ROW):
                prepare(g, lax.rem(x + k, ROW))
            rotate(g)
            score[...] += jnp.dot(rot_all[g], w_all[g], preferred_element_type=F32)

    prepare(zi, x)

    def down_later(i):
        pl.semaphore_wait(column_in.at[i], 1)
        down(i)

    with jax.named_scope("down_later"):
        each(zi + 1, SIDE, down_later)

    nearest = (0, 1, 2, 3), (1, 0, 1, 2), (2, 2, 0, 1), (3, 3, 3, 0)

    def place_of(step):
        return sum(
            jnp.where(jnp.logical_and(step == t, zi == k), nearest[t][k], 0) for t in range(SIDE) for k in range(SIDE)
        )

    def turn_of(step):
        @pl.when(step == 1)
        def _():
            for t in range(1, SIDE):
                pass_on(place_of(t))
                prepare(place_of(t), x)

        score_row(place_of(step))

    each(0, SIDE, turn_of)

    @pl.when(zi < SIDE - 1)
    def _():
        pl.semaphore_wait(others_in, (SIDE - 1 - zi) * (ROW - 1))

    def share(o):
        return score[rows_of(o, rows), :]

    share_size = rs_send.shape[1] + rs_scale.shape[1]
    for o in (1, 2, 0, 3):

        @pl.when(owner != o)
        def _():
            piece = share(o)
            one, two = piece[:, :LANES], piece[:, LANES:]
            most = jnp.max(jnp.maximum(one, two), axis=0, keepdims=True)
            least = jnp.min(jnp.minimum(one, two), axis=0, keepdims=True)
            middle = 0.5 * (most + least)
            reach = jnp.maximum(0.5 * (most - least), 1e-30)
            fit = 32767.0 / reach
            one = jnp.round((one - middle) * fit).astype(jnp.int32)
            two = jnp.round((two - middle) * fit).astype(jnp.int32)
            rs_send[o] = compact((one & 0xFFFF) | (two << 16))
            rs_scale[o] = jnp.concatenate([*spread(reach * (1.0 / 32767.0)), *spread(middle)], axis=0)

            @pl.when(jnp.logical_not(greets(home(o), zb)))
            def _():
                with jax.named_scope("owner_in"):
                    pl.semaphore_wait(owner_in.at[o], 1)

            with jax.named_scope("share_go"):
                remote(rs_send.at[o], rs_recv.at[zb], rs_ssem, rs_rsem.at[zb], far(home(o))).start()
                remote(rs_scale.at[o], rs_rscale.at[zb], rs_ssem, rs_rsem.at[zb], far(home(o))).start()

    @pl.when(zb == 1)
    def _():
        pl.semaphore_wait(first_in, 1)
        tell(owner_in.at[2], far(0))
        tell(owner_in.at[3], far(0))

    with jax.named_scope("sources"):
        each(0, NP // 2, prepare_sources)

    later = zb >= nb // 2

    def send_post(b):
        @pl.when(b != zb)
        def _():
            remote(ag_send, ag_recv.at[owner], ag_ssem, ag_rsem.at[owner], far(b)).start()

    @pl.when(owner < OWNERS)
    def _():
        own = share(owner)
        total = compact(own[:, :LANES]), compact(own[:, LANES:])

        def add_share(k, so_far):
            b = jnp.where(k < zb, k, k + 1)
            with jax.named_scope("share_in"):
                drain(rs_rsem.at[b], share_size)
            word = rs_recv[b]
            step = tiles(rs_rscale[b, 0:1], rs_rscale[b, 1:2], word.shape[0])
            middle = tiles(rs_rscale[b, 2:3], rs_rscale[b, 3:4], word.shape[0])
            return (
                so_far[0] + (((word << 16) >> 16).astype(F32) * step + middle),
                so_far[1] + ((word >> 16).astype(F32) * step + middle),
            )

        total_one, total_two = lax.fori_loop(0, nb - 1, add_share, total)
        peak = over_rows(jnp.maximum(total_one, total_two), jnp.maximum, jnp.max)
        shift = tiles(*spread(peak), total_one.shape[0])
        exp_one, exp_two = jnp.exp(total_one - shift), jnp.exp(total_two - shift)
        evidence = peak + jnp.log(over_rows(exp_one + exp_two, jnp.add, jnp.sum))
        top_send[...] = jnp.concatenate([peak, evidence], axis=0)
        lse_send[...] = evidence

        each(
            0,
            NP,
            lambda k: remote(
                lse_send, lse_first.at[owner * NP + me], ag_ssem, first_rsem, at(lax.rem(k, ROW), k // ROW)
            ).start(),
        )

        def send_top(b):
            @pl.when(b != zb)
            def _():
                remote(top_send, top_recv.at[owner], ag_ssem, top_rsem, far(b)).start()

        each(0, nb, send_top)
        one = (exp_one * 65535.0 + 0.5).astype(jnp.int32)
        two = (exp_two * 65535.0 + 0.5).astype(jnp.int32)
        ag_send[...] = (one & 0xFFFF) | (two << 16)


        def send_early(b):
            @pl.when(jnp.logical_not(jnp.logical_and(later, b == 1)))
            def _():
                send_post(b)

        each(0, nb - 2, send_early)
        ag_recv[owner] = ag_send[...]
        top_recv[owner] = top_send[...]

    with jax.named_scope("top_in"):

        @pl.when(owner < OWNERS)
        def _():
            drain(top_rsem, (OWNERS - 1) * top_send.shape[0])

        @pl.when(owner >= OWNERS)
        def _():
            drain(top_rsem, OWNERS * top_send.shape[0])

    def merged(parts, axis):
        most = jnp.max(parts, axis=axis, keepdims=True)
        return most + jnp.log(jnp.sum(jnp.exp(parts - most), axis=axis, keepdims=True))

    @pl.when(jnp.logical_and(owner < OWNERS, later))
    def _():
        each(nb - 2, nb, send_post)

    def pass_post(o, b):
        with jax.named_scope("post_in"):
            drain(ag_rsem.at[o], ag_send.shape[0])
        remote(ag_recv.at[o], ag_recv.at[o], pass_ssem, ag_rsem.at[o], far(b)).start()

    @pl.when(zb == 0)
    def _():
        for o in range(OWNERS):
            pass_post(o, nb - 1 if o < OWNERS // 2 else 1)

    @pl.when(zb == 0)
    def _():
        with jax.named_scope("first_in"):
            drain(first_rsem, OWNERS * NP)
        ev_ref[...] = merged(lse_first[...], 0)[0]

    @pl.when(zb > 0)
    def _():
        lse_own[...] = merged(jnp.concatenate([top_recv[o, 1:2] for o in range(OWNERS)], axis=0), 0)
        each(1, NP, lambda k: remote(lse_own, lse_all.at[me], lse_ssem, lse_rsem, mate(k)[1]).start())
        lse_all[me] = lse_own[...]
        with jax.named_scope("lse_in"):
            drain(lse_rsem, NP - 1)
        drain(lse_ssem, NP - 1)
        ev_ref[...] = merged(lse_all[...], 0)[0]

    evidence = ev_ref[...]
    used = lane((rows, LANES)) < count

    def take_post(o):
        passes = jnp.logical_and(zb == nb - 1, o < OWNERS // 2)

        @pl.when(passes)
        def _():
            pass_post(o, nb - 2)

        @pl.when(jnp.logical_not(jnp.logical_or(passes, jnp.logical_or(o == owner, zb == 0))))
        def _():
            with jax.named_scope("post_in"):
                drain(ag_rsem.at[o], ag_send.shape[0])

        word = expand(ag_recv[o])
        scale = jnp.exp(top_recv[o, 0:1] - evidence) * (1.0 / 65535.0)
        one = jnp.where(used, (word & 0xFFFF).astype(F32) * scale, 0.0)
        two = jnp.where(used, lax.shift_right_logical(word, 16).astype(F32) * scale, 0.0)
        post[rows_of(o, rows), 0:128] = one.astype(BF16)
        post[rows_of(o, rows), 128:256] = two.astype(BF16)

    each(0, OWNERS, take_post)

    def class_row(i):
        pairs_in = [i * (ROW // 2) + k for k in range(ROW // 2)]
        for k, pair in enumerate(pairs_in):
            frames = jnp.dot(post[...], src_all[pair], preferred_element_type=F32)
            for j in range(half):
                for t in range(6):
                    to = ((t // 2) * 3 + t % 2 if t < 4 else (t - 4) * 3 + 2) * kb
                    frame[k, to : to + kb, j * LANES : (j + 1) * LANES] = frames[
                        j * kb : (j + 1) * kb, t * LANES : (t + 1) * LANES
                    ].astype(BF16)
        low_out = lane((kb, LANES)) < coef
        for k, pair in enumerate(pairs_in):
            sums = jnp.zeros((6 * kb, LANES), F32)
            for at_depth in range(0, half * LANES, 2 * LANES):
                depth = slice(at_depth, at_depth + 2 * LANES)
                sums += jnp.dot(frame[k, :, depth], place_turned[pair, depth, :], preferred_element_type=F32)
            for t in range(2):
                mine = sums[3 * t * kb : 3 * (t + 1) * kb]
                other = pltpu.roll(mine, coef, 1)
                lower, upper = (mine, other) if t == 0 else (other, mine)
                out_send[i * ROW + 2 * k + t] = jnp.concatenate(
                    [
                        jnp.where(low_out, lower[:kb], upper[kb : 2 * kb]),
                        jnp.where(
                            low_out[: kb // 2], lower[2 * kb : 2 * kb + kb // 2], upper[2 * kb + kb // 2 : 3 * kb]
                        ),
                    ],
                    axis=0,
                ).astype(BF16)
            nearer = jnp.where(lax.rem(x + 2, ROW) == 2 * k + 1, 0, 1)
            for t in range(2):
                to = 2 * k + (1 - nearer if t == 0 else nearer)
                b = i * ROW + to

                @pl.when(b != me)
                def _():
                    remote(out_send.at[b], mine_ref.at[me], o_ssem, o_rsem, at(to, zb * SIDE + i)).start()

    with jax.named_scope("class_rows"):
        each(0, SIDE, class_row)
    mine_ref[me] = out_send[me]
    out_size = (NP - 1) * out_send.shape[1] // 2
    with jax.named_scope("take_out"):
        drain(o_rsem, out_size)

    @pl.when(core > 0)
    def _():
        pl.semaphore_wait(partner_in, 1)

    swap = remote(mine_ref, other_ref, c_ssem, c_rsem, partner)
    swap.start()

    drain(g_ssem, (SIDE - 1) * (bundle_size + ROW * kb // 2) + SIDE * (ROW - 1) * (bundle_size + kb // 2))
    drain(o_ssem, out_size)

    @pl.when(owner < OWNERS)
    def _():
        drain(rs_ssem, (OWNERS - 1) * share_size)
        drain(ag_ssem, (nb - 3) * ag_send.shape[0] + (nb - 1) * top_send.shape[0] + NP)

        @pl.when(later)
        def _():
            drain(ag_ssem, ag_send.shape[0])

    @pl.when(zb == 0)
    def _():
        drain(pass_ssem, OWNERS * ag_send.shape[0])

    @pl.when(zb == nb - 1)
    def _():
        drain(pass_ssem, OWNERS // 2 * ag_send.shape[0])

    @pl.when(owner >= OWNERS)
    def _():
        drain(rs_ssem, OWNERS * share_size)

    with jax.named_scope("swap"):
        swap.wait()


def finish(mine_ref, other_ref, ev_ref, cs_ref, cw_ref, out_ref):
    coef, kb = cw_ref.shape[0], cs_ref.shape[0] // NP
    halves = []
    for b in range(NP):
        both = mine_ref[b].astype(F32) + other_ref[b].astype(F32)
        cs_ref[b * kb : (b + 1) * kb, :] = both[:kb]
        halves.append(both[kb:])
    for first in range(0, NP, NP // 2):
        turned = jnp.concatenate(halves[first : first + NP // 2], axis=0).T
        for k in range(NP // 2):
            lanes = slice(k * kb // 2, (k + 1) * kb // 2)
            to = (first + k) * kb
            cw_ref[:, to : to + kb // 2] = turned[:coef, lanes]
            cw_ref[:, to + kb // 2 : to + kb] = turned[coef:, lanes]
    out_ref[...] = ev_ref[:, : out_ref.shape[1]]


def body(nz, particles, classes, ctf, sigma2, shell_of, rot_table, ctf_group):
    count, coef = particles.shape[0], shell_of.shape[0]
    classes_n, rotations = classes.shape[0], rot_table.shape[0]
    nb = nz // SIDE
    kb = classes_n // NP
    half = rotations // 2
    pairs = half * kb
    piece = pairs // OWNERS * 2 // 3
    dma = pltpu.SemaphoreType.DMA
    regular = pltpu.SemaphoreType.REGULAR
    vmem = pltpu.VMEM
    i32 = jnp.int32
    arrays = (
        particles,
        classes,
        ctf,
        sigma2.reshape(1, -1),
        shell_of.reshape(1, -1),
        rot_table,
        ctf_group.reshape(1, -1),
    )
    mine, other, evidence = pl.pallas_call(
        functools.partial(kernel, nz),
        out_shape=[
            jax.ShapeDtypeStruct((NP, 24, LANES), BF16),
            jax.ShapeDtypeStruct((NP, 24, LANES), BF16),
            jax.ShapeDtypeStruct((1, LANES), F32),
        ],
        in_specs=[pl.BlockSpec(memory_space=pltpu.HBM)] * 7,
        out_specs=[pl.BlockSpec(memory_space=vmem)] * 3,
        scratch_shapes=[
            *[vmem(a.shape, a.dtype) for a in arrays[1:]],
            vmem((NP, count + half + 24, LANES), BF16),
            vmem((SIDE, ROW * kb, LANES), BF16),
            vmem((NP, kb, LANES), BF16),
            vmem((NP * coef, half * LANES), BF16),
            vmem((NP // 2, half * LANES, 2 * coef), BF16),
            vmem((SIDE, ROW * 5 * LANES, 2 * LANES), BF16),
            vmem((NP // 2, 2 * LANES, 6 * LANES), BF16),
            vmem((NP // 4, 8 * kb, 4 * coef), BF16),
            vmem((SIDE, pairs, ROW * 5 * LANES), BF16),
            vmem((pairs, 2 * LANES), F32),
            vmem((OWNERS, piece, LANES), i32),
            vmem((OWNERS, 4, LANES), F32),
            vmem((nb, piece, LANES), i32),
            vmem((nb, 4, LANES), F32),
            vmem((piece, LANES), i32),
            vmem((2, LANES), F32),
            vmem((OWNERS, piece, LANES), i32),
            vmem((OWNERS, 2, LANES), F32),
            vmem((1, LANES), F32),
            vmem((OWNERS * NP, 1, LANES), F32),
            vmem((1, LANES), F32),
            vmem((NP, 1, LANES), F32),
            vmem((pairs, 2 * LANES), BF16),
            vmem((ROW // 2, 6 * kb, half * LANES), BF16),
            vmem((NP, 24, LANES), BF16),
            vmem((1152, 1, LANES), F32),
            dma((len(arrays) + 1,)),
            dma,
            dma((SIDE,)),
            dma((SIDE,)),
            dma,
            dma((nb,)),
            dma,
            dma,
            dma((OWNERS,)),
            *[dma] * 8,
            regular((SIDE,)),
            regular,
            regular((OWNERS,)),
            regular,
            regular,
        ],
        compiler_params=pltpu.CompilerParams(
            collective_id=0, has_side_effects=True, vmem_limit_bytes=40 * 1024 * 1024
        ),
        name="averaging",
    )(*[pltpu.with_memory_space_constraint(a, pltpu.HBM) for a in arrays])
    sums, weights, evidence = pl.pallas_call(
        finish,
        out_shape=[
            jax.ShapeDtypeStruct((classes_n, 2 * coef), F32),
            jax.ShapeDtypeStruct((coef, classes_n), F32),
            jax.ShapeDtypeStruct((1, count), F32),
        ],
        in_specs=[pl.BlockSpec(memory_space=vmem)] * 3,
        out_specs=[pl.BlockSpec(memory_space=vmem)] * 3,
        compiler_params=pltpu.CompilerParams(vmem_limit_bytes=4 * 1024 * 1024),
        name="finish",
    )(mine, other, evidence)
    return sums, weights.T, evidence.reshape(-1)


def solution(mesh):
    nz = mesh.shape["shell"] // ROW
    split = Mesh(mesh.devices.reshape(mesh.shape["groups"], ROW, nz, mesh.shape["batch"]), AXES)
    shell = ("x", "z")
    placed = (
        P(("groups", "batch"), shell),
        P("groups", shell),
        P("groups", shell),
        P("groups"),
        P(shell),
        P(None, shell),
        P(("groups", "batch")),
    )
    return jax.shard_map(
        functools.partial(body, nz),
        mesh=split,
        in_specs=placed,
        out_specs=(P("groups", shell), P("groups", shell), P(("groups", "batch"))),
        check_vma=False,
    )
```

```python
import functools

import jax
import jax.numpy as jnp
from jax import lax
from jax.experimental import pallas as pl
from jax.experimental.pallas import tpu as pltpu
from jax.sharding import Mesh
from jax.sharding import PartitionSpec as P

MESH = pl.DeviceIdType.MESH
ROW = 4
SIDE = 4
NP = ROW * SIDE
OUTWARD = 2, 1, 3
OWNERS = 4
LANES = 128
F32 = jnp.float32
BF16 = jnp.bfloat16
NT = (((1,), (1,)), ((), ()))
AXES = ("groups", "x", "z", "batch")


def lane(shape):
    return lax.broadcasted_iota(jnp.int32, shape, 1)


def compact(w):
    free = lane((8, LANES)) >= 80
    kept = []
    for r in range(0, w.shape[0], 48):
        a, b = w[r + 32 : r + 40], w[r + 40 : r + 48]
        kept += [
            jnp.where(free, pltpu.roll(a, 80, 1), w[r : r + 8]),
            jnp.where(free, pltpu.roll(a, 32, 1), w[r + 8 : r + 16]),
            jnp.where(free, pltpu.roll(b, 80, 1), w[r + 16 : r + 24]),
            jnp.where(free, pltpu.roll(b, 32, 1), w[r + 24 : r + 32]),
        ]
    return jnp.concatenate(kept, axis=0)


def expand(w):
    first = lane((8, LANES)) < 48
    whole = []
    for r in range(0, w.shape[0], 32):
        part = w[r : r + 32]
        whole += [
            part,
            jnp.where(first, pltpu.roll(part[0:8], 48, 1), pltpu.roll(part[8:16], 96, 1)),
            jnp.where(first, pltpu.roll(part[16:24], 48, 1), pltpu.roll(part[24:32], 96, 1)),
        ]
    return jnp.concatenate(whole, axis=0)


def spread(row):
    free = lane((1, LANES)) >= 80
    return jnp.where(free, pltpu.roll(row, 80, 1), row), jnp.where(free, pltpu.roll(row, 32, 1), row)


def tiles(even, odd, rows):
    e = jnp.broadcast_to(even, (8, LANES))
    o = jnp.broadcast_to(odd, (8, LANES))
    return jnp.concatenate([e, o] * (rows // 16), axis=0)


def over_rows(values, combine, reduce):
    split = [values[r : r + 8] for r in range(0, values.shape[0], 8)]
    even = reduce(functools.reduce(combine, split[0::2]), axis=0, keepdims=True)
    odd = reduce(functools.reduce(combine, split[1::2]), axis=0, keepdims=True)
    first = lane((1, LANES)) < 48
    moved = jnp.where(first, pltpu.roll(even, 48, 1), pltpu.roll(odd, 96, 1))
    return combine(combine(even, odd), moved)


def kernel(
    nz,
    part_hbm,
    cls_hbm,
    ctf_hbm,
    sig_hbm,
    sh_hbm,
    tab_hbm,
    grp_hbm,
    mine_ref,
    other_ref,
    ev_ref,
    cls_ref,
    ctf_ref,
    sig_ref,
    sh_ref,
    tab_ref,
    grp_ref,
    bundle,
    cls_z,
    cls_all,
    place,
    place_turned,
    w_all,
    src_all,
    left,
    rot_all,
    score,
    rs_send,
    rs_scale,
    rs_recv,
    rs_rscale,
    ag_send,
    top_send,
    ag_recv,
    top_recv,
    lse_send,
    lse_first,
    lse_own,
    lse_all,
    raw,
    post,
    frame,
    out_send,
    sizes,
    in_sem,
    g_ssem,
    z_rsem,
    x_rsem,
    rs_ssem,
    rs_rsem,
    ag_ssem,
    pass_ssem,
    ag_rsem,
    top_rsem,
    first_rsem,
    lse_ssem,
    lse_rsem,
    o_ssem,
    o_rsem,
    c_ssem,
    c_rsem,
    column_in,
    others_in,
    owner_in,
    first_in,
    partner_in,
):
    nb = nz // SIDE
    count, coef = part_hbm.shape[0], ctf_ref.shape[1]
    kb = cls_all.shape[1]
    half = tab_ref.shape[0] // 2
    rows = half * kb // OWNERS
    group = lax.axis_index("groups")
    x = lax.axis_index("x")
    z = lax.axis_index("z")
    core = lax.axis_index("batch")
    zb, zi = z // SIDE, lax.rem(z, SIDE)
    me = zi * ROW + x
    def owns(b):
        return jnp.logical_or(
            jnp.logical_and(b >= 1, b < 3), jnp.logical_and(b >= nb - 3, b < nb - 1)
        )

    def home(o):
        return jnp.where(o < 2, o + 1, o + nb - 5)

    owner = jnp.where(owns(zb), jnp.where(zb < 3, zb - 1, zb - nb + 5), OWNERS)

    def greets(a, b):
        between = jnp.logical_and(jnp.logical_and(a >= 1, a < b), b < nb - 1)
        return jnp.logical_or(
            jnp.logical_and(between, jnp.logical_or(owns(a), owns(b))),
            jnp.logical_or(
                jnp.logical_and(b == 0, jnp.logical_and(a >= 1, a < 3)), jnp.logical_and(b == nb - 1, owns(a))
            ),
        )

    def at(x_, z_):
        return (group, x_, z_, core)

    def mate(k):
        i = lax.rem(me + k, NP)
        return i, at(lax.rem(i, ROW), zb * SIDE + i // ROW)

    def far(b):
        return at(x, b * SIDE + zi)

    partner = (group, x, z, 1 - core)

    def remote(src, dst, ssem, rsem, device):
        return pltpu.make_async_remote_copy(
            src_ref=src, dst_ref=dst, send_sem=ssem, recv_sem=rsem, device_id=device, device_id_type=MESH
        )

    def drain(semaphore, size):
        whole = sizes.at[0:size]
        remote(whole, whole, semaphore, semaphore, partner).wait_recv()

    def each(lower, upper, step):
        def turn(k, _):
            step(k)
            return 0

        lax.fori_loop(lower, upper, turn, 0)

    def tell(semaphore, device):
        pl.semaphore_signal(semaphore, inc=1, device_id=device, device_id_type=MESH)

    def rows_of(i, n):
        return pl.ds(pl.multiple_of(i * n, n), n)

    given = (ctf_hbm, sig_hbm, sh_hbm, tab_hbm, part_hbm, cls_hbm.at[rows_of(zi, ROW * kb)], cls_hbm, grp_hbm)
    taken = (ctf_ref, sig_ref, sh_ref, tab_ref, bundle.at[me, 0:count], cls_z.at[zi], cls_ref, grp_ref)
    loads = [pltpu.make_async_copy(a, b, in_sem.at[k]) for k, (a, b) in enumerate(zip(given, taken))]
    for load in loads:
        load.start()

    barrier = pltpu.get_barrier_semaphore()
    each(1, ROW, lambda k: tell(barrier, at(lax.rem(x + k, ROW), z)))
    each((zi + 1) * ROW, NP, lambda i: tell(barrier, at(lax.rem(i, ROW), zb * SIDE + i // ROW)))

    @pl.when(core > 0)
    def _():
        tell(barrier, partner)

    def greet(b):
        @pl.when(greets(zb, b))
        def _():
            tell(barrier, far(b))

    each(0, nb, greet)
    for load in loads[:4]:
        load.wait()

    levels = sig_ref.shape[1]
    pick = lax.broadcasted_iota(jnp.int32, (levels, coef), 0) == sh_ref[...]
    noise_of = jnp.broadcast_to(sig_ref[...], (coef, levels)).T
    noise = jnp.sum(jnp.where(pick, noise_of, 0.0), axis=0, keepdims=True)
    ctf = ctf_ref[...]
    par = jnp.concatenate([ctf, (1.0 / noise) * ctf], axis=1)
    par_high = par.astype(BF16).astype(F32)
    par_mid = (par - par_high).astype(BF16).astype(F32)
    offset = (x * nz + z) * coef
    table = (tab_ref[...] - offset).astype(F32)
    table = jnp.concatenate([table[:half], table[half:]], axis=1)
    bundle[me, count:] = jnp.concatenate([table, par_high, par_mid, (par - par_high) - par_mid], axis=0).astype(BF16)
    for load in loads[4:]:
        load.wait()
    with jax.named_scope("barrier"):
        greeted = sum(jnp.where(greets(b, zb), 1, 0) for b in range(nb))
        pl.semaphore_wait(barrier, ROW - 1 + zi * ROW + jnp.where(core > 0, 0, 1) + greeted)

    def down(i):
        device = at(x, zb * SIDE + i)
        remote(bundle.at[me], bundle.at[me], g_ssem, z_rsem.at[zi], device).start()
        remote(cls_ref.at[rows_of(i, ROW * kb)], cls_z.at[zi], g_ssem, z_rsem.at[zi], device).start()

    def across(i):
        b = i * ROW + x
        for k in OUTWARD:
            to = lax.rem(x + k, ROW)
            device = at(to, z)
            remote(bundle.at[b], bundle.at[b], g_ssem, x_rsem.at[i], device).start()
            remote(cls_z.at[i, rows_of(to, kb)], cls_all.at[b], g_ssem, x_rsem.at[i], device).start()

    bundle_size = bundle.shape[1] // 2
    def tell_above(i):
        tell(column_in.at[zi], at(x, zb * SIDE + i))
        each(1, ROW, lambda k: tell(others_in, at(lax.rem(x + k, ROW), zb * SIDE + i)))

    each(0, zi, tell_above)
    each(0, zi, lambda k: down(zi - 1 - k))
    across(zi)

    @pl.when(owner < OWNERS)
    def _():
        def tell_earlier(b):
            @pl.when(greets(b, zb))
            def _():
                tell(owner_in.at[owner], far(b))

        each(0, nb, tell_earlier)

    @pl.when(zb == 0)
    def _():
        tell(first_in, far(1))

    @pl.when(core == 0)
    def _():
        tell(partner_in, partner)

    with jax.named_scope("zeros"):
        w_all[...] = jnp.zeros_like(w_all)
        src_all[...] = jnp.zeros_like(src_all)
        left[...] = jnp.zeros_like(left)
    score[...] = jnp.zeros_like(score)
    cls_all[me] = cls_z[zi, rows_of(x, kb), :]
    member = jnp.broadcast_to(grp_ref[...].astype(F32), (LANES, count)).T
    low = lane((count, LANES)) < coef
    low_kb = lane((kb, LANES)) < coef

    def pass_on(i):
        with jax.named_scope("came_down"):
            drain(z_rsem.at[i], bundle_size + ROW * kb // 2)
        across(i)
        cls_all[i * ROW + x] = cls_z[i, rows_of(x, kb), :]

    def amplitudes(tail):
        par = tail[half : half + 8] + tail[half + 8 : half + 16] + tail[half + 16 : half + 24]
        sel = jnp.broadcast_to(par[0:1], (count, LANES))
        for g in range(1, par.shape[0]):
            sel = jnp.where(member == g, par[g : g + 1], sel)
        other = pltpu.roll(sel, coef, 1)
        return jnp.where(low, sel, other), jnp.where(low, other, sel)

    def turned_over(a):
        return jnp.concatenate([a, jnp.zeros((LANES - count, LANES), F32)], axis=0).astype(BF16).T

    def prepare(g, i):
        b = g * ROW + i
        landing = bundle[b, count:].astype(F32)
        amp, wamp = amplitudes(landing)
        weighted = turned_over(wamp * bundle[b, 0:count].astype(F32))
        pen = -0.5 * (wamp * amp)
        pen_hi = pen.astype(BF16).astype(F32)
        pen = turned_over(jnp.where(low, pen_hi, pen - pen_hi))
        for k, piece in enumerate((weighted[:coef], weighted[coef:], pen[:coef], pen[:coef], pen[coef:])):
            for s in range(2):
                top = pl.multiple_of((5 * i + k) * LANES + s * coef, coef)
                w_all[g, pl.ds(top, coef), s * LANES : (s + 1) * LANES] = piece
        index = lax.broadcasted_iota(jnp.int32, (coef, LANES), 0).astype(F32).astype(BF16)
        ones, zeros = jnp.ones((coef, LANES), BF16), jnp.zeros((coef, LANES), BF16)
        for j in range(half):
            row = jnp.broadcast_to(landing[j : j + 1], (16, LANES)).astype(BF16)
            row = jnp.concatenate([row] * (coef // 16), axis=0)
            place[rows_of(b, coef), j * LANES : (j + 1) * LANES] = jnp.where(index == row, ones, zeros)

    def prepare_sources(pair):
        for i in range(2):
            b = pair * 2 + i
            amp, _ = amplitudes(bundle[b, count:].astype(F32))
            source = amp * bundle[b, 0:count].astype(F32)
            source_turned = pltpu.roll(source, coef, 1)
            power = amp * amp
            for s in range(2):
                top = s * LANES

                def keep(lower, upper):
                    return (jnp.where(low, lower, 0.0) if s == 0 else jnp.where(low, 0.0, upper)).astype(BF16)

                for t, kept in (
                    (2 * i, keep(source, source_turned)),
                    (2 * i + 1, keep(source_turned, source)),
                    (4 + i, keep(power, power)),
                ):
                    src_all[pair, top : top + count, t * LANES : (t + 1) * LANES] = kept
        for j in range(half):
            lanes = slice(j * LANES, (j + 1) * LANES)
            place_turned[pair, lanes, :] = place[rows_of(pair, 2 * coef), lanes].T

    def rotate(g):
        for i in range(4):
            image = cls_all[g * 4 + i].astype(F32)
            turned = pltpu.roll(image, coef, 1)
            if i % 2 == 0:
                re, im = jnp.where(low_kb, image, 0.0), jnp.where(low_kb, turned, 0.0)
            else:
                re, im = jnp.where(low_kb, 0.0, turned), jnp.where(low_kb, 0.0, image)
            top = (i // 2) * LANES
            left[g, 2 * i * kb : (2 * i + 1) * kb, top : top + LANES] = re.astype(BF16)
            left[g, (2 * i + 1) * kb : (2 * i + 2) * kb, top : top + LANES] = im.astype(BF16)
        lhs = left[g]
        for jj in range(half // 2):
            turned = jnp.dot(
                lhs, place[rows_of(g, 4 * coef), jj * 256 : (jj + 1) * 256], preferred_element_type=F32
            )
            for i in range(4):
                for t in range(2):
                    j = jj * 2 + t
                    re = turned[2 * i * kb : (2 * i + 1) * kb, t * LANES : (t + 1) * LANES]
                    im = turned[(2 * i + 1) * kb : (2 * i + 2) * kb, t * LANES : (t + 1) * LANES]
                    power = re * re + im * im
                    power_hi = power.astype(BF16)
                    power_lo = (power - power_hi.astype(F32)).astype(BF16)
                    to = slice(j * kb, (j + 1) * kb)
                    pieces = re.astype(BF16), im.astype(BF16), power_hi, power_lo, power_hi
                    for k, piece in enumerate(pieces):
                        at_lane = (5 * i + k) * LANES
                        rot_all[g, to, at_lane : at_lane + LANES] = piece

    def score_row(g):
        with jax.named_scope("arrive"):
            drain(x_rsem.at[g], (ROW - 1) * (bundle_size + kb // 2))
        with jax.named_scope("scores"):
            for k in range(1, ROW):
                prepare(g, lax.rem(x + k, ROW))
            rotate(g)
            score[...] += jnp.dot(rot_all[g], w_all[g], preferred_element_type=F32)

    prepare(zi, x)

    def down_later(i):
        pl.semaphore_wait(column_in.at[i], 1)
        down(i)

    with jax.named_scope("down_later"):
        each(zi + 1, SIDE, down_later)

    nearest = (0, 1, 2, 3), (1, 0, 1, 2), (2, 2, 0, 1), (3, 3, 3, 0)

    def place_of(step):
        return sum(
            jnp.where(jnp.logical_and(step == t, zi == k), nearest[t][k], 0) for t in range(SIDE) for k in range(SIDE)
        )

    def turn_of(step):
        @pl.when(step == 1)
        def _():
            for t in range(1, SIDE):
                pass_on(place_of(t))
                prepare(place_of(t), x)

        score_row(place_of(step))

    each(0, SIDE, turn_of)

    @pl.when(zi < SIDE - 1)
    def _():
        pl.semaphore_wait(others_in, (SIDE - 1 - zi) * (ROW - 1))

    def share(o):
        return score[rows_of(o, rows), :]

    share_size = rs_send.shape[1] + rs_scale.shape[1]
    for o in (1, 2, 0, 3):

        @pl.when(owner != o)
        def _():
            piece = share(o)
            one, two = piece[:, :LANES], piece[:, LANES:]
            most = jnp.max(jnp.maximum(one, two), axis=0, keepdims=True)
            least = jnp.min(jnp.minimum(one, two), axis=0, keepdims=True)
            middle = 0.5 * (most + least)
            reach = jnp.maximum(0.5 * (most - least), 1e-30)
            fit = 32767.0 / reach
            one = jnp.round((one - middle) * fit).astype(jnp.int32)
            two = jnp.round((two - middle) * fit).astype(jnp.int32)
            rs_send[o] = compact((one & 0xFFFF) | (two << 16))
            rs_scale[o] = jnp.concatenate([*spread(reach * (1.0 / 32767.0)), *spread(middle)], axis=0)

            @pl.when(jnp.logical_not(greets(home(o), zb)))
            def _():
                with jax.named_scope("owner_in"):
                    pl.semaphore_wait(owner_in.at[o], 1)

            with jax.named_scope("share_go"):
                remote(rs_send.at[o], rs_recv.at[zb], rs_ssem, rs_rsem.at[zb], far(home(o))).start()
                remote(rs_scale.at[o], rs_rscale.at[zb], rs_ssem, rs_rsem.at[zb], far(home(o))).start()

    @pl.when(zb == 1)
    def _():
        pl.semaphore_wait(first_in, 1)
        tell(owner_in.at[2], far(0))
        tell(owner_in.at[3], far(0))

    with jax.named_scope("sources"):
        each(0, NP // 2, prepare_sources)

    later = zb >= nb // 2

    def send_post(b):
        @pl.when(b != zb)
        def _():
            remote(ag_send, ag_recv.at[owner], ag_ssem, ag_rsem.at[owner], far(b)).start()

    @pl.when(owner < OWNERS)
    def _():
        own = share(owner)
        total = compact(own[:, :LANES]), compact(own[:, LANES:])

        def add_share(k, so_far):
            b = jnp.where(k < zb, k, k + 1)
            with jax.named_scope("share_in"):
                drain(rs_rsem.at[b], share_size)
            word = rs_recv[b]
            step = tiles(rs_rscale[b, 0:1], rs_rscale[b, 1:2], word.shape[0])
            middle = tiles(rs_rscale[b, 2:3], rs_rscale[b, 3:4], word.shape[0])
            return (
                so_far[0] + (((word << 16) >> 16).astype(F32) * step + middle),
                so_far[1] + ((word >> 16).astype(F32) * step + middle),
            )

        total_one, total_two = lax.fori_loop(0, nb - 1, add_share, total)
        peak = over_rows(jnp.maximum(total_one, total_two), jnp.maximum, jnp.max)
        shift = tiles(*spread(peak), total_one.shape[0])
        exp_one, exp_two = jnp.exp(total_one - shift), jnp.exp(total_two - shift)
        evidence = peak + jnp.log(over_rows(exp_one + exp_two, jnp.add, jnp.sum))
        top_send[...] = jnp.concatenate([peak, evidence], axis=0)
        lse_send[...] = evidence

        for k in range(NP):
            remote(
                lse_send, lse_first.at[owner * NP + me], ag_ssem, first_rsem, at(k % ROW, k // ROW)
            ).start()
        for b in range(nb):

            @pl.when(b != zb)
            def _():
                remote(top_send, top_recv.at[owner], ag_ssem, top_rsem, far(b)).start()

        one = (exp_one * 65535.0 + 0.5).astype(jnp.int32)
        two = (exp_two * 65535.0 + 0.5).astype(jnp.int32)
        ag_send[...] = (one & 0xFFFF) | (two << 16)


        def send_early(b):
            @pl.when(jnp.logical_not(jnp.logical_and(later, b == 1)))
            def _():
                send_post(b)

        each(0, nb - 2, send_early)
        ag_recv[owner] = ag_send[...]
        top_recv[owner] = top_send[...]

    with jax.named_scope("top_in"):

        @pl.when(owner < OWNERS)
        def _():
            drain(top_rsem, (OWNERS - 1) * top_send.shape[0])

        @pl.when(owner >= OWNERS)
        def _():
            drain(top_rsem, OWNERS * top_send.shape[0])

    def merged(parts, axis):
        most = jnp.max(parts, axis=axis, keepdims=True)
        return most + jnp.log(jnp.sum(jnp.exp(parts - most), axis=axis, keepdims=True))

    @pl.when(jnp.logical_and(owner < OWNERS, later))
    def _():
        each(nb - 2, nb, send_post)

    def pass_post(o, b):
        with jax.named_scope("post_in"):
            drain(ag_rsem.at[o], ag_send.shape[0])
        remote(ag_recv.at[o], ag_recv.at[o], pass_ssem, ag_rsem.at[o], far(b)).start()

    used = lane((rows, LANES)) < count

    def unpack(o):
        word = expand(ag_recv[o])
        raw[rows_of(o, rows), 0:128] = jnp.where(used, (word & 0xFFFF).astype(F32), 0.0)
        raw[rows_of(o, rows), 128:256] = jnp.where(used, lax.shift_right_logical(word, 16).astype(F32), 0.0)

    @pl.when(zb == 0)
    def _():
        for o in range(OWNERS):
            pass_post(o, nb - 1 if o < OWNERS // 2 else 1)
        each(0, OWNERS, unpack)
        with jax.named_scope("first_in"):
            drain(first_rsem, OWNERS * NP)
        ev_ref[...] = merged(lse_first[...], 0)[0]

    @pl.when(zb > 0)
    def _():
        lse_own[...] = merged(jnp.concatenate([top_recv[o, 1:2] for o in range(OWNERS)], axis=0), 0)
        each(1, NP, lambda k: remote(lse_own, lse_all.at[me], lse_ssem, lse_rsem, mate(k)[1]).start())
        lse_all[me] = lse_own[...]
        with jax.named_scope("lse_in"):
            drain(lse_rsem, NP - 1)
        drain(lse_ssem, NP - 1)
        ev_ref[...] = merged(lse_all[...], 0)[0]

    evidence = ev_ref[...]
    def take_post(o):
        passes = jnp.logical_and(zb == nb - 1, o < OWNERS // 2)

        @pl.when(passes)
        def _():
            pass_post(o, nb - 2)

        @pl.when(jnp.logical_not(jnp.logical_or(passes, jnp.logical_or(o == owner, zb == 0))))
        def _():
            with jax.named_scope("post_in"):
                drain(ag_rsem.at[o], ag_send.shape[0])

        @pl.when(zb > 0)
        def _():
            unpack(o)

        scale = jnp.exp(top_recv[o, 0:1] - evidence) * (1.0 / 65535.0)
        scale = jnp.where(lane((1, LANES)) < count, scale, 0.0)
        post[rows_of(o, rows), 0:128] = (raw[rows_of(o, rows), 0:128] * scale).astype(BF16)
        post[rows_of(o, rows), 128:256] = (raw[rows_of(o, rows), 128:256] * scale).astype(BF16)

    each(0, OWNERS, take_post)

    def class_row(i):
        pairs_in = [i * (ROW // 2) + k for k in range(ROW // 2)]
        for k, pair in enumerate(pairs_in):
            frames = jnp.dot(post[...], src_all[pair], preferred_element_type=F32)
            for j in range(half):
                for t in range(6):
                    to = ((t // 2) * 3 + t % 2 if t < 4 else (t - 4) * 3 + 2) * kb
                    frame[k, to : to + kb, j * LANES : (j + 1) * LANES] = frames[
                        j * kb : (j + 1) * kb, t * LANES : (t + 1) * LANES
                    ].astype(BF16)
        low_out = lane((kb, LANES)) < coef
        for k, pair in enumerate(pairs_in):
            sums = jnp.zeros((6 * kb, LANES), F32)
            for at_depth in range(0, half * LANES, 2 * LANES):
                depth = slice(at_depth, at_depth + 2 * LANES)
                sums += jnp.dot(frame[k, :, depth], place_turned[pair, depth, :], preferred_element_type=F32)
            for t in range(2):
                mine = sums[3 * t * kb : 3 * (t + 1) * kb]
                other = pltpu.roll(mine, coef, 1)
                lower, upper = (mine, other) if t == 0 else (other, mine)
                out_send[i * ROW + 2 * k + t] = jnp.concatenate(
                    [
                        jnp.where(low_out, lower[:kb], upper[kb : 2 * kb]),
                        jnp.where(
                            low_out[: kb // 2], lower[2 * kb : 2 * kb + kb // 2], upper[2 * kb + kb // 2 : 3 * kb]
                        ),
                    ],
                    axis=0,
                ).astype(BF16)
            nearer = jnp.where(lax.rem(x + 2, ROW) == 2 * k + 1, 0, 1)
            for t in range(2):
                to = 2 * k + (1 - nearer if t == 0 else nearer)
                b = i * ROW + to

                @pl.when(b != me)
                def _():
                    remote(out_send.at[b], mine_ref.at[me], o_ssem, o_rsem, at(to, zb * SIDE + i)).start()

    with jax.named_scope("class_rows"):
        each(0, SIDE, class_row)
    mine_ref[me] = out_send[me]
    out_size = (NP - 1) * out_send.shape[1] // 2
    with jax.named_scope("take_out"):
        drain(o_rsem, out_size)

    @pl.when(core > 0)
    def _():
        pl.semaphore_wait(partner_in, 1)

    swap = remote(mine_ref, other_ref, c_ssem, c_rsem, partner)
    swap.start()

    drain(g_ssem, (SIDE - 1) * (bundle_size + ROW * kb // 2) + SIDE * (ROW - 1) * (bundle_size + kb // 2))
    drain(o_ssem, out_size)

    @pl.when(owner < OWNERS)
    def _():
        drain(rs_ssem, (OWNERS - 1) * share_size)
        drain(ag_ssem, (nb - 3) * ag_send.shape[0] + (nb - 1) * top_send.shape[0] + NP)

        @pl.when(later)
        def _():
            drain(ag_ssem, ag_send.shape[0])

    @pl.when(zb == 0)
    def _():
        drain(pass_ssem, OWNERS * ag_send.shape[0])

    @pl.when(zb == nb - 1)
    def _():
        drain(pass_ssem, OWNERS // 2 * ag_send.shape[0])

    @pl.when(owner >= OWNERS)
    def _():
        drain(rs_ssem, OWNERS * share_size)

    with jax.named_scope("swap"):
        swap.wait()


def finish(mine_ref, other_ref, ev_ref, cs_ref, cw_ref, out_ref):
    coef, kb = cw_ref.shape[0], cs_ref.shape[0] // NP
    halves = []
    for b in range(NP):
        both = mine_ref[b].astype(F32) + other_ref[b].astype(F32)
        cs_ref[b * kb : (b + 1) * kb, :] = both[:kb]
        halves.append(both[kb:])
    for first in range(0, NP, NP // 2):
        turned = jnp.concatenate(halves[first : first + NP // 2], axis=0).T
        for k in range(NP // 2):
            lanes = slice(k * kb // 2, (k + 1) * kb // 2)
            to = (first + k) * kb
            cw_ref[:, to : to + kb // 2] = turned[:coef, lanes]
            cw_ref[:, to + kb // 2 : to + kb] = turned[coef:, lanes]
    out_ref[...] = ev_ref[:, : out_ref.shape[1]]


def body(nz, particles, classes, ctf, sigma2, shell_of, rot_table, ctf_group):
    count, coef = particles.shape[0], shell_of.shape[0]
    classes_n, rotations = classes.shape[0], rot_table.shape[0]
    nb = nz // SIDE
    kb = classes_n // NP
    half = rotations // 2
    pairs = half * kb
    piece = pairs // OWNERS * 2 // 3
    dma = pltpu.SemaphoreType.DMA
    regular = pltpu.SemaphoreType.REGULAR
    vmem = pltpu.VMEM
    i32 = jnp.int32
    arrays = (
        particles,
        classes,
        ctf,
        sigma2.reshape(1, -1),
        shell_of.reshape(1, -1),
        rot_table,
        ctf_group.reshape(1, -1),
    )
    mine, other, evidence = pl.pallas_call(
        functools.partial(kernel, nz),
        out_shape=[
            jax.ShapeDtypeStruct((NP, 24, LANES), BF16),
            jax.ShapeDtypeStruct((NP, 24, LANES), BF16),
            jax.ShapeDtypeStruct((1, LANES), F32),
        ],
        in_specs=[pl.BlockSpec(memory_space=pltpu.HBM)] * 7,
        out_specs=[pl.BlockSpec(memory_space=vmem)] * 3,
        scratch_shapes=[
            *[vmem(a.shape, a.dtype) for a in arrays[1:]],
            vmem((NP, count + half + 24, LANES), BF16),
            vmem((SIDE, ROW * kb, LANES), BF16),
            vmem((NP, kb, LANES), BF16),
            vmem((NP * coef, half * LANES), BF16),
            vmem((NP // 2, half * LANES, 2 * coef), BF16),
            vmem((SIDE, ROW * 5 * LANES, 2 * LANES), BF16),
            vmem((NP // 2, 2 * LANES, 6 * LANES), BF16),
            vmem((NP // 4, 8 * kb, 4 * coef), BF16),
            vmem((SIDE, pairs, ROW * 5 * LANES), BF16),
            vmem((pairs, 2 * LANES), F32),
            vmem((OWNERS, piece, LANES), i32),
            vmem((OWNERS, 4, LANES), F32),
            vmem((nb, piece, LANES), i32),
            vmem((nb, 4, LANES), F32),
            vmem((piece, LANES), i32),
            vmem((2, LANES), F32),
            vmem((OWNERS, piece, LANES), i32),
            vmem((OWNERS, 2, LANES), F32),
            vmem((1, LANES), F32),
            vmem((OWNERS * NP, 1, LANES), F32),
            vmem((1, LANES), F32),
            vmem((NP, 1, LANES), F32),
            vmem((pairs, 2 * LANES), F32),
            vmem((pairs, 2 * LANES), BF16),
            vmem((ROW // 2, 6 * kb, half * LANES), BF16),
            vmem((NP, 24, LANES), BF16),
            vmem((1152, 1, LANES), F32),
            dma((len(arrays) + 1,)),
            dma,
            dma((SIDE,)),
            dma((SIDE,)),
            dma,
            dma((nb,)),
            dma,
            dma,
            dma((OWNERS,)),
            *[dma] * 8,
            regular((SIDE,)),
            regular,
            regular((OWNERS,)),
            regular,
            regular,
        ],
        compiler_params=pltpu.CompilerParams(
            collective_id=0, has_side_effects=True, vmem_limit_bytes=40 * 1024 * 1024
        ),
        name="averaging",
    )(*[pltpu.with_memory_space_constraint(a, pltpu.HBM) for a in arrays])
    sums, weights, evidence = pl.pallas_call(
        finish,
        out_shape=[
            jax.ShapeDtypeStruct((classes_n, 2 * coef), F32),
            jax.ShapeDtypeStruct((coef, classes_n), F32),
            jax.ShapeDtypeStruct((1, count), F32),
        ],
        in_specs=[pl.BlockSpec(memory_space=vmem)] * 3,
        out_specs=[pl.BlockSpec(memory_space=vmem)] * 3,
        compiler_params=pltpu.CompilerParams(vmem_limit_bytes=4 * 1024 * 1024),
        name="finish",
    )(mine, other, evidence)
    return sums, weights.T, evidence.reshape(-1)


def solution(mesh):
    nz = mesh.shape["shell"] // ROW
    split = Mesh(mesh.devices.reshape(mesh.shape["groups"], ROW, nz, mesh.shape["batch"]), AXES)
    shell = ("x", "z")
    placed = (
        P(("groups", "batch"), shell),
        P("groups", shell),
        P("groups", shell),
        P("groups"),
        P(shell),
        P(None, shell),
        P(("groups", "batch")),
    )
    return jax.shard_map(
        functools.partial(body, nz),
        mesh=split,
        in_specs=placed,
        out_specs=(P("groups", shell), P("groups", shell), P(("groups", "batch"))),
        check_vma=False,
    )
```

```python
import functools

import jax
import jax.numpy as jnp
from jax import lax
from jax.experimental import pallas as pl
from jax.experimental.pallas import tpu as pltpu
from jax.sharding import Mesh
from jax.sharding import PartitionSpec as P

MESH = pl.DeviceIdType.MESH
ROW = 4
SIDE = 4
NP = ROW * SIDE
OUTWARD = 2, 1, 3
OWNERS = 4
LANES = 128
F32 = jnp.float32
BF16 = jnp.bfloat16
NT = (((1,), (1,)), ((), ()))
AXES = ("groups", "x", "z", "batch")


def lane(shape):
    return lax.broadcasted_iota(jnp.int32, shape, 1)


def compact(w):
    free = lane((8, LANES)) >= 80
    kept = []
    for r in range(0, w.shape[0], 48):
        a, b = w[r + 32 : r + 40], w[r + 40 : r + 48]
        kept += [
            jnp.where(free, pltpu.roll(a, 80, 1), w[r : r + 8]),
            jnp.where(free, pltpu.roll(a, 32, 1), w[r + 8 : r + 16]),
            jnp.where(free, pltpu.roll(b, 80, 1), w[r + 16 : r + 24]),
            jnp.where(free, pltpu.roll(b, 32, 1), w[r + 24 : r + 32]),
        ]
    return jnp.concatenate(kept, axis=0)


def expand(w):
    first = lane((8, LANES)) < 48
    whole = []
    for r in range(0, w.shape[0], 32):
        part = w[r : r + 32]
        whole += [
            part,
            jnp.where(first, pltpu.roll(part[0:8], 48, 1), pltpu.roll(part[8:16], 96, 1)),
            jnp.where(first, pltpu.roll(part[16:24], 48, 1), pltpu.roll(part[24:32], 96, 1)),
        ]
    return jnp.concatenate(whole, axis=0)


def spread(row):
    free = lane((1, LANES)) >= 80
    return jnp.where(free, pltpu.roll(row, 80, 1), row), jnp.where(free, pltpu.roll(row, 32, 1), row)


def tiles(even, odd, rows):
    e = jnp.broadcast_to(even, (8, LANES))
    o = jnp.broadcast_to(odd, (8, LANES))
    return jnp.concatenate([e, o] * (rows // 16), axis=0)


def over_rows(values, combine, reduce):
    split = [values[r : r + 8] for r in range(0, values.shape[0], 8)]
    even = reduce(functools.reduce(combine, split[0::2]), axis=0, keepdims=True)
    odd = reduce(functools.reduce(combine, split[1::2]), axis=0, keepdims=True)
    first = lane((1, LANES)) < 48
    moved = jnp.where(first, pltpu.roll(even, 48, 1), pltpu.roll(odd, 96, 1))
    return combine(combine(even, odd), moved)


def kernel(
    nz,
    part_hbm,
    cls_hbm,
    ctf_hbm,
    sig_hbm,
    sh_hbm,
    tab_hbm,
    grp_hbm,
    mine_ref,
    other_ref,
    ev_ref,
    cls_ref,
    ctf_ref,
    sig_ref,
    sh_ref,
    tab_ref,
    grp_ref,
    bundle,
    cls_z,
    cls_all,
    place,
    place_turned,
    w_all,
    src_all,
    left,
    rot_all,
    score,
    rs_send,
    rs_scale,
    rs_recv,
    rs_rscale,
    ag_send,
    top_send,
    ag_recv,
    top_recv,
    lse_send,
    lse_first,
    lse_own,
    lse_all,
    raw,
    post,
    frame,
    out_send,
    sizes,
    in_sem,
    g_ssem,
    z_rsem,
    x_rsem,
    rs_ssem,
    rs_rsem,
    ag_ssem,
    pass_ssem,
    ag_rsem,
    top_rsem,
    first_rsem,
    lse_ssem,
    lse_rsem,
    o_ssem,
    o_rsem,
    c_ssem,
    c_rsem,
    column_in,
    others_in,
    owner_in,
    first_in,
    partner_in,
):
    nb = nz // SIDE
    count, coef = part_hbm.shape[0], ctf_ref.shape[1]
    kb = cls_all.shape[1]
    half = tab_ref.shape[0] // 2
    rows = half * kb // OWNERS
    group = lax.axis_index("groups")
    x = lax.axis_index("x")
    z = lax.axis_index("z")
    core = lax.axis_index("batch")
    zb, zi = z // SIDE, lax.rem(z, SIDE)
    me = zi * ROW + x
    def owns(b):
        return jnp.logical_or(
            jnp.logical_and(b >= 1, b < 3), jnp.logical_and(b >= nb - 3, b < nb - 1)
        )

    def home(o):
        return jnp.where(o < 2, o + 1, o + nb - 5)

    owner = jnp.where(owns(zb), jnp.where(zb < 3, zb - 1, zb - nb + 5), OWNERS)

    def greets(a, b):
        between = jnp.logical_and(jnp.logical_and(a >= 1, a < b), b < nb - 1)
        return jnp.logical_or(
            jnp.logical_and(between, jnp.logical_or(owns(a), owns(b))),
            jnp.logical_or(
                jnp.logical_and(b == 0, jnp.logical_and(a >= 1, a < 3)), jnp.logical_and(b == nb - 1, owns(a))
            ),
        )

    def at(x_, z_):
        return (group, x_, z_, core)

    def mate(k):
        i = lax.rem(me + k, NP)
        return i, at(lax.rem(i, ROW), zb * SIDE + i // ROW)

    def far(b):
        return at(x, b * SIDE + zi)

    partner = (group, x, z, 1 - core)

    def remote(src, dst, ssem, rsem, device):
        return pltpu.make_async_remote_copy(
            src_ref=src, dst_ref=dst, send_sem=ssem, recv_sem=rsem, device_id=device, device_id_type=MESH
        )

    def drain(semaphore, size):
        whole = sizes.at[0:size]
        remote(whole, whole, semaphore, semaphore, partner).wait_recv()

    def each(lower, upper, step):
        def turn(k, _):
            step(k)
            return 0

        lax.fori_loop(lower, upper, turn, 0)

    def tell(semaphore, device):
        pl.semaphore_signal(semaphore, inc=1, device_id=device, device_id_type=MESH)

    def rows_of(i, n):
        return pl.ds(pl.multiple_of(i * n, n), n)

    given = (ctf_hbm, sig_hbm, sh_hbm, tab_hbm, part_hbm, cls_hbm.at[rows_of(zi, ROW * kb)], cls_hbm, grp_hbm)
    taken = (ctf_ref, sig_ref, sh_ref, tab_ref, bundle.at[me, 0:count], cls_z.at[zi], cls_ref, grp_ref)
    loads = [pltpu.make_async_copy(a, b, in_sem.at[k]) for k, (a, b) in enumerate(zip(given, taken))]
    for load in loads:
        load.start()

    barrier = pltpu.get_barrier_semaphore()
    each(1, ROW, lambda k: tell(barrier, at(lax.rem(x + k, ROW), z)))
    each((zi + 1) * ROW, NP, lambda i: tell(barrier, at(lax.rem(i, ROW), zb * SIDE + i // ROW)))

    @pl.when(core > 0)
    def _():
        tell(barrier, partner)

    def greet(b):
        @pl.when(greets(zb, b))
        def _():
            tell(barrier, far(b))

    each(0, nb, greet)
    for load in loads[:4]:
        load.wait()

    levels = sig_ref.shape[1]
    pick = lax.broadcasted_iota(jnp.int32, (levels, coef), 0) == sh_ref[...]
    noise_of = jnp.broadcast_to(sig_ref[...], (coef, levels)).T
    noise = jnp.sum(jnp.where(pick, noise_of, 0.0), axis=0, keepdims=True)
    ctf = ctf_ref[...]
    par = jnp.concatenate([ctf, (1.0 / noise) * ctf], axis=1)
    par_high = par.astype(BF16).astype(F32)
    par_mid = (par - par_high).astype(BF16).astype(F32)
    offset = (x * nz + z) * coef
    table = (tab_ref[...] - offset).astype(F32)
    table = jnp.concatenate([table[:half], table[half:]], axis=1)
    bundle[me, count:] = jnp.concatenate([table, par_high, par_mid, (par - par_high) - par_mid], axis=0).astype(BF16)
    for load in loads[4:]:
        load.wait()
    with jax.named_scope("barrier"):
        greeted = sum(jnp.where(greets(b, zb), 1, 0) for b in range(nb))
        pl.semaphore_wait(barrier, ROW - 1 + zi * ROW + jnp.where(core > 0, 0, 1) + greeted)

    def down(i):
        device = at(x, zb * SIDE + i)
        remote(bundle.at[me], bundle.at[me], g_ssem, z_rsem.at[zi], device).start()
        remote(cls_ref.at[rows_of(i, ROW * kb)], cls_z.at[zi], g_ssem, z_rsem.at[zi], device).start()

    def across(i):
        b = i * ROW + x
        for k in OUTWARD:
            to = lax.rem(x + k, ROW)
            device = at(to, z)
            remote(bundle.at[b], bundle.at[b], g_ssem, x_rsem.at[i], device).start()
            remote(cls_z.at[i, rows_of(to, kb)], cls_all.at[b], g_ssem, x_rsem.at[i], device).start()

    bundle_size = bundle.shape[1] // 2
    def tell_above(i):
        tell(column_in.at[zi], at(x, zb * SIDE + i))
        each(1, ROW, lambda k: tell(others_in, at(lax.rem(x + k, ROW), zb * SIDE + i)))

    each(0, zi, tell_above)
    each(0, zi, lambda k: down(zi - 1 - k))
    across(zi)

    @pl.when(owner < OWNERS)
    def _():
        def tell_earlier(b):
            @pl.when(greets(b, zb))
            def _():
                tell(owner_in.at[owner], far(b))

        each(0, nb, tell_earlier)

    @pl.when(zb == 0)
    def _():
        tell(first_in, far(1))

    @pl.when(core == 0)
    def _():
        tell(partner_in, partner)

    with jax.named_scope("zeros"):
        w_all[...] = jnp.zeros_like(w_all)
        src_all[...] = jnp.zeros_like(src_all)
        left[...] = jnp.zeros_like(left)
    score[...] = jnp.zeros_like(score)
    cls_all[me] = cls_z[zi, rows_of(x, kb), :]
    member = jnp.broadcast_to(grp_ref[...].astype(F32), (LANES, count)).T
    low = lane((count, LANES)) < coef
    low_kb = lane((kb, LANES)) < coef

    def pass_on(i):
        with jax.named_scope("came_down"):
            drain(z_rsem.at[i], bundle_size + ROW * kb // 2)
        across(i)
        cls_all[i * ROW + x] = cls_z[i, rows_of(x, kb), :]

    def amplitudes(tail):
        par = tail[half : half + 8] + tail[half + 8 : half + 16] + tail[half + 16 : half + 24]
        sel = jnp.broadcast_to(par[0:1], (count, LANES))
        for g in range(1, par.shape[0]):
            sel = jnp.where(member == g, par[g : g + 1], sel)
        other = pltpu.roll(sel, coef, 1)
        return jnp.where(low, sel, other), jnp.where(low, other, sel)

    def turned_over(a):
        return jnp.concatenate([a, jnp.zeros((LANES - count, LANES), F32)], axis=0).astype(BF16).T

    def prepare(g, i):
        b = g * ROW + i
        landing = bundle[b, count:].astype(F32)
        amp, wamp = amplitudes(landing)
        weighted = turned_over(wamp * bundle[b, 0:count].astype(F32))
        pen = -0.5 * (wamp * amp)
        pen_hi = pen.astype(BF16).astype(F32)
        pen = turned_over(jnp.where(low, pen_hi, pen - pen_hi))
        for k, piece in enumerate((weighted[:coef], weighted[coef:], pen[:coef], pen[:coef], pen[coef:])):
            for s in range(2):
                top = pl.multiple_of((5 * i + k) * LANES + s * coef, coef)
                w_all[g, pl.ds(top, coef), s * LANES : (s + 1) * LANES] = piece
        index = lax.broadcasted_iota(jnp.int32, (coef, LANES), 0).astype(F32).astype(BF16)
        ones, zeros = jnp.ones((coef, LANES), BF16), jnp.zeros((coef, LANES), BF16)
        for j in range(half):
            row = jnp.broadcast_to(landing[j : j + 1], (16, LANES)).astype(BF16)
            row = jnp.concatenate([row] * (coef // 16), axis=0)
            place[rows_of(b, coef), j * LANES : (j + 1) * LANES] = jnp.where(index == row, ones, zeros)

    def prepare_sources(pair):
        for i in range(2):
            b = pair * 2 + i
            amp, _ = amplitudes(bundle[b, count:].astype(F32))
            source = amp * bundle[b, 0:count].astype(F32)
            source_turned = pltpu.roll(source, coef, 1)
            power = amp * amp
            for s in range(2):
                top = s * LANES

                def keep(lower, upper):
                    return (jnp.where(low, lower, 0.0) if s == 0 else jnp.where(low, 0.0, upper)).astype(BF16)

                for t, kept in (
                    (2 * i, keep(source, source_turned)),
                    (2 * i + 1, keep(source_turned, source)),
                    (4 + i, keep(power, power)),
                ):
                    src_all[pair, top : top + count, t * LANES : (t + 1) * LANES] = kept
        for j in range(half):
            lanes = slice(j * LANES, (j + 1) * LANES)
            place_turned[pair, lanes, :] = place[rows_of(pair, 2 * coef), lanes].T

    def rotate(g):
        for i in range(4):
            image = cls_all[g * 4 + i].astype(F32)
            turned = pltpu.roll(image, coef, 1)
            if i % 2 == 0:
                re, im = jnp.where(low_kb, image, 0.0), jnp.where(low_kb, turned, 0.0)
            else:
                re, im = jnp.where(low_kb, 0.0, turned), jnp.where(low_kb, 0.0, image)
            top = (i // 2) * LANES
            left[g, 2 * i * kb : (2 * i + 1) * kb, top : top + LANES] = re.astype(BF16)
            left[g, (2 * i + 1) * kb : (2 * i + 2) * kb, top : top + LANES] = im.astype(BF16)
        lhs = left[g]
        for jj in range(half // 2):
            turned = jnp.dot(
                lhs, place[rows_of(g, 4 * coef), jj * 256 : (jj + 1) * 256], preferred_element_type=F32
            )
            for i in range(4):
                for t in range(2):
                    j = jj * 2 + t
                    re = turned[2 * i * kb : (2 * i + 1) * kb, t * LANES : (t + 1) * LANES]
                    im = turned[(2 * i + 1) * kb : (2 * i + 2) * kb, t * LANES : (t + 1) * LANES]
                    power = re * re + im * im
                    power_hi = power.astype(BF16)
                    power_lo = (power - power_hi.astype(F32)).astype(BF16)
                    to = slice(j * kb, (j + 1) * kb)
                    pieces = re.astype(BF16), im.astype(BF16), power_hi, power_lo, power_hi
                    for k, piece in enumerate(pieces):
                        at_lane = (5 * i + k) * LANES
                        rot_all[g, to, at_lane : at_lane + LANES] = piece

    def score_row(g):
        with jax.named_scope("arrive"):
            drain(x_rsem.at[g], (ROW - 1) * (bundle_size + kb // 2))
        with jax.named_scope("scores"):
            for k in range(1, ROW):
                prepare(g, lax.rem(x + k, ROW))
            rotate(g)
            score[...] += jnp.dot(rot_all[g], w_all[g], preferred_element_type=F32)

    prepare(zi, x)

    def down_later(i):
        pl.semaphore_wait(column_in.at[i], 1)
        down(i)

    with jax.named_scope("down_later"):
        each(zi + 1, SIDE, down_later)

    nearest = (0, 1, 2, 3), (1, 0, 1, 2), (2, 2, 0, 1), (3, 3, 3, 0)

    def place_of(step):
        return sum(
            jnp.where(jnp.logical_and(step == t, zi == k), nearest[t][k], 0) for t in range(SIDE) for k in range(SIDE)
        )

    def turn_of(step):
        @pl.when(step == 1)
        def _():
            for t in range(1, SIDE):
                pass_on(place_of(t))
                prepare(place_of(t), x)

        score_row(place_of(step))

    each(0, SIDE, turn_of)

    @pl.when(zi < SIDE - 1)
    def _():
        pl.semaphore_wait(others_in, (SIDE - 1 - zi) * (ROW - 1))

    def share(o):
        return score[rows_of(o, rows), :]

    share_size = rs_send.shape[1] + rs_scale.shape[1]
    for o in (1, 2, 0, 3):

        @pl.when(owner != o)
        def _():
            piece = share(o)
            one, two = piece[:, :LANES], piece[:, LANES:]
            most = jnp.max(jnp.maximum(one, two), axis=0, keepdims=True)
            least = jnp.min(jnp.minimum(one, two), axis=0, keepdims=True)
            middle = 0.5 * (most + least)
            reach = jnp.maximum(0.5 * (most - least), 1e-30)
            fit = 32767.0 / reach
            one = jnp.round((one - middle) * fit).astype(jnp.int32)
            two = jnp.round((two - middle) * fit).astype(jnp.int32)
            rs_send[o] = compact((one & 0xFFFF) | (two << 16))
            rs_scale[o] = jnp.concatenate([*spread(reach * (1.0 / 32767.0)), *spread(middle)], axis=0)

            @pl.when(jnp.logical_not(greets(home(o), zb)))
            def _():
                with jax.named_scope("owner_in"):
                    pl.semaphore_wait(owner_in.at[o], 1)

            with jax.named_scope("share_go"):
                remote(rs_send.at[o], rs_recv.at[zb], rs_ssem, rs_rsem.at[zb], far(home(o))).start()
                remote(rs_scale.at[o], rs_rscale.at[zb], rs_ssem, rs_rsem.at[zb], far(home(o))).start()

    @pl.when(zb == 1)
    def _():
        pl.semaphore_wait(first_in, 1)
        tell(owner_in.at[2], far(0))
        tell(owner_in.at[3], far(0))

    with jax.named_scope("sources"):
        each(0, NP // 2, prepare_sources)

    later = zb >= nb // 2

    def send_post(b):
        @pl.when(b != zb)
        def _():
            remote(ag_send, ag_recv.at[owner], ag_ssem, ag_rsem.at[owner], far(b)).start()

    @pl.when(owner < OWNERS)
    def _():
        own = share(owner)
        total = compact(own[:, :LANES]), compact(own[:, LANES:])

        def add_share(k, so_far):
            b = jnp.where(k < zb, k, k + 1)
            with jax.named_scope("share_in"):
                drain(rs_rsem.at[b], share_size)
            word = rs_recv[b]
            step = tiles(rs_rscale[b, 0:1], rs_rscale[b, 1:2], word.shape[0])
            middle = tiles(rs_rscale[b, 2:3], rs_rscale[b, 3:4], word.shape[0])
            return (
                so_far[0] + (((word << 16) >> 16).astype(F32) * step + middle),
                so_far[1] + ((word >> 16).astype(F32) * step + middle),
            )

        total_one, total_two = lax.fori_loop(0, nb - 1, add_share, total)
        peak = over_rows(jnp.maximum(total_one, total_two), jnp.maximum, jnp.max)
        shift = tiles(*spread(peak), total_one.shape[0])
        exp_one, exp_two = jnp.exp(total_one - shift), jnp.exp(total_two - shift)
        evidence = peak + jnp.log(over_rows(exp_one + exp_two, jnp.add, jnp.sum))
        top_send[...] = jnp.concatenate([peak, evidence], axis=0)
        lse_send[...] = evidence

        for k in range(NP):
            row = jnp.where(later, SIDE - 1 - k // ROW, k // ROW)
            remote(
                lse_send, lse_first.at[owner * NP + me], ag_ssem, first_rsem, at(k % ROW, row)
            ).start()
        for b in range(nb):

            @pl.when(b != zb)
            def _():
                remote(top_send, top_recv.at[owner], ag_ssem, top_rsem, far(b)).start()

        one = (exp_one * 65535.0 + 0.5).astype(jnp.int32)
        two = (exp_two * 65535.0 + 0.5).astype(jnp.int32)
        ag_send[...] = (one & 0xFFFF) | (two << 16)


        def send_early(b):
            @pl.when(jnp.logical_not(jnp.logical_and(later, b == 1)))
            def _():
                send_post(b)

        each(0, nb - 2, send_early)
        ag_recv[owner] = ag_send[...]
        top_recv[owner] = top_send[...]

    with jax.named_scope("top_in"):

        @pl.when(owner < OWNERS)
        def _():
            drain(top_rsem, (OWNERS - 1) * top_send.shape[0])

        @pl.when(owner >= OWNERS)
        def _():
            drain(top_rsem, OWNERS * top_send.shape[0])

    def merged(parts, axis):
        most = jnp.max(parts, axis=axis, keepdims=True)
        return most + jnp.log(jnp.sum(jnp.exp(parts - most), axis=axis, keepdims=True))

    @pl.when(jnp.logical_and(owner < OWNERS, later))
    def _():
        each(nb - 2, nb, send_post)

    def pass_post(o, b):
        with jax.named_scope("post_in"):
            drain(ag_rsem.at[o], ag_send.shape[0])
        remote(ag_recv.at[o], ag_recv.at[o], pass_ssem, ag_rsem.at[o], far(b)).start()

    used = lane((rows, LANES)) < count

    def unpack(o):
        word = expand(ag_recv[o])
        raw[rows_of(o, rows), 0:128] = jnp.where(used, (word & 0xFFFF).astype(F32), 0.0)
        raw[rows_of(o, rows), 128:256] = jnp.where(used, lax.shift_right_logical(word, 16).astype(F32), 0.0)

    @pl.when(zb == 0)
    def _():
        for o in range(OWNERS):
            pass_post(o, nb - 1 if o < OWNERS // 2 else 1)
        each(0, OWNERS, unpack)
        with jax.named_scope("first_in"):
            drain(first_rsem, OWNERS * NP)
        ev_ref[...] = merged(lse_first[...], 0)[0]

    @pl.when(zb > 0)
    def _():
        lse_own[...] = merged(jnp.concatenate([top_recv[o, 1:2] for o in range(OWNERS)], axis=0), 0)
        each(1, NP, lambda k: remote(lse_own, lse_all.at[me], lse_ssem, lse_rsem, mate(k)[1]).start())
        lse_all[me] = lse_own[...]
        with jax.named_scope("lse_in"):
            drain(lse_rsem, NP - 1)
        drain(lse_ssem, NP - 1)
        ev_ref[...] = merged(lse_all[...], 0)[0]

    evidence = ev_ref[...]
    def take_post(o):
        passes = jnp.logical_and(zb == nb - 1, o < OWNERS // 2)

        @pl.when(passes)
        def _():
            pass_post(o, nb - 2)

        @pl.when(jnp.logical_not(jnp.logical_or(passes, jnp.logical_or(o == owner, zb == 0))))
        def _():
            with jax.named_scope("post_in"):
                drain(ag_rsem.at[o], ag_send.shape[0])

        @pl.when(zb > 0)
        def _():
            unpack(o)

        scale = jnp.exp(top_recv[o, 0:1] - evidence) * (1.0 / 65535.0)
        scale = jnp.where(lane((1, LANES)) < count, scale, 0.0)
        post[rows_of(o, rows), 0:128] = (raw[rows_of(o, rows), 0:128] * scale).astype(BF16)
        post[rows_of(o, rows), 128:256] = (raw[rows_of(o, rows), 128:256] * scale).astype(BF16)

    for o in range(OWNERS):
        take_post(o)

    def class_row(i):
        pairs_in = [i * (ROW // 2) + k for k in range(ROW // 2)]
        for k, pair in enumerate(pairs_in):
            frames = jnp.dot(post[...], src_all[pair], preferred_element_type=F32)
            for j in range(half):
                for t in range(6):
                    to = ((t // 2) * 3 + t % 2 if t < 4 else (t - 4) * 3 + 2) * kb
                    frame[k, to : to + kb, j * LANES : (j + 1) * LANES] = frames[
                        j * kb : (j + 1) * kb, t * LANES : (t + 1) * LANES
                    ].astype(BF16)
        low_out = lane((kb, LANES)) < coef
        for k, pair in enumerate(pairs_in):
            sums = jnp.zeros((6 * kb, LANES), F32)
            for at_depth in range(0, half * LANES, 2 * LANES):
                depth = slice(at_depth, at_depth + 2 * LANES)
                sums += jnp.dot(frame[k, :, depth], place_turned[pair, depth, :], preferred_element_type=F32)
            for t in range(2):
                mine = sums[3 * t * kb : 3 * (t + 1) * kb]
                other = pltpu.roll(mine, coef, 1)
                lower, upper = (mine, other) if t == 0 else (other, mine)
                out_send[i * ROW + 2 * k + t] = jnp.concatenate(
                    [
                        jnp.where(low_out, lower[:kb], upper[kb : 2 * kb]),
                        jnp.where(
                            low_out[: kb // 2], lower[2 * kb : 2 * kb + kb // 2], upper[2 * kb + kb // 2 : 3 * kb]
                        ),
                    ],
                    axis=0,
                ).astype(BF16)
            nearer = jnp.where(lax.rem(x + 2, ROW) == 2 * k + 1, 0, 1)
            for t in range(2):
                to = 2 * k + (1 - nearer if t == 0 else nearer)
                b = i * ROW + to

                @pl.when(b != me)
                def _():
                    remote(out_send.at[b], mine_ref.at[me], o_ssem, o_rsem, at(to, zb * SIDE + i)).start()

    with jax.named_scope("class_rows"):
        each(0, SIDE, class_row)
    mine_ref[me] = out_send[me]
    out_size = (NP - 1) * out_send.shape[1] // 2
    with jax.named_scope("take_out"):
        drain(o_rsem, out_size)

    @pl.when(core > 0)
    def _():
        pl.semaphore_wait(partner_in, 1)

    swap = remote(mine_ref, other_ref, c_ssem, c_rsem, partner)
    swap.start()

    drain(g_ssem, (SIDE - 1) * (bundle_size + ROW * kb // 2) + SIDE * (ROW - 1) * (bundle_size + kb // 2))
    drain(o_ssem, out_size)

    @pl.when(owner < OWNERS)
    def _():
        drain(rs_ssem, (OWNERS - 1) * share_size)
        drain(ag_ssem, (nb - 3) * ag_send.shape[0] + (nb - 1) * top_send.shape[0] + NP)

        @pl.when(later)
        def _():
            drain(ag_ssem, ag_send.shape[0])

    @pl.when(zb == 0)
    def _():
        drain(pass_ssem, OWNERS * ag_send.shape[0])

    @pl.when(zb == nb - 1)
    def _():
        drain(pass_ssem, OWNERS // 2 * ag_send.shape[0])

    @pl.when(owner >= OWNERS)
    def _():
        drain(rs_ssem, OWNERS * share_size)

    with jax.named_scope("swap"):
        swap.wait()


def finish(mine_ref, other_ref, ev_ref, cs_ref, cw_ref, out_ref):
    coef, kb = cw_ref.shape[0], cs_ref.shape[0] // NP
    halves = []
    for b in range(NP):
        both = mine_ref[b].astype(F32) + other_ref[b].astype(F32)
        cs_ref[b * kb : (b + 1) * kb, :] = both[:kb]
        halves.append(both[kb:])
    for first in range(0, NP, NP // 2):
        turned = jnp.concatenate(halves[first : first + NP // 2], axis=0).T
        for k in range(NP // 2):
            lanes = slice(k * kb // 2, (k + 1) * kb // 2)
            to = (first + k) * kb
            cw_ref[:, to : to + kb // 2] = turned[:coef, lanes]
            cw_ref[:, to + kb // 2 : to + kb] = turned[coef:, lanes]
    out_ref[...] = ev_ref[:, : out_ref.shape[1]]


def body(nz, particles, classes, ctf, sigma2, shell_of, rot_table, ctf_group):
    count, coef = particles.shape[0], shell_of.shape[0]
    classes_n, rotations = classes.shape[0], rot_table.shape[0]
    nb = nz // SIDE
    kb = classes_n // NP
    half = rotations // 2
    pairs = half * kb
    piece = pairs // OWNERS * 2 // 3
    dma = pltpu.SemaphoreType.DMA
    regular = pltpu.SemaphoreType.REGULAR
    vmem = pltpu.VMEM
    i32 = jnp.int32
    arrays = (
        particles,
        classes,
        ctf,
        sigma2.reshape(1, -1),
        shell_of.reshape(1, -1),
        rot_table,
        ctf_group.reshape(1, -1),
    )
    mine, other, evidence = pl.pallas_call(
        functools.partial(kernel, nz),
        out_shape=[
            jax.ShapeDtypeStruct((NP, 24, LANES), BF16),
            jax.ShapeDtypeStruct((NP, 24, LANES), BF16),
            jax.ShapeDtypeStruct((1, LANES), F32),
        ],
        in_specs=[pl.BlockSpec(memory_space=pltpu.HBM)] * 7,
        out_specs=[pl.BlockSpec(memory_space=vmem)] * 3,
        scratch_shapes=[
            *[vmem(a.shape, a.dtype) for a in arrays[1:]],
            vmem((NP, count + half + 24, LANES), BF16),
            vmem((SIDE, ROW * kb, LANES), BF16),
            vmem((NP, kb, LANES), BF16),
            vmem((NP * coef, half * LANES), BF16),
            vmem((NP // 2, half * LANES, 2 * coef), BF16),
            vmem((SIDE, ROW * 5 * LANES, 2 * LANES), BF16),
            vmem((NP // 2, 2 * LANES, 6 * LANES), BF16),
            vmem((NP // 4, 8 * kb, 4 * coef), BF16),
            vmem((SIDE, pairs, ROW * 5 * LANES), BF16),
            vmem((pairs, 2 * LANES), F32),
            vmem((OWNERS, piece, LANES), i32),
            vmem((OWNERS, 4, LANES), F32),
            vmem((nb, piece, LANES), i32),
            vmem((nb, 4, LANES), F32),
            vmem((piece, LANES), i32),
            vmem((2, LANES), F32),
            vmem((OWNERS, piece, LANES), i32),
            vmem((OWNERS, 2, LANES), F32),
            vmem((1, LANES), F32),
            vmem((OWNERS * NP, 1, LANES), F32),
            vmem((1, LANES), F32),
            vmem((NP, 1, LANES), F32),
            vmem((pairs, 2 * LANES), F32),
            vmem((pairs, 2 * LANES), BF16),
            vmem((ROW // 2, 6 * kb, half * LANES), BF16),
            vmem((NP, 24, LANES), BF16),
            vmem((1152, 1, LANES), F32),
            dma((len(arrays) + 1,)),
            dma,
            dma((SIDE,)),
            dma((SIDE,)),
            dma,
            dma((nb,)),
            dma,
            dma,
            dma((OWNERS,)),
            *[dma] * 8,
            regular((SIDE,)),
            regular,
            regular((OWNERS,)),
            regular,
            regular,
        ],
        compiler_params=pltpu.CompilerParams(
            collective_id=0, has_side_effects=True, vmem_limit_bytes=40 * 1024 * 1024
        ),
        name="averaging",
    )(*[pltpu.with_memory_space_constraint(a, pltpu.HBM) for a in arrays])
    sums, weights, evidence = pl.pallas_call(
        finish,
        out_shape=[
            jax.ShapeDtypeStruct((classes_n, 2 * coef), F32),
            jax.ShapeDtypeStruct((coef, classes_n), F32),
            jax.ShapeDtypeStruct((1, count), F32),
        ],
        in_specs=[pl.BlockSpec(memory_space=vmem)] * 3,
        out_specs=[pl.BlockSpec(memory_space=vmem)] * 3,
        compiler_params=pltpu.CompilerParams(vmem_limit_bytes=4 * 1024 * 1024),
        name="finish",
    )(mine, other, evidence)
    return sums, weights.T, evidence.reshape(-1)


def solution(mesh):
    nz = mesh.shape["shell"] // ROW
    split = Mesh(mesh.devices.reshape(mesh.shape["groups"], ROW, nz, mesh.shape["batch"]), AXES)
    shell = ("x", "z")
    placed = (
        P(("groups", "batch"), shell),
        P("groups", shell),
        P("groups", shell),
        P("groups"),
        P(shell),
        P(None, shell),
        P(("groups", "batch")),
    )
    return jax.shard_map(
        functools.partial(body, nz),
        mesh=split,
        in_specs=placed,
        out_specs=(P("groups", shell), P("groups", shell), P(("groups", "batch"))),
        check_vma=False,
    )
```
